8 devices in a mesh: dp: 1 (over z), tp: 2 (over y), sp: 4 (over x, core).
Axes of the slice: x: 2, y: 2, z: 1, core: 2. Of those that a mesh axis runs over, the one named last changes fastest.
Arguments:
- hidden: bfloat16 [64, 4096], P('dp')
- positions: int32 [64], P('dp')
- k_cache: bfloat16 [2, 64, 512, 8, 128], P(None, 'dp', 'sp', 'tp')
- v_cache: bfloat16 [2, 64, 512, 8, 128], P(None, 'dp', 'sp', 'tp')
- ln_gain: bfloat16 [2, 2, 4096], replicated
- ln_bias: bfloat16 [2, 2, 4096], replicated
- w_qkv: bfloat16 [2, 4096, 6144], P(None, None, 'tp')
- b_qkv: bfloat16 [2, 6144], P(None, 'tp')
- w_dense: bfloat16 [2, 4096, 4096], P(None, 'tp')
- b_dense: bfloat16 [2, 4096], replicated
- w_up: bfloat16 [2, 4096, 28672], P(None, None, 'tp')
- b_up: bfloat16 [2, 28672], P(None, 'tp')
- w_down: bfloat16 [2, 14336, 4096], P(None, 'tp')
- b_down: bfloat16 [2, 4096], replicated
Outputs:
- output 1: bfloat16 [64, 4096], P('dp')
- output 2: bfloat16 [2, 64, 512, 8, 128], P(None, 'dp', 'sp', 'tp')
- output 3: bfloat16 [2, 64, 512, 8, 128], P(None, 'dp', 'sp', 'tp')
All inputs are finite; a program needn't handle non-finite values.
Results may differ from the reference program's by a relative error of at most 0.0172843.
Values sent between devices are 32-bit elements.
A program may use at most 2 GiB of HBM per device.

```python
import functools
import jax
import jax.numpy as jnp
from jax import lax

NUM_SEQS = 64
SEQ_LEN = 512
D_MODEL = 4096
N_HEADS = 32
KV_HEADS = 8
HEAD_DIM = 128
FF_DIM = 14336
BLOCK_SIZE = 64
LOCAL_BLOCKS = 16
VERT_STRIDE = 8
ROPE_THETA = 1000000.0
GELU_LIMIT = 20.0
NORM_EPS = 0.00001
MASKED = -1e30
GROUP_SIZE = N_HEADS // KV_HEADS
QKV_COLS = KV_HEADS * (GROUP_SIZE + 2) * HEAD_DIM
QK_GAIN = (3.0 * HEAD_DIM ** 0.5) ** 0.5
V_GAIN = 1.5


def normal_draw(key, shape, scale):
    return (jax.random.normal(key, shape, jnp.float32) * scale).astype(jnp.bfloat16)


def setup_inputs(seed: int = 0, part: int = 0) -> dict:
    base = jax.random.key(seed)
    shared = jax.random.split(base, 10)
    local = jax.random.split(jax.random.fold_in(base, part), 4)
    slot_gain = jnp.concatenate([jnp.full((GROUP_SIZE + 1,), QK_GAIN, jnp.float32), jnp.full((1,), V_GAIN, jnp.float32)])
    col_gain = jnp.tile(jnp.repeat(slot_gain, HEAD_DIM), KV_HEADS)
    seq_ids = jnp.arange(NUM_SEQS)
    rand_pos = jax.random.randint(local[1], (NUM_SEQS,), 0, SEQ_LEN)
    positions = jnp.where(seq_ids == 0, SEQ_LEN - 1, jnp.where(seq_ids == 1, SEQ_LEN // 2 + BLOCK_SIZE // 2, rand_pos))
    cache_shape = (2, NUM_SEQS, SEQ_LEN, KV_HEADS, HEAD_DIM)
    return {
        'hidden': normal_draw(local[0], (NUM_SEQS, D_MODEL), 1.0),
        'positions': positions.astype(jnp.int32),
        'k_cache': normal_draw(local[2], cache_shape, QK_GAIN),
        'v_cache': normal_draw(local[3], cache_shape, V_GAIN),
        'ln_gain': jax.random.uniform(shared[0], (2, 2, D_MODEL), jnp.float32, 0.5, 1.5).astype(jnp.bfloat16),
        'ln_bias': normal_draw(shared[1], (2, 2, D_MODEL), 0.3),
        'w_qkv': normal_draw(shared[2], (2, D_MODEL, QKV_COLS), col_gain * D_MODEL ** -0.5),
        'b_qkv': normal_draw(shared[3], (2, QKV_COLS), col_gain * 0.5),
        'w_dense': normal_draw(shared[4], (2, N_HEADS * HEAD_DIM, D_MODEL), (N_HEADS * HEAD_DIM) ** -0.5),
        'b_dense': normal_draw(shared[5], (2, D_MODEL), 0.3),
        'w_up': normal_draw(shared[6], (2, D_MODEL, 2 * FF_DIM), D_MODEL ** -0.5),
        'b_up': normal_draw(shared[7], (2, 2 * FF_DIM), 0.3),
        'w_down': normal_draw(shared[8], (2, FF_DIM, D_MODEL), FF_DIM ** -0.5),
        'b_down': normal_draw(shared[9], (2, D_MODEL), 0.3),
    }


def layer_norm(vec, gain, shift):
    wide_vec = vec.astype(jnp.float32)
    mean_val = jnp.mean(wide_vec, axis=-1, keepdims=True)
    variance = jnp.mean(jnp.square(wide_vec - mean_val), axis=-1, keepdims=True)
    normed = (wide_vec - mean_val) * lax.rsqrt(variance + NORM_EPS)
    return (normed * gain.astype(jnp.float32) + shift.astype(jnp.float32)).astype(jnp.bfloat16)


def rotary(col_pairs, positions):
    half_dim = HEAD_DIM // 2
    inv_freq = ROPE_THETA ** (-jnp.arange(half_dim).astype(jnp.float32) * (2.0 / HEAD_DIM))
    angles = positions.astype(jnp.float32)[:, None] * inv_freq[None, :]
    cos_part = jnp.cos(angles)[:, None, None, :]
    sin_part = jnp.sin(angles)[:, None, None, :]
    first_half = col_pairs[..., :half_dim]
    second_half = col_pairs[..., half_dim:]
    return jnp.concatenate([first_half * cos_part - second_half * sin_part, second_half * cos_part + first_half * sin_part], axis=-1)


def gegelu(up_proj):
    col_pairs = up_proj.reshape(up_proj.shape[0], -1, 2)
    gate_part = jnp.minimum(col_pairs[..., 0], GELU_LIMIT)
    linear_part = jnp.clip(col_pairs[..., 1], -GELU_LIMIT, GELU_LIMIT)
    return gate_part * jax.nn.sigmoid(1.702 * gate_part) * (linear_part + 1.0)


def seq_attention(packed, sparse):
    query_rot, key_rows, value_rows, position = packed
    slot_ids = jnp.arange(SEQ_LEN)
    keep_mask = (slot_ids <= position)[None, None, :]
    if sparse:
        blocks = slot_ids // BLOCK_SIZE
        head_ids = jnp.arange(N_HEADS).reshape(KV_HEADS, GROUP_SIZE)
        near_mask = (position // BLOCK_SIZE - blocks) < LOCAL_BLOCKS
        vertical = (blocks[None, None, :] + head_ids[:, :, None] + 1) % VERT_STRIDE == 0
        keep_mask = keep_mask & (near_mask[None, None, :] | vertical)
    scores = jnp.einsum('kgd,skd->kgs', query_rot.astype(jnp.float32), key_rows.astype(jnp.float32)) / HEAD_DIM
    scores = jnp.where(keep_mask, scores, MASKED)
    peak_score = jnp.max(scores, axis=-1, keepdims=True)
    weights = jnp.where(keep_mask, jnp.exp(scores - peak_score), 0.0)
    mixed_vals = jnp.einsum('kgs,skd->kgd', weights, value_rows.astype(jnp.float32))
    return (mixed_vals / jnp.sum(weights, axis=-1, keepdims=True)).astype(jnp.bfloat16)


def decoder_layer(hidden, positions, k_layer, v_layer, params, sparse):
    gains, shifts, w_qkv, b_qkv, w_dense, b_dense, w_up, b_up, w_down, b_down = params
    normed = layer_norm(hidden, gains[0], shifts[0])
    qkv_proj = jnp.dot(normed, w_qkv, preferred_element_type=jnp.float32) + b_qkv.astype(jnp.float32)
    qkv_proj = qkv_proj.reshape(NUM_SEQS, KV_HEADS, GROUP_SIZE + 2, HEAD_DIM)
    turned = rotary(qkv_proj[:, :, :GROUP_SIZE + 1], positions)
    query_rot = turned[:, :, :GROUP_SIZE].astype(jnp.bfloat16)
    k_new = turned[:, :, GROUP_SIZE].astype(jnp.bfloat16)
    v_new = qkv_proj[:, :, GROUP_SIZE + 1].astype(jnp.bfloat16)
    hit_mask = (jnp.arange(SEQ_LEN)[None, :] == positions[:, None])[:, :, None, None]
    k_layer = jnp.where(hit_mask, k_new[:, None], k_layer)
    v_layer = jnp.where(hit_mask, v_new[:, None], v_layer)
    attn_out = lax.map(functools.partial(seq_attention, sparse=sparse), (query_rot, k_layer, v_layer, positions))
    attn_proj = jnp.dot(attn_out.reshape(NUM_SEQS, N_HEADS * HEAD_DIM), w_dense, preferred_element_type=jnp.float32)
    residual = (hidden.astype(jnp.float32) + attn_proj + b_dense.astype(jnp.float32)).astype(jnp.bfloat16)
    normed_two = layer_norm(residual, gains[1], shifts[1])
    up_proj = jnp.dot(normed_two, w_up, preferred_element_type=jnp.float32) + b_up.astype(jnp.float32)
    gated = gegelu(up_proj).astype(jnp.bfloat16)
    down_proj = jnp.dot(gated, w_down, preferred_element_type=jnp.float32)
    out_hidden = (residual.astype(jnp.float32) + down_proj + b_down.astype(jnp.float32)).astype(jnp.bfloat16)
    return out_hidden, k_layer, v_layer


def reference(hidden, positions, k_cache, v_cache, ln_gain, ln_bias, w_qkv, b_qkv, w_dense, b_dense, w_up, b_up, w_down, b_down):
    k_layers = []
    v_layers = []
    for layer_idx in range(2):
        params = tuple(arr[layer_idx] for arr in (ln_gain, ln_bias, w_qkv, b_qkv, w_dense, b_dense, w_up, b_up, w_down, b_down))
        hidden, k_layer, v_layer = decoder_layer(hidden, positions, k_cache[layer_idx], v_cache[layer_idx], params, layer_idx == 0)
        k_layers.append(k_layer)
        v_layers.append(v_layer)
    return hidden, jnp.stack(k_layers), jnp.stack(v_layers)
```

```python
import functools

import jax
import jax.numpy as jnp
from jax import lax
from jax.experimental import pallas as pl
from jax.experimental.pallas import tpu as pltpu
from jax.sharding import PartitionSpec as P

BLOCK_SIZE = 64
LOCAL_BLOCKS = 16
VERT_STRIDE = 8
ROPE_THETA = 1000000.0
GELU_LIMIT = 20.0
NORM_EPS = 0.00001
MASKED = -1e30

SEQS = 64
MODEL = 4096
HEAD = 128
KVL = 4
GROUP = 4
HEADS = KVL * GROUP
SLOTS = 128
ROWS = SLOTS * KVL
QKV_N = (GROUP + 2) * HEAD
UP_N = 512
UP_STEPS = 7
DOWN_K = 3584
HALF_K = DOWN_K // 2
PIECE = 256
CHUNK = 8
VMEM_LIMIT = 63 * 1024 * 1024

F32 = jnp.float32
BF16 = jnp.bfloat16
MESH = pl.DeviceIdType.MESH
VM = pl.BlockSpec(memory_space=pltpu.VMEM)
SM = pl.BlockSpec(memory_space=pltpu.SMEM)
ANY = pl.BlockSpec(memory_space=pl.ANY)


def dot(a, b):
    return jnp.dot(a, b, preferred_element_type=F32)


def place():
    sp = lax.axis_index('sp')
    return lax.axis_index('tp'), sp, sp // 2, lax.rem(sp, 2)


def enter(peers):
    barrier = pltpu.get_barrier_semaphore()
    for peer in peers:
        pl.semaphore_signal(barrier, inc=1, device_id=peer, device_id_type=MESH)
    pl.semaphore_wait(barrier, len(peers))


def remote(src, dst, send, recv, peer):
    return pltpu.make_async_remote_copy(src_ref=src, dst_ref=dst, send_sem=send, recv_sem=recv, device_id=peer, device_id_type=MESH)


def norm_into(pieces, gain, shift, out_ref):
    width = pieces[0]().shape[1]
    total = sum(jnp.sum(p(), axis=1, keepdims=True) for p in pieces)
    mean = total * (1.0 / MODEL)
    square = sum(jnp.sum(jnp.square(p() - mean), axis=1, keepdims=True) for p in pieces)
    scale = lax.rsqrt(square * (1.0 / MODEL) + NORM_EPS)
    for i, p in enumerate(pieces):
        cols = slice(i * width, (i + 1) * width)
        out_ref[:, cols] = ((p() - mean) * scale * gain(cols) + shift(cols)).astype(BF16)


def qkv_kernel(layer, h_ref, cos_ref, sin_ref, gain_ref, shift_ref, bias_ref, w_ref, out_ref, wbuf, u, heads, wsem, ssem, rsem):
    tp, sp, x, c = place()
    loads = []
    for j in range(2):
        cols = pl.ds(pl.multiple_of(c * (2 * QKV_N) + j * QKV_N, 128), QKV_N)
        loads.append(pltpu.make_async_copy(w_ref.at[layer, :, cols], wbuf.at[j], wsem.at[j]))
        loads[-1].start()
    partner = {'sp': sp + 1 - 2 * c}
    norm_into(
        [lambda i=i: h_ref[:, i * 512:(i + 1) * 512].astype(F32) for i in range(8)],
        lambda cols: gain_ref[layer, 0:1, cols].astype(F32),
        lambda cols: shift_ref[layer, 0:1, cols].astype(F32),
        u,
    )
    enter([partner])
    sent = []
    for j in range(2):
        loads[j].wait()
        kv = 2 * c + j
        cols = pl.ds(pl.multiple_of(kv * QKV_N, 128), QKV_N)
        proj = dot(u[...], wbuf[j]) + bias_ref[layer:layer + 1, cols].astype(F32)
        for i in range(GROUP + 2):
            part = proj[:, i * HEAD:(i + 1) * HEAD]
            if i <= GROUP:
                part = part * cos_ref[...] + pltpu.roll(part, HEAD // 2, 1) * sin_ref[...]
            slot = kv * GROUP + i if i < GROUP else HEADS + (i - GROUP) * KVL + kv
            heads[slot] = part.astype(BF16).astype(F32)
        for n, piece in enumerate((pl.ds(kv * GROUP, GROUP), pl.ds(HEADS + kv, 1), pl.ds(HEADS + KVL + kv, 1))):
            copy = remote(heads.at[piece], heads.at[piece], ssem.at[3 * j + n], rsem.at[3 * j + n], partner)
            copy.start()
            sent.append(copy)
    for copy in sent:
        copy.wait()
    out_ref[...] = heads[...]


def project(layer, h, cos, sin, gain, shift, bias, w):
    return pl.pallas_call(
        functools.partial(qkv_kernel, layer),
        out_shape=jax.ShapeDtypeStruct((HEADS + 2 * KVL, SEQS, HEAD), F32),
        in_specs=[VM] * 6 + [ANY],
        out_specs=VM,
        scratch_shapes=[
            pltpu.VMEM((2, MODEL, QKV_N), BF16),
            pltpu.VMEM((SEQS, MODEL), BF16),
            pltpu.VMEM((HEADS + 2 * KVL, SEQS, HEAD), F32),
            pltpu.SemaphoreType.DMA((2,)),
            pltpu.SemaphoreType.DMA((6,)),
            pltpu.SemaphoreType.DMA((6,)),
        ],
        compiler_params=pltpu.CompilerParams(collective_id=layer, has_side_effects=True, vmem_limit_bytes=VMEM_LIMIT),
        name=f'qkv_{layer}',
    )(h, cos, sin, gain, shift, bias, w)


def attend_kernel(layer, sparse, pos_ref, heads_ref, kc_ref, vc_ref, *rest):
    if layer:
        rest = rest[2:]
    ko_ref, vo_ref, o_ref, ml_ref, kb, vb, mref, lref, slot_of, keep_of, lsem, ssem = rest
    tp, sp, x, c = place()
    steps = SEQS // CHUNK

    def load(i, n):
        src, buf = ((kc_ref, kb), (vc_ref, vb))[n]
        rows = pl.ds(i * CHUNK, CHUNK)
        return pltpu.make_async_copy(src.at[layer, rows], buf.at[rows], lsem.at[n, i])

    def save(i, n):
        dst, buf = ((ko_ref, kb), (vo_ref, vb))[n]
        rows = pl.ds(i * CHUNK, CHUNK)
        return pltpu.make_async_copy(buf.at[rows], dst.at[layer, rows], ssem.at[n, i])

    for i in range(steps):
        for n in range(2):
            load(i, n).start()
    row = lax.broadcasted_iota(jnp.int32, (HEADS, ROWS), 0)
    col = lax.broadcasted_iota(jnp.int32, (HEADS, ROWS), 1)
    slot = sp * SLOTS + col // KVL
    slot_of[...] = jnp.where(lax.rem(col, KVL) == row // GROUP, slot, jnp.int32(1 << 30))
    if sparse:
        block = slot // BLOCK_SIZE
        vertical = lax.rem(block + tp * HEADS + row + 1, VERT_STRIDE) == 0
        keep_of[...] = jnp.where(vertical, jnp.int32(1 << 20), block)
    mref[...] = jnp.zeros_like(mref)
    lref[...] = jnp.ones_like(lref)
    lane = lax.broadcasted_iota(jnp.int32, (HEADS, HEAD), 1)
    row16 = lax.broadcasted_iota(jnp.int32, (4 * KVL, HEAD), 0)

    def body(i, _):
        for n in range(2):
            load(i, n).wait()
        for s in range(CHUNK):
            b = i * CHUNK + s
            t = pos_ref[b] - sp * SLOTS
            inside = jnp.logical_and(t >= 0, t < SLOTS)
            t = jnp.clip(t, 0, SLOTS - 1)
            base = pl.multiple_of((t // 4) * (4 * KVL), 4 * KVL)
            hit = jnp.logical_and(row16 // KVL == lax.rem(t, 4), inside)
            new = heads_ref[pl.ds(HEADS * SEQS + b, 2 * KVL, stride=SEQS), :]
            for buf, part in ((kb, new[:KVL]), (vb, new[KVL:])):
                tile = buf[b, pl.ds(base, 4 * KVL), :].astype(F32)
                buf[b, pl.ds(base, 4 * KVL), :] = jnp.where(hit, jnp.concatenate([part] * 4, axis=0), tile).astype(BF16)
        for n in range(2):
            save(i, n).start()
        for first in range(0, CHUNK, 4):
            ids = [i * CHUNK + first + s for s in range(4)]
            keeps, scores = [], []
            for b in ids:
                q = heads_ref[pl.ds(b, HEADS, stride=SEQS), :].astype(BF16)
                raw = lax.dot_general(q, kb[b], (((1,), (1,)), ((), ())), preferred_element_type=F32)
                pos = pos_ref[b]
                keep = slot_of[...] <= pos
                if sparse:
                    keep = jnp.logical_and(keep, pos // BLOCK_SIZE - keep_of[...] < LOCAL_BLOCKS)
                keeps.append(keep)
                scores.append(jnp.where(keep, raw * (1.0 / HEAD), MASKED))
            weights = []
            for b, keep, score in zip(ids, keeps, scores):
                peak = jnp.max(score, axis=1, keepdims=True)
                weight = jnp.where(keep, jnp.exp(score - peak), 0.0)
                weights.append(weight.astype(BF16))
                mref[...] = jnp.where(lane == b, peak, mref[...])
                lref[...] = jnp.where(lane == b, jnp.sum(weight, axis=1, keepdims=True), lref[...])
            for b, weight in zip(ids, weights):
                o_ref[pl.ds(b, HEADS, stride=SEQS), :] = dot(weight, vb[b])
        return 0

    lax.fori_loop(0, steps, body, 0)
    for kv in range(KVL):
        ml_ref[kv, 0:GROUP] = mref[kv * GROUP:(kv + 1) * GROUP]
        ml_ref[kv, GROUP:2 * GROUP] = lref[kv * GROUP:(kv + 1) * GROUP]
    for i in range(steps):
        for n in range(2):
            save(i, n).wait()


def attend(layer, positions, heads, kc, vc, *done):
    cache = jax.ShapeDtypeStruct(kc.shape, BF16)
    return pl.pallas_call(
        functools.partial(attend_kernel, layer, layer == 0),
        out_shape=(cache, cache, jax.ShapeDtypeStruct((HEADS * SEQS, HEAD), F32), jax.ShapeDtypeStruct((KVL, 2 * GROUP, HEAD), F32)),
        in_specs=[SM, VM, ANY, ANY] + [ANY] * len(done),
        out_specs=(ANY, ANY, VM, VM),
        scratch_shapes=[
            pltpu.VMEM((SEQS, ROWS, HEAD), BF16),
            pltpu.VMEM((SEQS, ROWS, HEAD), BF16),
            pltpu.VMEM((HEADS, HEAD), F32),
            pltpu.VMEM((HEADS, HEAD), F32),
            pltpu.VMEM((HEADS, ROWS), jnp.int32),
            pltpu.VMEM((HEADS, ROWS), jnp.int32),
            pltpu.SemaphoreType.DMA((2, SEQS // CHUNK)),
            pltpu.SemaphoreType.DMA((2, SEQS // CHUNK)),
        ],
        input_output_aliases={4: 0, 5: 1} if done else {},
        compiler_params=pltpu.CompilerParams(vmem_limit_bytes=VMEM_LIMIT),
        name=f'attend_{layer}',
    )(positions, heads, kc, vc, *done)


def mlp_kernel(
    layer, o_ref, ml_ref, h_ref, gain_ref, shift_ref, bd_ref, bu_ref, bn_ref, wd_ref, wu_ref, wn_ref, out_ref,
    wd, wu, wn, mls, fromcore, tosend, kept, fromx, mine, other, ob, part, ra, rb, xs, u, mf, mp, mb,
    wsem, mls_s, mls_r, o_s, o_r, m_s, m_r, c_s, c_r,
):
    tp, sp, x, c = place()
    y = tp
    core_peer = {'sp': sp + 1 - 2 * c}
    x_peer = {'sp': lax.rem(sp + 2, 4)}
    x_diag = {'sp': 2 * (1 - x) + 1 - c}
    y_peer = {'tp': 1 - tp}
    quarter = [2 * (1 - x) + 1 - y, 2 * (1 - x) + y, 2 * x + 1 - y, 2 * x + y]

    def cols_of(k):
        return pl.ds(pl.multiple_of(c * 2048 + quarter[k] * 512, 512), 512)

    def load_dense(k):
        return pltpu.make_async_copy(wd_ref.at[layer, pl.ds(pl.multiple_of(x * 1024, 1024), 1024), cols_of(k)], wd.at[k], wsem.at[k])

    def load_up(j):
        cols = pl.ds(pl.multiple_of(x * 7168 + c * 3584 + j * UP_N, UP_N), UP_N)
        return pltpu.make_async_copy(wu_ref.at[layer, :, cols], wu.at[j], wsem.at[4 + j])

    def load_down(k):
        return pltpu.make_async_copy(wn_ref.at[layer, pl.ds(pl.multiple_of(x * DOWN_K, DOWN_K), DOWN_K), cols_of(k)], wn.at[k], wsem.at[4 + UP_STEPS + k])

    for k in range(4):
        load_dense(k).start()
    for j in range(UP_STEPS):
        load_up(j).start()
    for k in range(4):
        load_down(k).start()
    enter([core_peer, x_peer, x_diag, y_peer])

    waits = []

    def send(*args):
        copy = remote(*args)
        copy.start()
        waits.append(copy)
        return copy

    stats = []
    for r in range(1, 4):
        stats.append(send(ml_ref, mls.at[sp], mls_s.at[r - 1], mls_r.at[r - 1], {'sp': lax.rem(sp + r, 4)}))
    slabs = [None, None]
    for n, xd in enumerate((1 - x, x)):
        src = o_ref.at[pl.ds((2 * xd + 1 - c) * GROUP, GROUP)]
        slabs[n] = send(src, fromcore.at[n], o_s.at[n], o_r.at[n], core_peer)
    mls[sp] = ml_ref[...]
    for copy in stats:
        copy.wait_recv()
    rows = []
    for xd in (1 - x, x):
        kv = 2 * xd + c
        tiles = [mls[i, kv] for i in range(4)]
        top = functools.reduce(jnp.maximum, [t[:GROUP] for t in tiles])
        norm = sum(jnp.exp(t[:GROUP] - top) * t[GROUP:] for t in tiles)
        for who in (sp, sp + 1 - 2 * c):
            rows.append(jnp.exp(mls[who, kv][:GROUP] - top) / norm)
    scale = jnp.concatenate(rows + [jnp.zeros((HEAD - 4 * GROUP, HEAD), F32)], axis=0).T[:SEQS]
    for n, (xd, out) in enumerate(((1 - x, tosend), (x, kept))):
        slabs[n].wait_recv()
        kv = 2 * xd + c
        for g in range(GROUP):
            i = 2 * n * GROUP + g
            out[g] = o_ref[kv * GROUP + g] * scale[:, i:i + 1] + fromcore[n, g] * scale[:, i + GROUP:i + GROUP + 1]
        if n == 0:
            cross = send(tosend, fromx, o_s.at[2], o_r.at[2], x_peer)
    cross.wait_recv()
    for g in range(GROUP):
        val = (kept[g] + fromx[g]).astype(BF16)
        mine[g] = val.astype(F32)
        ob[:, pl.ds(pl.multiple_of(c * 512 + g * HEAD, HEAD), HEAD)] = val
    share = send(mine, other, o_s.at[3], o_r.at[3], core_peer)
    share.wait_recv()
    for g in range(GROUP):
        ob[:, pl.ds(pl.multiple_of((1 - c) * 512 + g * HEAD, HEAD), HEAD)] = other[g].astype(BF16)

    own = (c * 4 + quarter[3]) * 2

    def all_reduce(ph, chunk, residual, bias_ref):
        def post(i, src, dst, peer):
            return send(src, dst, c_s.at[ph, i], c_r.at[ph, i], peer)

        def keep(k):
            val = chunk(k)
            part[ph, k, 0] = val[:, :PIECE]
            part[ph, k, 1] = val[:, PIECE:]

        keep(0)
        a0 = post(0, part.at[ph, 0, 0], ra.at[ph, 0], x_peer)
        b0 = post(1, part.at[ph, 0, 1], rb.at[ph, 0], y_peer)
        keep(1)
        a1 = post(2, part.at[ph, 1, 0], ra.at[ph, 1], x_peer)
        keep(2)
        b1 = post(3, part.at[ph, 2, 1], rb.at[ph, 1], y_peer)
        keep(3)
        b0.wait_recv()
        part[ph, 1, 1] = part[ph, 1, 1] + rb[ph, 0]
        b2 = post(4, part.at[ph, 1, 1], rb.at[ph, 2], x_peer)
        a0.wait_recv()
        part[ph, 2, 0] = part[ph, 2, 0] + ra[ph, 0]
        a2 = post(5, part.at[ph, 2, 0], ra.at[ph, 2], y_peer)
        gather = {}
        for half, (first, second, landed) in enumerate(((a1, a2, ra), (b1, b2, rb))):
            first.wait_recv()
            second.wait_recv()
            cols = pl.ds(pl.multiple_of((own + half) * PIECE, PIECE), PIECE)
            full = part[ph, 3, half] + landed[ph, 1] + landed[ph, 2]
            xs[ph, own + half] = (residual(half, cols) + full + bias_ref[layer:layer + 1, cols].astype(F32)).astype(BF16).astype(F32)
            mine_ref = xs.at[ph, own + half]
            for n, peer in enumerate((x_peer, y_peer, core_peer) if half == 0 else (y_peer, x_peer, core_peer)):
                gather[half, n] = post(6 + 3 * half + n, mine_ref, mine_ref, peer)
        base = c * 8
        from_x = base + quarter[1] * 2
        from_y = base + quarter[2] * 2
        far = base + quarter[0] * 2

        def forward(i, piece, peer):
            ref = xs.at[ph, piece]
            return post(i, ref, ref, peer)

        gather[0, 0].wait_recv()
        far_a = forward(12, from_x, y_peer)
        arrived = [forward(14, from_x, core_peer)]
        gather[1, 0].wait_recv()
        far_b = forward(13, from_y + 1, x_peer)
        arrived.append(forward(15, from_y + 1, core_peer))
        gather[0, 1].wait_recv()
        arrived.append(forward(16, from_y, core_peer))
        gather[1, 1].wait_recv()
        arrived.append(forward(17, from_x + 1, core_peer))
        far_a.wait_recv()
        arrived.append(forward(18, far, core_peer))
        far_b.wait_recv()
        arrived.append(forward(19, far + 1, core_peer))
        for copy in arrived + [gather[0, 2], gather[1, 2]]:
            copy.wait_recv()

    def dense_chunk(k):
        load_dense(k).wait()
        return dot(ob[...], wd[k])

    all_reduce(0, dense_chunk, lambda half, cols: h_ref[:, cols].astype(F32), bd_ref)
    norm_into(
        [lambda i=i: xs[0, i] for i in range(16)],
        lambda cols: gain_ref[layer, 1:2, cols].astype(F32),
        lambda cols: shift_ref[layer, 1:2, cols].astype(F32),
        u,
    )
    take = (lax.broadcasted_iota(jnp.int32, (2 * HEAD, HEAD), 0) == 2 * lax.broadcasted_iota(jnp.int32, (2 * HEAD, HEAD), 1)).astype(BF16)
    even = lax.rem(lax.broadcasted_iota(jnp.int32, (SEQS, UP_N), 1), 2) == 0

    def share_m(j):
        return remote(mf.at[j], mp.at[j], m_s.at[j], m_r.at[j], core_peer)

    def up_step(j, _):
        load_up(j).wait()
        cols = pl.ds(pl.multiple_of(x * 7168 + c * 3584 + j * UP_N, UP_N), UP_N)
        val = dot(u[...], wu[j]) + bu_ref[layer:layer + 1, cols].astype(F32)
        gate = jnp.minimum(val, GELU_LIMIT)
        gate = gate * (1.0 / (1.0 + jnp.exp(-1.702 * gate)))
        linear = jnp.clip(val, -GELU_LIMIT, GELU_LIMIT) + 1.0
        mixed = jnp.where(even, gate * pltpu.roll(linear, UP_N - 1, 1), 0.0).astype(BF16)
        packed = jnp.concatenate([dot(mixed[:, i:i + 2 * HEAD], take) for i in range(0, UP_N, 2 * HEAD)], axis=1)
        mf[j] = packed
        share_m(j).start()
        mb[:, pl.ds(pl.multiple_of(c * HALF_K + j * 256, 256), 256)] = packed.astype(BF16)
        return 0

    lax.fori_loop(0, UP_STEPS, up_step, 0)
    for j in range(UP_STEPS):
        share_m(j).wait()
        mb[:, pl.ds(pl.multiple_of((1 - c) * HALF_K + j * 256, 256), 256)] = mp[j].astype(BF16)

    def down_chunk(k):
        load_down(k).wait()
        return dot(mb[...], wn[k])

    all_reduce(1, down_chunk, lambda half, cols: xs[0, own + half], bn_ref)
    for i in range(16):
        out_ref[:, i * PIECE:(i + 1) * PIECE] = xs[1, i].astype(BF16)
    for copy in waits:
        copy.wait_send()


def finish(layer, o, ml, h, gain, shift, bd, bu, bn, wd, wu, wn):
    slab = pltpu.VMEM((GROUP, SEQS, HEAD), F32)
    dma = pltpu.SemaphoreType.DMA
    return pl.pallas_call(
        functools.partial(mlp_kernel, layer),
        out_shape=jax.ShapeDtypeStruct((SEQS, MODEL), BF16),
        in_specs=[VM] * 8 + [ANY] * 3,
        out_specs=VM,
        scratch_shapes=[
            pltpu.VMEM((4, 1024, 512), BF16),
            pltpu.VMEM((UP_STEPS, MODEL, UP_N), BF16),
            pltpu.VMEM((4, DOWN_K, 512), BF16),
            pltpu.VMEM((4, KVL, 2 * GROUP, HEAD), F32),
            pltpu.VMEM((2, GROUP, SEQS, HEAD), F32),
            slab, slab, slab, slab, slab,
            pltpu.VMEM((SEQS, 1024), BF16),
            pltpu.VMEM((2, 4, 2, SEQS, PIECE), F32),
            pltpu.VMEM((2, 3, SEQS, PIECE), F32),
            pltpu.VMEM((2, 3, SEQS, PIECE), F32),
            pltpu.VMEM((2, 16, SEQS, PIECE), F32),
            pltpu.VMEM((SEQS, MODEL), BF16),
            pltpu.VMEM((UP_STEPS, SEQS, 256), F32),
            pltpu.VMEM((UP_STEPS, SEQS, 256), F32),
            pltpu.VMEM((SEQS, DOWN_K), BF16),
            dma((8 + UP_STEPS,)), dma((3,)), dma((3,)), dma((4,)), dma((4,)), dma((UP_STEPS,)), dma((UP_STEPS,)), dma((2, 20)), dma((2, 20)),
        ],
        compiler_params=pltpu.CompilerParams(collective_id=2 + layer, has_side_effects=True, vmem_limit_bytes=VMEM_LIMIT),
        name=f'mlp_{layer}',
    )(o, ml, h, gain, shift, bd, bu, bn, wd, wu, wn)


def solution(mesh):
    cache_spec = P(None, 'dp', 'sp', 'tp', None)
    in_specs = (P('dp', None), P('dp'), cache_spec, cache_spec, P(), P(), P(None, None, 'tp'), P(None, 'tp'), P(None, 'tp', None), P(), P(None, None, 'tp'), P(None, 'tp'), P(None, 'tp', None), P())
    out_specs = (P('dp', None), cache_spec, cache_spec)

    def device_step(hidden, positions, k_cache, v_cache, ln_gain, ln_bias, w_qkv, b_qkv, w_dense, b_dense, w_up, b_up, w_down, b_down):
        half = HEAD // 2
        inv_freq = ROPE_THETA ** (-jnp.arange(half).astype(F32) * (2.0 / HEAD))
        angles = positions.astype(F32)[:, None] * inv_freq[None, :]
        cos = jnp.cos(angles)
        sin = jnp.sin(angles)
        cos = jnp.concatenate([cos, cos], axis=1)
        sin = jnp.concatenate([-sin, sin], axis=1)
        shape = k_cache.shape
        flat = (2, SEQS, ROWS, HEAD)
        kc = k_cache.reshape(flat)
        vc = v_cache.reshape(flat)
        done = ()
        for layer in range(2):
            heads = project(layer, hidden, cos, sin, ln_gain, ln_bias, b_qkv, w_qkv)
            ko, vo, o, ml = attend(layer, positions, heads.reshape(-1, HEAD), kc, vc, *done)
            done = (ko, vo)
            hidden = finish(layer, o.reshape(HEADS, SEQS, HEAD), ml, hidden, ln_gain, ln_bias, b_dense, b_up, b_down, w_dense, w_up, w_down)
        return hidden, done[0].reshape(shape), done[1].reshape(shape)

    return jax.shard_map(device_step, mesh=mesh, in_specs=in_specs, out_specs=out_specs, check_vma=False)
```

```python
import functools

import jax
import jax.numpy as jnp
import numpy as np
from jax import lax
from jax.experimental import pallas as pl
from jax.experimental.pallas import tpu as pltpu
from jax.sharding import PartitionSpec as P

BLOCK_SIZE = 64
LOCAL_BLOCKS = 16
VERT_STRIDE = 8
ROPE_THETA = 1000000.0
GELU_LIMIT = 20.0
NORM_EPS = 0.00001
MASKED = -1e30

SEQS = 64
MODEL = 4096
HEAD = 128
KVL = 4
GROUP = 4
HEADS = KVL * GROUP
SLOTS = 128
ROWS = SLOTS * KVL
QKV_N = (GROUP + 2) * HEAD
UP_N = 512
UP_STEPS = 7
DOWN_K = 3584
HALF_K = DOWN_K // 2
PIECE = 256
CHUNK = 8
MIB = 1024 * 1024

F32 = jnp.float32
BF16 = jnp.bfloat16
MESH = pl.DeviceIdType.MESH
VM = pl.BlockSpec(memory_space=pltpu.VMEM)
SM = pl.BlockSpec(memory_space=pltpu.SMEM)
ANY = pl.BlockSpec(memory_space=pl.ANY)


def dot(a, b):
    return jnp.dot(a, b, preferred_element_type=F32)


def place():
    sp = lax.axis_index('sp')
    return lax.axis_index('tp'), sp, sp // 2, lax.rem(sp, 2)


def enter(peers):
    barrier = pltpu.get_barrier_semaphore()
    for peer in peers:
        pl.semaphore_signal(barrier, inc=1, device_id=peer, device_id_type=MESH)
    pl.semaphore_wait(barrier, len(peers))


def remote(src, dst, send, recv, peer):
    return pltpu.make_async_remote_copy(src_ref=src, dst_ref=dst, send_sem=send, recv_sem=recv, device_id=peer, device_id_type=MESH)


def norm_into(pieces, gain, shift, out_ref):
    width = pieces[0]().shape[1]
    total = sum(jnp.sum(p(), axis=1, keepdims=True) for p in pieces)
    mean = total * (1.0 / MODEL)
    square = sum(jnp.sum(jnp.square(p() - mean), axis=1, keepdims=True) for p in pieces)
    scale = lax.rsqrt(square * (1.0 / MODEL) + NORM_EPS)
    for i, p in enumerate(pieces):
        cols = slice(i * width, (i + 1) * width)
        out_ref[:, cols] = ((p() - mean) * scale * gain(cols) + shift(cols)).astype(BF16)


def rope_tables(pos_ref, freq_ref, cos_ref, sin_ref):
    row = lax.broadcasted_iota(jnp.int32, (8, HEAD), 0)
    sign = jnp.where(lax.broadcasted_iota(jnp.int32, (8, HEAD), 1) < HEAD // 2, -1.0, 1.0)
    for first in range(0, SEQS, 8):
        pos = jnp.zeros((8, HEAD), jnp.int32)
        for i in range(8):
            pos = jnp.where(row == i, pos_ref[first + i], pos)
        angle = pos.astype(F32) * freq_ref[...]
        cos_ref[first:first + 8] = jnp.cos(angle)
        sin_ref[first:first + 8] = jnp.sin(angle) * sign


def load_qkv(layer, c, w_ref, wbuf, sem):
    loads = []
    for j in range(3):
        cols = pl.ds(pl.multiple_of(c * (2 * QKV_N) + j * UP_N, UP_N), UP_N)
        loads.append(pltpu.make_async_copy(w_ref.at[layer, :, cols], wbuf.at[j], sem.at[j]))
        loads[-1].start()
    return loads


def qkv_phase(layer, c, partner, u, wbuf, loads, bias_ref, cos_ref, sin_ref, heads, ssem, rsem):
    sent = []
    for j in range(3):
        loads[j].wait()
        cols = pl.ds(pl.multiple_of(c * (2 * QKV_N) + j * UP_N, UP_N), UP_N)
        proj = dot(u[...], wbuf[j]) + bias_ref[layer:layer + 1, cols].astype(F32)
        for n in range(4):
            local, i = divmod(4 * j + n, GROUP + 2)
            kv = 2 * c + local
            part = proj[:, n * HEAD:(n + 1) * HEAD]
            if i <= GROUP:
                part = part * cos_ref[...] + pltpu.roll(part, HEAD // 2, 1) * sin_ref[...]
            slot = kv * GROUP + i if i < GROUP else HEADS + (i - GROUP) * KVL + kv
            heads[slot] = part.astype(BF16).astype(F32)
            piece = {GROUP - 1: pl.ds(kv * GROUP, GROUP), GROUP: pl.ds(HEADS + kv, 1), GROUP + 1: pl.ds(HEADS + KVL + kv, 1)}.get(i)
            if piece is not None:
                k = len(sent)
                sent.append(remote(heads.at[piece], heads.at[piece], ssem.at[k], rsem.at[k], partner))
                sent[-1].start()
    for copy in sent:
        copy.wait()


def qkv_kernel(layer, pos_ref, freq_ref, h_ref, gain_ref, shift_ref, bias_ref, w_ref, out_ref, wbuf, u, heads, cos, sin, wsem, ssem, rsem):
    tp, sp, x, c = place()
    loads = load_qkv(layer, c, w_ref, wbuf, wsem)
    partner = {'sp': sp + 1 - 2 * c}
    norm_into(
        [lambda i=i: h_ref[:, i * 512:(i + 1) * 512].astype(F32) for i in range(8)],
        lambda cols: gain_ref[layer, 0:1, cols].astype(F32),
        lambda cols: shift_ref[layer, 0:1, cols].astype(F32),
        u,
    )
    rope_tables(pos_ref, freq_ref, cos, sin)
    enter([partner])
    qkv_phase(layer, c, partner, u, wbuf, loads, bias_ref, cos, sin, heads, ssem, rsem)
    out_ref[...] = heads[...]


HEADS_SHAPE = (HEADS + 2 * KVL, SEQS, HEAD)


def project(layer, positions, freq, h, gain, shift, bias, w):
    return pl.pallas_call(
        functools.partial(qkv_kernel, layer),
        out_shape=jax.ShapeDtypeStruct(HEADS_SHAPE, F32),
        in_specs=[SM] + [VM] * 5 + [ANY],
        out_specs=VM,
        scratch_shapes=[
            pltpu.VMEM((3, MODEL, UP_N), BF16),
            pltpu.VMEM((SEQS, MODEL), BF16),
            pltpu.VMEM(HEADS_SHAPE, F32),
            pltpu.VMEM((SEQS, HEAD), F32),
            pltpu.VMEM((SEQS, HEAD), F32),
            pltpu.SemaphoreType.DMA((3,)),
            pltpu.SemaphoreType.DMA((6,)),
            pltpu.SemaphoreType.DMA((6,)),
        ],
        compiler_params=pltpu.CompilerParams(collective_id=layer, has_side_effects=True, vmem_limit_bytes=63 * MIB),
        name=f'qkv_{layer}',
    )(positions, freq, h, gain, shift, bias, w)


def attend_kernel(layer, sparse, pos_ref, heads_ref, kc_ref, vc_ref, *rest):
    if layer:
        rest = rest[2:]
    ko_ref, vo_ref, o_ref, ml_ref, kb, vb, mref, lref, slot_of, keep_of, lsem, ssem = rest
    tp, sp, x, c = place()
    steps = SEQS // CHUNK

    def load(i, n):
        src, buf = ((kc_ref, kb), (vc_ref, vb))[n]
        rows = pl.ds(i * CHUNK, CHUNK)
        return pltpu.make_async_copy(src.at[layer, rows], buf.at[rows], lsem.at[n, i])

    def save(i, n):
        dst, buf = ((ko_ref, kb), (vo_ref, vb))[n]
        rows = pl.ds(i * CHUNK, CHUNK)
        return pltpu.make_async_copy(buf.at[rows], dst.at[layer, rows], ssem.at[n, i])

    for i in range(steps):
        for n in range(2):
            load(i, n).start()
    row = lax.broadcasted_iota(jnp.int32, (HEADS, ROWS), 0)
    col = lax.broadcasted_iota(jnp.int32, (HEADS, ROWS), 1)
    slot = sp * SLOTS + col // KVL
    slot_of[...] = jnp.where(lax.rem(col, KVL) == row // GROUP, slot, jnp.int32(1 << 30))
    if sparse:
        block = slot // BLOCK_SIZE
        vertical = lax.rem(block + tp * HEADS + row + 1, VERT_STRIDE) == 0
        keep_of[...] = jnp.where(vertical, jnp.int32(1 << 20), block)
    mref[...] = jnp.zeros_like(mref)
    lref[...] = jnp.ones_like(lref)
    lane = lax.broadcasted_iota(jnp.int32, (HEADS, HEAD), 1)
    row16 = lax.broadcasted_iota(jnp.int32, (4 * KVL, HEAD), 0)

    def body(i, _):
        for n in range(2):
            load(i, n).wait()
        for s in range(CHUNK):
            b = i * CHUNK + s
            t = pos_ref[b] - sp * SLOTS
            inside = jnp.logical_and(t >= 0, t < SLOTS)
            t = jnp.clip(t, 0, SLOTS - 1)
            base = pl.multiple_of((t // 4) * (4 * KVL), 4 * KVL)
            hit = jnp.logical_and(row16 // KVL == lax.rem(t, 4), inside)
            new = heads_ref[pl.ds(HEADS * SEQS + b, 2 * KVL, stride=SEQS), :]
            for buf, part in ((kb, new[:KVL]), (vb, new[KVL:])):
                tile = buf[b, pl.ds(base, 4 * KVL), :].astype(F32)
                buf[b, pl.ds(base, 4 * KVL), :] = jnp.where(hit, jnp.concatenate([part] * 4, axis=0), tile).astype(BF16)
        for n in range(2):
            save(i, n).start()
        for first in range(0, CHUNK, 4):
            ids = [i * CHUNK + first + s for s in range(4)]
            keeps, scores = [], []
            for b in ids:
                q = heads_ref[pl.ds(b, HEADS, stride=SEQS), :].astype(BF16)
                raw = lax.dot_general(q, kb[b], (((1,), (1,)), ((), ())), preferred_element_type=F32)
                pos = pos_ref[b]
                keep = slot_of[...] <= pos
                if sparse:
                    keep = jnp.logical_and(keep, pos // BLOCK_SIZE - keep_of[...] < LOCAL_BLOCKS)
                keeps.append(keep)
                scores.append(jnp.where(keep, raw * (1.0 / HEAD), MASKED))
            weights = []
            for b, keep, score in zip(ids, keeps, scores):
                peak = jnp.max(score, axis=1, keepdims=True)
                weight = jnp.where(keep, jnp.exp(score - peak), 0.0)
                weights.append(weight.astype(BF16))
                mref[...] = jnp.where(lane == b, peak, mref[...])
                lref[...] = jnp.where(lane == b, jnp.sum(weight, axis=1, keepdims=True), lref[...])
            for b, weight in zip(ids, weights):
                o_ref[pl.ds(b, HEADS, stride=SEQS), :] = dot(weight, vb[b])
        return 0

    lax.fori_loop(0, steps, body, 0)
    for kv in range(KVL):
        ml_ref[kv, 0:GROUP] = mref[kv * GROUP:(kv + 1) * GROUP]
        ml_ref[kv, GROUP:2 * GROUP] = lref[kv * GROUP:(kv + 1) * GROUP]
    for i in range(steps):
        for n in range(2):
            save(i, n).wait()


def attend(layer, positions, heads, kc, vc, *done):
    cache = jax.ShapeDtypeStruct(kc.shape, BF16)
    return pl.pallas_call(
        functools.partial(attend_kernel, layer, layer == 0),
        out_shape=(cache, cache, jax.ShapeDtypeStruct((HEADS * SEQS, HEAD), F32), jax.ShapeDtypeStruct((KVL, 2 * GROUP, HEAD), F32)),
        in_specs=[SM, VM, ANY, ANY] + [ANY] * len(done),
        out_specs=(ANY, ANY, VM, VM),
        scratch_shapes=[
            pltpu.VMEM((SEQS, ROWS, HEAD), BF16),
            pltpu.VMEM((SEQS, ROWS, HEAD), BF16),
            pltpu.VMEM((HEADS, HEAD), F32),
            pltpu.VMEM((HEADS, HEAD), F32),
            pltpu.VMEM((HEADS, ROWS), jnp.int32),
            pltpu.VMEM((HEADS, ROWS), jnp.int32),
            pltpu.SemaphoreType.DMA((2, SEQS // CHUNK)),
            pltpu.SemaphoreType.DMA((2, SEQS // CHUNK)),
        ],
        input_output_aliases={4: 0, 5: 1} if done else {},
        compiler_params=pltpu.CompilerParams(vmem_limit_bytes=63 * MIB),
        name=f'attend_{layer}',
    )(positions, heads, kc, vc, *done)


def mlp_kernel(layer, last, o_ref, ml_ref, h_ref, gain_ref, shift_ref, bd_ref, bu_ref, bn_ref, wd_ref, wu_ref, wn_ref, *rest):
    if not last:
        pos_ref, freq_ref, bq_ref, wq_ref, out_ref, heads_out = rest[:6]
        heads, cos, sin, q_s, q_r = rest[-5:]
        rest = rest[6:-5]
    else:
        out_ref, rest = rest[0], rest[1:]
    (
        wd, wu, wn, mls, mlx, fromcore, tosend, kept, fromx, mine, other, ob, part, ra, rb, xs, u, mf, mp, mb, ps,
        wsem, o_s, o_r, m_s, m_r, c_s, c_r,
    ) = rest
    tp, sp, x, c = place()
    y = tp
    core_peer = {'sp': sp + 1 - 2 * c}
    x_peer = {'sp': lax.rem(sp + 2, 4)}
    y_peer = {'tp': 1 - tp}
    quarter = [2 * (1 - x) + 1 - y, 2 * (1 - x) + y, 2 * x + 1 - y, 2 * x + y]

    def cols_of(k):
        return pl.ds(pl.multiple_of(c * 2048 + quarter[k] * 512, 512), 512)

    def load_dense(k):
        return pltpu.make_async_copy(wd_ref.at[layer, pl.ds(pl.multiple_of(x * 1024, 1024), 1024), cols_of(k)], wd.at[k], wsem.at[k])

    def load_up(j):
        cols = pl.ds(pl.multiple_of(x * 7168 + c * 3584 + j * UP_N, UP_N), UP_N)
        return pltpu.make_async_copy(wu_ref.at[layer, :, cols], wu.at[j], wsem.at[4 + j])

    def load_down(k):
        return pltpu.make_async_copy(wn_ref.at[layer, pl.ds(pl.multiple_of(x * DOWN_K, DOWN_K), DOWN_K), cols_of(k)], wn.at[k], wsem.at[4 + UP_STEPS + k])

    for k in range(4):
        load_dense(k).start()
    for j in range(UP_STEPS):
        load_up(j).start()
    for k in range(4):
        load_down(k).start()
    enter([core_peer, x_peer, y_peer])
    waits = []

    def send(*args):
        copy = remote(*args)
        copy.start()
        waits.append(copy)
        return copy

    stats = send(ml_ref, mls, o_s.at[4], o_r.at[4], core_peer)
    slabs = [None, None]
    for n, xd in enumerate((1 - x, x)):
        src = o_ref.at[pl.ds((2 * xd + 1 - c) * GROUP, GROUP)]
        slabs[n] = send(src, fromcore.at[n], o_s.at[n], o_r.at[n], core_peer)

    def columns(rows):
        return jnp.concatenate(rows + [jnp.zeros((HEAD - GROUP * len(rows), HEAD), F32)], axis=0).T[:SEQS]

    def merge(one, two):
        top = jnp.maximum(one[:GROUP], two[:GROUP])
        first, second = jnp.exp(one[:GROUP] - top), jnp.exp(two[:GROUP] - top)
        return first, second, top, first * one[GROUP:] + second * two[GROUP:]

    stats.wait_recv()
    rows = []
    for n, xd in enumerate((1 - x, x)):
        first, second, top, total = merge(ml_ref[2 * xd + c], mls[2 * xd + c])
        rows += [first, second]
        mlx[n] = jnp.concatenate([top, total], axis=0)
    cross_ml = send(mlx.at[0], mlx.at[2], o_s.at[5], o_r.at[5], x_peer)
    scale = columns(rows)
    for n, (xd, out) in enumerate(((1 - x, tosend), (x, kept))):
        slabs[n].wait_recv()
        kv = 2 * xd + c
        for g in range(GROUP):
            i = 2 * n * GROUP + g
            out[g] = o_ref[kv * GROUP + g] * scale[:, i:i + 1] + fromcore[n, g] * scale[:, i + GROUP:i + GROUP + 1]
        if n == 0:
            cross = send(tosend, fromx, o_s.at[2], o_r.at[2], x_peer)
    cross_ml.wait_recv()
    first, second, _, total = merge(mlx[1], mlx[2])
    scale = columns([first / total, second / total])
    cross.wait_recv()
    for g in range(GROUP):
        val = (kept[g] * scale[:, g:g + 1] + fromx[g] * scale[:, g + GROUP:g + GROUP + 1]).astype(BF16)
        mine[g] = val.astype(F32)
        ob[:, pl.ds(pl.multiple_of(c * 512 + g * HEAD, HEAD), HEAD)] = val
    share = send(mine, other, o_s.at[3], o_r.at[3], core_peer)
    share.wait_recv()
    for g in range(GROUP):
        ob[:, pl.ds(pl.multiple_of((1 - c) * 512 + g * HEAD, HEAD), HEAD)] = other[g].astype(BF16)

    own = (c * 4 + quarter[3]) * 2

    def all_reduce(ph, chunk, residual, bias_ref):
        def post(i, src, dst, peer):
            return send(src, dst, c_s.at[ph, i], c_r.at[ph, i], peer)

        def keep(k):
            val = chunk(k)
            part[ph, k, 0] = val[:, :PIECE]
            part[ph, k, 1] = val[:, PIECE:]

        keep(0)
        a0 = post(0, part.at[ph, 0, 0], ra.at[ph, 0], x_peer)
        b0 = post(1, part.at[ph, 0, 1], rb.at[ph, 0], y_peer)
        keep(1)
        a1 = post(2, part.at[ph, 1, 0], ra.at[ph, 1], x_peer)
        keep(2)
        b1 = post(3, part.at[ph, 2, 1], rb.at[ph, 1], y_peer)
        keep(3)
        b0.wait_recv()
        part[ph, 1, 1] = part[ph, 1, 1] + rb[ph, 0]
        b2 = post(4, part.at[ph, 1, 1], rb.at[ph, 2], x_peer)
        a0.wait_recv()
        part[ph, 2, 0] = part[ph, 2, 0] + ra[ph, 0]
        a2 = post(5, part.at[ph, 2, 0], ra.at[ph, 2], y_peer)
        for half, (first, second, landed) in enumerate(((a1, a2, ra), (b1, b2, rb))):
            first.wait_recv()
            second.wait_recv()
            cols = pl.ds(pl.multiple_of((own + half) * PIECE, PIECE), PIECE)
            full = part[ph, 3, half] + landed[ph, 1] + landed[ph, 2]
            xs[ph, own + half] = (residual(half, cols) + full + bias_ref[layer:layer + 1, cols].astype(F32)).astype(BF16).astype(F32)
        gather = {}
        for n in range(3):
            for half in range(2):
                peer = core_peer if n == 2 else (x_peer, y_peer)[(n + half) % 2]
                mine_ref = xs.at[ph, own + half]
                gather[half, n] = post(6 + 3 * half + n, mine_ref, mine_ref, peer)
        base = c * 8
        from_x = base + quarter[1] * 2
        from_y = base + quarter[2] * 2
        far = base + quarter[0] * 2

        def forward(i, piece, peer):
            ref = xs.at[ph, piece]
            return post(i, ref, ref, peer)

        gather[0, 0].wait_recv()
        far_a = forward(12, from_x, y_peer)
        arrived = [forward(14, from_x, core_peer)]
        gather[1, 0].wait_recv()
        far_b = forward(13, from_y + 1, x_peer)
        arrived.append(forward(15, from_y + 1, core_peer))
        gather[0, 1].wait_recv()
        arrived.append(forward(16, from_y, core_peer))
        gather[1, 1].wait_recv()
        arrived.append(forward(17, from_x + 1, core_peer))
        far_a.wait_recv()
        arrived.append(forward(18, far, core_peer))
        far_b.wait_recv()
        arrived.append(forward(19, far + 1, core_peer))
        for copy in arrived + [gather[0, 2], gather[1, 2]]:
            copy.wait_recv()

    def dense_chunk(k):
        load_dense(k).wait()
        return dot(ob[...], wd[k])

    all_reduce(0, dense_chunk, lambda half, cols: h_ref[:, cols].astype(F32), bd_ref)
    norm_into(
        [lambda i=i: xs[0, i] for i in range(16)],
        lambda cols: gain_ref[layer, 1:2, cols].astype(F32),
        lambda cols: shift_ref[layer, 1:2, cols].astype(F32),
        u,
    )
    take = (lax.broadcasted_iota(jnp.int32, (2 * HEAD, HEAD), 0) == 2 * lax.broadcasted_iota(jnp.int32, (2 * HEAD, HEAD), 1)).astype(BF16)
    even = lax.rem(lax.broadcasted_iota(jnp.int32, (SEQS, UP_N), 1), 2) == 0

    def share_m(j):
        return remote(mf.at[j], mp.at[j], m_s.at[j], m_r.at[j], core_peer)

    def up_step(j, _):
        load_up(j).wait()
        cols = pl.ds(pl.multiple_of(x * 7168 + c * 3584 + j * UP_N, UP_N), UP_N)
        val = dot(u[...], wu[j]) + bu_ref[layer:layer + 1, cols].astype(F32)
        gate = jnp.minimum(val, GELU_LIMIT)
        gate = gate * (1.0 / (1.0 + jnp.exp(-1.702 * gate)))
        linear = jnp.clip(val, -GELU_LIMIT, GELU_LIMIT) + 1.0
        mixed = jnp.where(even, gate * pltpu.roll(linear, UP_N - 1, 1), 0.0).astype(BF16)
        packed = jnp.concatenate([dot(mixed[:, i:i + 2 * HEAD], take) for i in range(0, UP_N, 2 * HEAD)], axis=1)
        mf[j] = packed
        share_m(j).start()
        mb[:, pl.ds(pl.multiple_of(c * HALF_K + j * 256, 256), 256)] = packed.astype(BF16)
        return 0

    lax.fori_loop(0, UP_STEPS, up_step, 0)
    if not last:
        loads = load_qkv(layer + 1, c, wq_ref, wu, wsem)
        rope_tables(pos_ref, freq_ref, cos, sin)
    own_k = pl.ds(pl.multiple_of(c * HALF_K, HALF_K), HALF_K)
    other_k = pl.ds(pl.multiple_of((1 - c) * HALF_K, HALF_K), HALF_K)
    for k in range(4):
        load_down(k).wait()
        ps[k] = dot(mb[:, own_k], wn[k, own_k])
    for j in range(UP_STEPS):
        share_m(j).wait()
        mb[:, pl.ds(pl.multiple_of((1 - c) * HALF_K + j * 256, 256), 256)] = mp[j].astype(BF16)

    def down_chunk(k):
        return ps[k] + dot(mb[:, other_k], wn[k, other_k])

    all_reduce(1, down_chunk, lambda half, cols: xs[0, own + half], bn_ref)
    for i in range(16):
        out_ref[:, i * PIECE:(i + 1) * PIECE] = xs[1, i].astype(BF16)
    if not last:
        norm_into(
            [lambda i=i: xs[1, i] for i in range(16)],
            lambda cols: gain_ref[layer + 1, 0:1, cols].astype(F32),
            lambda cols: shift_ref[layer + 1, 0:1, cols].astype(F32),
            u,
        )
        qkv_phase(layer + 1, c, core_peer, u, wu, loads, bq_ref, cos, sin, heads, q_s, q_r)
        heads_out[...] = heads[...]
    for copy in waits:
        copy.wait_send()


def finish(layer, o, ml, h, gain, shift, bd, bu, bn, wd, wu, wn, *following):
    slab = pltpu.VMEM((GROUP, SEQS, HEAD), F32)
    dma = pltpu.SemaphoreType.DMA
    last = not following
    hidden = jax.ShapeDtypeStruct((SEQS, MODEL), BF16)
    table = pltpu.VMEM((SEQS, HEAD), F32)
    return pl.pallas_call(
        functools.partial(mlp_kernel, layer, last),
        out_shape=hidden if last else (hidden, jax.ShapeDtypeStruct(HEADS_SHAPE, F32)),
        in_specs=[VM] * 8 + [ANY] * 3 + ([] if last else [SM, VM, VM, ANY]),
        out_specs=VM if last else (VM, VM),
        scratch_shapes=[
            pltpu.VMEM((4, 1024, 512), BF16),
            pltpu.VMEM((UP_STEPS, MODEL, UP_N), BF16),
            pltpu.VMEM((4, DOWN_K, 512), BF16),
            pltpu.VMEM((KVL, 2 * GROUP, HEAD), F32),
            pltpu.VMEM((3, 2 * GROUP, HEAD), F32),
            pltpu.VMEM((2, GROUP, SEQS, HEAD), F32),
            slab, slab, slab, slab, slab,
            pltpu.VMEM((SEQS, 1024), BF16),
            pltpu.VMEM((2, 4, 2, SEQS, PIECE), F32),
            pltpu.VMEM((2, 3, SEQS, PIECE), F32),
            pltpu.VMEM((2, 3, SEQS, PIECE), F32),
            pltpu.VMEM((2, 16, SEQS, PIECE), F32),
            pltpu.VMEM((SEQS, MODEL), BF16),
            pltpu.VMEM((UP_STEPS, SEQS, 256), F32),
            pltpu.VMEM((UP_STEPS, SEQS, 256), F32),
            pltpu.VMEM((SEQS, DOWN_K), BF16),
            pltpu.VMEM((4, SEQS, 512), F32),
            dma((8 + UP_STEPS,)), dma((6,)), dma((6,)), dma((UP_STEPS,)), dma((UP_STEPS,)), dma((2, 20)), dma((2, 20)),
        ] + ([] if last else [pltpu.VMEM(HEADS_SHAPE, F32), table, table, dma((6,)), dma((6,))]),
        compiler_params=pltpu.CompilerParams(collective_id=2 + layer, has_side_effects=True, vmem_limit_bytes=63 * MIB),
        name=f'mlp_{layer}',
    )(o, ml, h, gain, shift, bd, bu, bn, wd, wu, wn, *following)


def solution(mesh):
    cache_spec = P(None, 'dp', 'sp', 'tp', None)
    in_specs = (P('dp', None), P('dp'), cache_spec, cache_spec, P(), P(), P(None, None, 'tp'), P(None, 'tp'), P(None, 'tp', None), P(), P(None, None, 'tp'), P(None, 'tp'), P(None, 'tp', None), P())
    out_specs = (P('dp', None), cache_spec, cache_spec)

    def device_step(hidden, positions, k_cache, v_cache, ln_gain, ln_bias, w_qkv, b_qkv, w_dense, b_dense, w_up, b_up, w_down, b_down):
        freq = ROPE_THETA ** (-np.arange(HEAD // 2) * (2.0 / HEAD))
        freq = jnp.asarray(np.tile(freq, 2)[None].astype(np.float32))
        shape = k_cache.shape
        flat = (2, SEQS, ROWS, HEAD)
        kc = k_cache.reshape(flat)
        vc = v_cache.reshape(flat)
        done = ()
        heads = project(0, positions, freq, hidden, ln_gain, ln_bias, b_qkv, w_qkv)
        for layer in range(2):
            ko, vo, o, ml = attend(layer, positions, heads.reshape(-1, HEAD), kc, vc, *done)
            done = (ko, vo)
            following = () if layer else (positions, freq, b_qkv, w_qkv)
            out = finish(layer, o.reshape(HEADS, SEQS, HEAD), ml, hidden, ln_gain, ln_bias, b_dense, b_up, b_down, w_dense, w_up, w_down, *following)
            hidden, heads = out if following else (out, None)
        return hidden, done[0].reshape(shape), done[1].reshape(shape)

    return jax.shard_map(device_step, mesh=mesh, in_specs=in_specs, out_specs=out_specs, check_vma=False)
```

```python
import functools

import jax
import jax.numpy as jnp
import numpy as np
from jax import lax
from jax.experimental import pallas as pl
from jax.experimental.pallas import tpu as pltpu
from jax.sharding import PartitionSpec as P

BLOCK_SIZE = 64
LOCAL_BLOCKS = 16
VERT_STRIDE = 8
ROPE_THETA = 1000000.0
GELU_LIMIT = 20.0
NORM_EPS = 0.00001
MASKED = -1e30

SEQS = 64
MODEL = 4096
HEAD = 128
KVL = 4
GROUP = 4
HEADS = KVL * GROUP
SLOTS = 128
ROWS = SLOTS * KVL
QKV_N = (GROUP + 2) * HEAD
UP_N = 512
UP_STEPS = 7
DOWN_K = 3584
HALF_K = DOWN_K // 2
PIECE = 256
CHUNK = 8
MIB = 1024 * 1024
QKV_MIB = 20
ATTEND_MIB = 8
MLP_MIB = 40

F32 = jnp.float32
BF16 = jnp.bfloat16
MESH = pl.DeviceIdType.MESH
VM = pl.BlockSpec(memory_space=pltpu.VMEM)
SM = pl.BlockSpec(memory_space=pltpu.SMEM)
HBM = pl.BlockSpec(memory_space=pltpu.HBM)


def kept(shape, dtype):
    return pltpu.VMEM(shape, dtype)


def pin(x):
    return pltpu.with_memory_space_constraint(x, pltpu.HBM)


def near(x):
    return pltpu.with_memory_space_constraint(x, pltpu.VMEM)


def dot(a, b):
    return jnp.dot(a, b, preferred_element_type=F32)


def place():
    sp = lax.axis_index('sp')
    return lax.axis_index('tp'), sp, sp // 2, lax.rem(sp, 2)


def enter(peers):
    barrier = pltpu.get_barrier_semaphore()
    for peer in peers:
        pl.semaphore_signal(barrier, inc=1, device_id=peer, device_id_type=MESH)
    pl.semaphore_wait(barrier, len(peers))


def remote(src, dst, send, recv, peer):
    return pltpu.make_async_remote_copy(src_ref=src, dst_ref=dst, send_sem=send, recv_sem=recv, device_id=peer, device_id_type=MESH)


def norm_into(pieces, gain, shift, out_ref):
    width = pieces[0]().shape[1]
    total = sum(jnp.sum(p(), axis=1, keepdims=True) for p in pieces)
    mean = total * (1.0 / MODEL)
    square = sum(jnp.sum(jnp.square(p() - mean), axis=1, keepdims=True) for p in pieces)
    scale = lax.rsqrt(square * (1.0 / MODEL) + NORM_EPS)
    for i, p in enumerate(pieces):
        cols = slice(i * width, (i + 1) * width)
        out_ref[:, cols] = ((p() - mean) * scale * gain(cols) + shift(cols)).astype(BF16)


def rope_tables(pos_ref, freq_ref, cos_ref, sin_ref):
    row = lax.broadcasted_iota(jnp.int32, (8, HEAD), 0)
    sign = jnp.where(lax.broadcasted_iota(jnp.int32, (8, HEAD), 1) < HEAD // 2, -1.0, 1.0)
    for first in range(0, SEQS, 8):
        pos = jnp.zeros((8, HEAD), jnp.int32)
        for i in range(8):
            pos = jnp.where(row == i, pos_ref[first + i], pos)
        angle = pos.astype(F32) * freq_ref[...]
        cos_ref[first:first + 8] = jnp.cos(angle)
        sin_ref[first:first + 8] = jnp.sin(angle) * sign


def load_qkv(layer, c, w_ref, wbuf, sem, j):
    cols = pl.ds(pl.multiple_of(c * (2 * QKV_N) + j * UP_N, UP_N), UP_N)
    return pltpu.make_async_copy(w_ref.at[layer, :, cols], wbuf.at[j], sem.at[j])


def qkv_phase(layer, c, partner, u, wbuf, loads, bias_ref, cos_ref, sin_ref, heads, ssem, rsem):
    sent = []
    for j in range(3):
        loads[j].wait()
        cols = pl.ds(pl.multiple_of(c * (2 * QKV_N) + j * UP_N, UP_N), UP_N)
        proj = dot(u[...], wbuf[j]) + bias_ref[layer:layer + 1, cols].astype(F32)
        for n in range(4):
            local, i = divmod(4 * j + n, GROUP + 2)
            kv = 2 * c + local
            part = proj[:, n * HEAD:(n + 1) * HEAD]
            if i <= GROUP:
                part = part * cos_ref[...] + pltpu.roll(part, HEAD // 2, 1) * sin_ref[...]
            slot = kv * GROUP + i if i < GROUP else HEADS + (i - GROUP) * KVL + kv
            heads[slot] = part.astype(BF16).astype(F32)
            piece = {GROUP - 1: pl.ds(kv * GROUP, GROUP), GROUP: pl.ds(HEADS + kv, 1), GROUP + 1: pl.ds(HEADS + KVL + kv, 1)}.get(i)
            if piece is not None:
                k = len(sent)
                sent.append(remote(heads.at[piece], heads.at[piece], ssem.at[k], rsem.at[k], partner))
                sent[-1].start()
    for copy in sent:
        copy.wait()


def copy_in(pairs, sems):
    copies = [pltpu.make_async_copy(src, dst, sems.at[i]) for i, (src, dst) in enumerate(pairs)]
    for copy in copies:
        copy.start()
    return copies


def cache_copies(layer, kc_ref, vc_ref, k_out, v_out, sems):
    return [pltpu.make_async_copy(src.at[layer], dst, sems.at[n]) for n, (src, dst) in enumerate(((kc_ref, k_out), (vc_ref, v_out)))]


def qkv_kernel(
    layer, pos_hbm, freq_hbm, h_hbm, gain_hbm, shift_hbm, bias_hbm, w_ref, kc_ref, vc_ref, out_ref, k_out, v_out,
    wbuf, u, heads, cos, sin, pos, freq, h, gain, shift, bias, isem, wsem, ksem, ssem, rsem,
):
    tp, sp, x, c = place()
    small = copy_in([(h_hbm, h), (gain_hbm, gain), (shift_hbm, shift), (pos_hbm, pos), (freq_hbm, freq), (bias_hbm, bias)], isem)
    loads = [load_qkv(layer, c, w_ref, wbuf, wsem, j) for j in range(3)]
    partner = {'sp': sp + 1 - 2 * c}
    for copy in small:
        copy.wait()

    def begin(j, _):
        load_qkv(layer, c, w_ref, wbuf, wsem, j).start()
        return 0

    lax.fori_loop(0, 3, begin, 0)
    for copy in cache_copies(layer, kc_ref, vc_ref, k_out, v_out, ksem):
        copy.start()
    norm_into(
        [lambda i=i: h[:, i * 512:(i + 1) * 512].astype(F32) for i in range(8)],
        lambda cols: gain[layer, 0:1, cols].astype(F32),
        lambda cols: shift[layer, 0:1, cols].astype(F32),
        u,
    )
    rope_tables(pos, freq, cos, sin)
    enter([partner])
    qkv_phase(layer, c, partner, u, wbuf, loads, bias, cos, sin, heads, ssem, rsem)
    out_ref[...] = heads[...]
    for copy in cache_copies(layer, kc_ref, vc_ref, k_out, v_out, ksem):
        copy.wait()


HEADS_SHAPE = (HEADS + 2 * KVL, SEQS, HEAD)


CACHE = kept((SEQS, ROWS, HEAD), BF16)


def project(layer, positions, freq, h, gain, shift, bias, w, kc, vc):
    dma = pltpu.SemaphoreType.DMA
    return pl.pallas_call(
        functools.partial(qkv_kernel, layer),
        out_shape=(kept(HEADS_SHAPE, F32), CACHE, CACHE),
        in_specs=[HBM] * 9,
        out_specs=(VM, VM, VM),
        scratch_shapes=[
            pltpu.VMEM((3, MODEL, UP_N), BF16),
            pltpu.VMEM((SEQS, MODEL), BF16),
            pltpu.VMEM(HEADS_SHAPE, F32),
            pltpu.VMEM((SEQS, HEAD), F32),
            pltpu.VMEM((SEQS, HEAD), F32),
            pltpu.SMEM((SEQS,), jnp.int32),
            pltpu.VMEM((1, HEAD), F32),
            pltpu.VMEM((SEQS, MODEL), BF16),
            pltpu.VMEM(gain.shape, BF16),
            pltpu.VMEM(shift.shape, BF16),
            pltpu.VMEM(bias.shape, BF16),
            dma((6,)), dma((3,)), dma((2,)), dma((6,)), dma((6,)),
        ],
        compiler_params=pltpu.CompilerParams(collective_id=layer, has_side_effects=True, vmem_limit_bytes=QKV_MIB * MIB),
        name=f'qkv_{layer}',
    )(*map(pin, (positions, freq, h, gain, shift, bias, w, kc, vc)))


def attend_kernel(layer, sparse, pos_hbm, heads_ref, kb, vb, *rest):
    if layer:
        rest = rest[2:]
    ko_ref, vo_ref, o_ref, ml_ref, pos_ref, mref, lref, slot_of, keep_of, tiles, psem, ssem, tsem = rest
    tp, sp, x, c = place()
    steps = SEQS // CHUNK
    copy_in([(pos_hbm, pos_ref)], psem)

    def save(i, n):
        dst, buf = ((ko_ref, kb), (vo_ref, vb))[n]
        rows = pl.ds(i * CHUNK, CHUNK)
        return pltpu.make_async_copy(buf.at[rows], dst.at[layer, rows], ssem.at[n, i])

    def place_of(b):
        t = pos_ref[b] - sp * SLOTS
        inside = jnp.logical_and(t >= 0, t < SLOTS)
        t = jnp.clip(t, 0, SLOTS - 1)
        return t, inside, pl.multiple_of((t // 4) * (4 * KVL), 4 * KVL)

    def patch(b, n):
        base = place_of(b)[2]
        return pltpu.make_async_copy(tiles.at[n, b], (ko_ref, vo_ref)[n].at[layer, b, pl.ds(base, 4 * KVL)], tsem.at[n])

    for i in range(steps):
        for n in range(2):
            save(i, n).start()
    row = lax.broadcasted_iota(jnp.int32, (HEADS, ROWS), 0)
    col = lax.broadcasted_iota(jnp.int32, (HEADS, ROWS), 1)
    slot = sp * SLOTS + col // KVL
    slot_of[...] = jnp.where(lax.rem(col, KVL) == row // GROUP, slot, jnp.int32(1 << 30))
    if sparse:
        block = slot // BLOCK_SIZE
        vertical = lax.rem(block + tp * HEADS + row + 1, VERT_STRIDE) == 0
        keep_of[...] = jnp.where(vertical, jnp.int32(1 << 20), block)
    mref[...] = jnp.zeros_like(mref)
    lref[...] = jnp.ones_like(lref)
    lane = lax.broadcasted_iota(jnp.int32, (HEADS, HEAD), 1)
    row16 = lax.broadcasted_iota(jnp.int32, (4 * KVL, HEAD), 0)
    copy_of_pos = pltpu.make_async_copy(pos_hbm, pos_ref, psem.at[0])
    copy_of_pos.wait()

    def repeat(part):
        return jnp.concatenate([jnp.broadcast_to(part[kv:kv + 1], (GROUP, HEAD)) for kv in range(KVL)], axis=0)

    def body(i, _):
        for first in range(0, CHUNK, 4):
            ids = [i * CHUNK + first + s for s in range(4)]
            keeps, hits, scores, news = [], [], [], []
            for b in ids:
                q = heads_ref[pl.ds(b, HEADS, stride=SEQS), :]
                new = heads_ref[pl.ds(HEADS * SEQS + b, 2 * KVL, stride=SEQS), :]
                raw = lax.dot_general(q.astype(BF16), kb[b], (((1,), (1,)), ((), ())), preferred_element_type=F32)
                pos = pos_ref[b]
                keep = slot_of[...] <= pos
                hit = slot_of[...] == pos
                if sparse:
                    keep = jnp.logical_and(keep, pos // BLOCK_SIZE - keep_of[...] < LOCAL_BLOCKS)
                raw = jnp.where(hit, jnp.sum(q * repeat(new[:KVL]), axis=1, keepdims=True), raw)
                keeps.append(keep)
                hits.append(hit)
                news.append(new)
                scores.append(jnp.where(keep, raw * (1.0 / HEAD), MASKED))
            weights, added = [], []
            for b, keep, hit, score in zip(ids, keeps, hits, scores):
                peak = jnp.max(score, axis=1, keepdims=True)
                weight = jnp.where(keep, jnp.exp(score - peak), 0.0)
                mref[...] = jnp.where(lane == b, peak, mref[...])
                lref[...] = jnp.where(lane == b, jnp.sum(weight, axis=1, keepdims=True), lref[...])
                weight = weight.astype(BF16).astype(F32)
                added.append(jnp.sum(jnp.where(hit, weight, 0.0), axis=1, keepdims=True))
                weights.append(jnp.where(hit, 0.0, weight).astype(BF16))
            for b, weight, extra, new in zip(ids, weights, added, news):
                o_ref[pl.ds(b, HEADS, stride=SEQS), :] = dot(weight, vb[b]) + extra * repeat(new[KVL:])
            for b, new in zip(ids, news):
                t, inside, base = place_of(b)
                hit = jnp.logical_and(row16 // KVL == lax.rem(t, 4), inside)
                for n, buf in enumerate((kb, vb)):
                    fresh = jnp.concatenate([new[n * KVL:(n + 1) * KVL]] * 4, axis=0)
                    tiles[n, b] = jnp.where(hit, fresh, buf[b, pl.ds(base, 4 * KVL), :].astype(F32)).astype(BF16)
        for n in range(2):
            save(i, n).wait()
        for s in range(CHUNK):
            for n in range(2):
                patch(i * CHUNK + s, n).start()
        return 0

    lax.fori_loop(0, steps, body, 0)
    for kv in range(KVL):
        ml_ref[kv, 0:GROUP] = mref[kv * GROUP:(kv + 1) * GROUP]
        ml_ref[kv, GROUP:2 * GROUP] = lref[kv * GROUP:(kv + 1) * GROUP]

    for n in range(2):
        pltpu.make_async_copy(tiles.at[n], (ko_ref, vo_ref)[n].at[layer, :, pl.ds(0, 4 * KVL)], tsem.at[n]).wait()


def attend(layer, positions, heads, kb, vb, shape, *done):
    cache = jax.ShapeDtypeStruct(shape, BF16)
    dma = pltpu.SemaphoreType.DMA
    return pl.pallas_call(
        functools.partial(attend_kernel, layer, layer == 0),
        out_shape=(cache, cache, kept((HEADS * SEQS, HEAD), F32), kept((KVL, 2 * GROUP, HEAD), F32)),
        in_specs=[HBM, VM, VM, VM] + [HBM] * len(done),
        out_specs=(HBM, HBM, VM, VM),
        scratch_shapes=[
            pltpu.SMEM((SEQS,), jnp.int32),
            pltpu.VMEM((HEADS, HEAD), F32),
            pltpu.VMEM((HEADS, HEAD), F32),
            pltpu.VMEM((HEADS, ROWS), jnp.int32),
            pltpu.VMEM((HEADS, ROWS), jnp.int32),
            pltpu.VMEM((2, SEQS, 4 * KVL, HEAD), BF16),
            dma((1,)), dma((2, SEQS // CHUNK)), dma((2,)),
        ],
        input_output_aliases={4: 0, 5: 1} if done else {},
        compiler_params=pltpu.CompilerParams(vmem_limit_bytes=ATTEND_MIB * MIB),
        name=f'attend_{layer}',
    )(pin(positions), *map(near, (heads, kb, vb)), *map(pin, done))


def mlp_kernel(layer, last, o_ref, ml_ref, h_ref, gain_ref, shift_ref, bd_ref, bu_ref, bn_ref, wd_ref, wu_ref, wn_ref, *rest):
    if not last:
        pos_hbm, freq_ref, bq_ref, wq_ref, kc_ref, vc_ref, out_ref, heads_out, k_out, v_out = rest[:10]
        pos_ref, heads, cos, sin, p_s, k_s, q_s, q_r = rest[-8:]
        rest = rest[10:-8]
    else:
        out_ref, rest = rest[0], rest[1:]
    (
        wu, mls, mlx, fromcore, tosend, kept, fromx, mine, other, ob, part, ra, rb, xs, u, mf, mp, mb, ps,
        wsem, o_s, o_r, m_s, m_r, c_s, c_r,
    ) = rest
    tp, sp, x, c = place()
    y = tp
    core_peer = {'sp': sp + 1 - 2 * c}
    x_peer = {'sp': lax.rem(sp + 2, 4)}
    y_peer = {'tp': 1 - tp}
    quarter = [2 * (1 - x) + 1 - y, 2 * (1 - x) + y, 2 * x + 1 - y, 2 * x + y]

    def turn(k):
        far, near = 1 - k // 2, k // 2
        return 2 * (far * (1 - x) + near * x) + (1 - k % 2) * (1 - y) + k % 2 * y

    def cols_of(k):
        return pl.ds(pl.multiple_of(c * 2048 + turn(k) * 512, 512), 512)

    def load_dense(k):
        return pltpu.make_async_copy(wd_ref.at[layer, pl.ds(pl.multiple_of(x * 1024, 1024), 1024), cols_of(k)], wu.at[UP_STEPS - 1, pl.ds(k * 1024, 1024)], wsem.at[k])

    def load_up(j):
        cols = pl.ds(pl.multiple_of(x * 7168 + c * 3584 + j * UP_N, UP_N), UP_N)
        return pltpu.make_async_copy(wu_ref.at[layer, :, cols], wu.at[j], wsem.at[4 + j])

    def load_down(k):
        rows = pl.ds(pl.multiple_of(x * DOWN_K, DOWN_K), DOWN_K)
        return pltpu.make_async_copy(wn_ref.at[layer, rows, cols_of(k)], wu.at[k, pl.ds(0, DOWN_K)], wsem.at[4 + UP_STEPS + k])

    def load_next(j):
        return load_qkv(layer + 1, c, wq_ref, wu.at[pl.ds(4, 3)], wsem, j)

    for k in range(4):
        load_dense(k).start()
    for j in range(UP_STEPS - 1):
        load_up(j).start()
    if not last:
        cache = cache_copies(layer + 1, kc_ref, vc_ref, k_out, v_out, k_s)
        for copy in cache:
            copy.start()
        copy_in([(pos_hbm, pos_ref)], p_s)[0].wait()
        rope_tables(pos_ref, freq_ref, cos, sin)
    enter([core_peer, x_peer, y_peer])
    waits = []

    def send(*args):
        copy = remote(*args)
        copy.start()
        waits.append(copy)
        return copy

    stats = send(ml_ref, mls, o_s.at[4], o_r.at[4], core_peer)
    slabs = [None, None]
    for n, xd in enumerate((1 - x, x)):
        src = o_ref.at[pl.ds((2 * xd + 1 - c) * GROUP, GROUP)]
        slabs[n] = send(src, fromcore.at[n], o_s.at[n], o_r.at[n], core_peer)

    def columns(rows):
        return jnp.concatenate(rows + [jnp.zeros((HEAD - GROUP * len(rows), HEAD), F32)], axis=0).T[:SEQS]

    def merge(one, two):
        top = jnp.maximum(one[:GROUP], two[:GROUP])
        first, second = jnp.exp(one[:GROUP] - top), jnp.exp(two[:GROUP] - top)
        return first, second, top, first * one[GROUP:] + second * two[GROUP:]

    stats.wait_recv()
    rows = []
    for n, xd in enumerate((1 - x, x)):
        first, second, top, total = merge(ml_ref[2 * xd + c], mls[2 * xd + c])
        rows += [first, second]
        mlx[n] = jnp.concatenate([top, total], axis=0)
    cross_ml = send(mlx.at[0], mlx.at[2], o_s.at[5], o_r.at[5], x_peer)
    scale = columns(rows)
    for n, (xd, out) in enumerate(((1 - x, tosend), (x, kept))):
        slabs[n].wait_recv()
        kv = 2 * xd + c
        for g in range(GROUP):
            i = 2 * n * GROUP + g
            out[g] = o_ref[kv * GROUP + g] * scale[:, i:i + 1] + fromcore[n, g] * scale[:, i + GROUP:i + GROUP + 1]
        if n == 0:
            cross = send(tosend, fromx, o_s.at[2], o_r.at[2], x_peer)
    cross_ml.wait_recv()
    first, second, _, total = merge(mlx[1], mlx[2])
    scale = columns([first / total, second / total])
    cross.wait_recv()
    for g in range(GROUP):
        val = (kept[g] * scale[:, g:g + 1] + fromx[g] * scale[:, g + GROUP:g + GROUP + 1]).astype(BF16)
        mine[g] = val.astype(F32)
        ob[:, pl.ds(pl.multiple_of(c * 512 + g * HEAD, HEAD), HEAD)] = val
    share = send(mine, other, o_s.at[3], o_r.at[3], core_peer)
    own_o = pl.ds(pl.multiple_of(c * 512, 512), 512)
    other_o = pl.ds(pl.multiple_of((1 - c) * 512, 512), 512)

    def dense_half(k, cols):
        rows = pl.ds(pl.multiple_of(k * 1024 + cols.start, 512), 512)
        return dot(ob[:, cols], wu[UP_STEPS - 1, rows])

    for k in range(4):
        load_dense(k).wait()
        ps[k] = dense_half(k, own_o)
    share.wait_recv()
    for g in range(GROUP):
        ob[:, pl.ds(pl.multiple_of((1 - c) * 512 + g * HEAD, HEAD), HEAD)] = other[g].astype(BF16)

    own = (c * 4 + quarter[3]) * 2

    def all_reduce(ph, chunk, residual, bias_ref, after=lambda: None):
        def post(i, src, dst, peer):
            copy = remote(src, dst, c_s.at[ph, int(i > 5)], c_r.at[ph, i], peer)
            copy.start()
            return copy

        def keep(k):
            val = chunk(k)
            part[ph, k, 0] = val[:, :PIECE]
            part[ph, k, 1] = val[:, PIECE:]

        keep(0)
        a0 = post(0, part.at[ph, 0, 0], ra.at[ph, 0], x_peer)
        b0 = post(1, part.at[ph, 0, 1], rb.at[ph, 0], y_peer)
        keep(1)
        a1 = post(2, part.at[ph, 1, 0], ra.at[ph, 1], x_peer)
        keep(2)
        b1 = post(3, part.at[ph, 2, 1], rb.at[ph, 1], y_peer)
        keep(3)
        after()
        b0.wait_recv()
        part[ph, 1, 1] = part[ph, 1, 1] + rb[ph, 0]
        b2 = post(4, part.at[ph, 1, 1], rb.at[ph, 2], x_peer)
        a0.wait_recv()
        part[ph, 2, 0] = part[ph, 2, 0] + ra[ph, 0]
        a2 = post(5, part.at[ph, 2, 0], ra.at[ph, 2], y_peer)
        for half, (first, second, landed) in enumerate(((a1, a2, ra), (b1, b2, rb))):
            first.wait_recv()
            second.wait_recv()
            cols = pl.ds(pl.multiple_of((own + half) * PIECE, PIECE), PIECE)
            full = part[ph, 3, half] + landed[ph, 1] + landed[ph, 2]
            xs[ph, own + half] = (residual(half, cols) + full + bias_ref[layer:layer + 1, cols].astype(F32)).astype(BF16).astype(F32)
        gather = {}
        for n in range(3):
            for half in range(2):
                peer = core_peer if n == 2 else (x_peer, y_peer)[(n + half) % 2]
                mine_ref = xs.at[ph, own + half]
                gather[half, n] = post(6 + 3 * half + n, mine_ref, mine_ref, peer)
        base = c * 8
        from_x = base + quarter[1] * 2
        from_y = base + quarter[2] * 2
        far = base + quarter[0] * 2

        def forward(i, piece, peer):
            ref = xs.at[ph, piece]
            return post(i, ref, ref, peer)

        gather[0, 0].wait_recv()
        far_a = forward(12, from_x, y_peer)
        arrived = [forward(14, from_x, core_peer)]
        gather[1, 0].wait_recv()
        far_b = forward(13, from_y + 1, x_peer)
        arrived.append(forward(15, from_y + 1, core_peer))
        gather[0, 1].wait_recv()
        arrived.append(forward(16, from_y, core_peer))
        gather[1, 1].wait_recv()
        arrived.append(forward(17, from_x + 1, core_peer))
        far_a.wait_recv()
        arrived.append(forward(18, far, core_peer))
        far_b.wait_recv()
        arrived.append(forward(19, far + 1, core_peer))
        for copy in arrived + [gather[0, 2], gather[1, 2]]:
            copy.wait_recv()

    def dense_chunk(k):
        return ps[k] + dense_half(k, other_o)

    all_reduce(0, dense_chunk, lambda half, cols: h_ref[:, cols].astype(F32), bd_ref, load_up(UP_STEPS - 1).start)
    norm_into(
        [lambda i=i: xs[0, i] for i in range(16)],
        lambda cols: gain_ref[layer, 1:2, cols].astype(F32),
        lambda cols: shift_ref[layer, 1:2, cols].astype(F32),
        u,
    )
    take = (lax.broadcasted_iota(jnp.int32, (2 * HEAD, HEAD), 0) == 2 * lax.broadcasted_iota(jnp.int32, (2 * HEAD, HEAD), 1)).astype(BF16)
    even = lax.rem(lax.broadcasted_iota(jnp.int32, (SEQS, UP_N), 1), 2) == 0

    def share_m(j):
        return remote(mf.at[j], mp.at[j], m_s.at[0], m_r.at[0], core_peer)

    def up_step(j, _):
        load_up(j).wait()
        cols = pl.ds(pl.multiple_of(x * 7168 + c * 3584 + j * UP_N, UP_N), UP_N)
        val = dot(u[...], wu[j]) + bu_ref[layer:layer + 1, cols].astype(F32)
        gate = jnp.minimum(val, GELU_LIMIT)
        gate = gate * (1.0 / (1.0 + jnp.exp(-1.702 * gate)))
        linear = jnp.clip(val, -GELU_LIMIT, GELU_LIMIT) + 1.0
        mixed = jnp.where(even, gate * pltpu.roll(linear, UP_N - 1, 1), 0.0).astype(BF16)
        packed = jnp.concatenate([dot(mixed[:, i:i + 2 * HEAD], take) for i in range(0, UP_N, 2 * HEAD)], axis=1)
        mf[j] = packed
        share_m(j).start()
        mb[:, pl.ds(pl.multiple_of(c * HALF_K + j * 256, 256), 256)] = packed.astype(BF16)

        @pl.when(j < 4)
        def _():
            load_down(j).start()

        if not last:
            @pl.when(j >= 4)
            def _():
                load_next(j - 4).start()

        return 0

    lax.fori_loop(0, UP_STEPS, up_step, 0)
    own_k = pl.ds(pl.multiple_of(c * HALF_K, HALF_K), HALF_K)
    other_k = pl.ds(pl.multiple_of((1 - c) * HALF_K, HALF_K), HALF_K)
    for k in range(4):
        load_down(k).wait()
        ps[k] = dot(mb[:, own_k], wu[k, own_k])
    remote(mf, mp, m_s.at[0], m_r.at[0], core_peer).wait()
    for j in range(UP_STEPS):
        mb[:, pl.ds(pl.multiple_of((1 - c) * HALF_K + j * 256, 256), 256)] = mp[j].astype(BF16)

    def down_chunk(k):
        return ps[k] + dot(mb[:, other_k], wu[k, other_k])

    all_reduce(1, down_chunk, lambda half, cols: xs[0, own + half], bn_ref)
    for i in range(16):
        out_ref[:, i * PIECE:(i + 1) * PIECE] = xs[1, i].astype(BF16)
    if not last:
        norm_into(
            [lambda i=i: xs[1, i] for i in range(16)],
            lambda cols: gain_ref[layer + 1, 0:1, cols].astype(F32),
            lambda cols: shift_ref[layer + 1, 0:1, cols].astype(F32),
            u,
        )
        qkv_phase(layer + 1, c, core_peer, u, wu.at[pl.ds(4, 3)], [load_next(j) for j in range(3)], bq_ref, cos, sin, heads, q_s, q_r)
        heads_out[...] = heads[...]
        for copy in cache:
            copy.wait()
    for ph in range(2):
        for n, pieces in enumerate((6, 14)):
            remote(xs.at[ph, pl.ds(0, pieces)], xs.at[ph, pl.ds(0, pieces)], c_s.at[ph, n], c_r.at[ph, 0], x_peer).wait_send()
    for copy in waits:
        copy.wait_send()


def finish(layer, o, ml, h, gain, shift, bd, bu, bn, wd, wu, wn, *following):
    slab = pltpu.VMEM((GROUP, SEQS, HEAD), F32)
    dma = pltpu.SemaphoreType.DMA
    last = not following
    hidden = kept((SEQS, MODEL), BF16)
    table = pltpu.VMEM((SEQS, HEAD), F32)
    return pl.pallas_call(
        functools.partial(mlp_kernel, layer, last),
        out_shape=hidden if last else (hidden, kept(HEADS_SHAPE, F32), CACHE, CACHE),
        in_specs=[VM] * 8 + [HBM] * 3 + ([] if last else [HBM, VM, VM, HBM, HBM, HBM]),
        out_specs=VM if last else (VM, VM, VM, VM),
        scratch_shapes=[
            pltpu.VMEM((UP_STEPS, MODEL, UP_N), BF16),
            pltpu.VMEM((KVL, 2 * GROUP, HEAD), F32),
            pltpu.VMEM((3, 2 * GROUP, HEAD), F32),
            pltpu.VMEM((2, GROUP, SEQS, HEAD), F32),
            slab, slab, slab, slab, slab,
            pltpu.VMEM((SEQS, 1024), BF16),
            pltpu.VMEM((2, 4, 2, SEQS, PIECE), F32),
            pltpu.VMEM((2, 3, SEQS, PIECE), F32),
            pltpu.VMEM((2, 3, SEQS, PIECE), F32),
            pltpu.VMEM((2, 16, SEQS, PIECE), F32),
            pltpu.VMEM((SEQS, MODEL), BF16),
            pltpu.VMEM((UP_STEPS, SEQS, 256), F32),
            pltpu.VMEM((UP_STEPS, SEQS, 256), F32),
            pltpu.VMEM((SEQS, DOWN_K), BF16),
            pltpu.VMEM((4, SEQS, 512), F32),
            dma((8 + UP_STEPS,)), dma((6,)), dma((6,)), dma((1,)), dma((1,)), dma((2, 2)), dma((2, 20)),
        ] + ([] if last else [pltpu.SMEM((SEQS,), jnp.int32), pltpu.VMEM(HEADS_SHAPE, F32), table, table, dma((1,)), dma((2,)), dma((6,)), dma((6,))]),
        compiler_params=pltpu.CompilerParams(collective_id=2 + layer, has_side_effects=True, vmem_limit_bytes=(60 if last else MLP_MIB) * MIB),
        name=f'mlp_{layer}',
    )(near(o), near(ml), near(h) if last else pin(h), *map(pin, (gain, shift, bd, bu, bn, wd, wu, wn, *following)))


def solution(mesh):
    cache_spec = P(None, 'dp', 'sp', 'tp', None)
    in_specs = (P('dp', None), P('dp'), cache_spec, cache_spec, P(), P(), P(None, None, 'tp'), P(None, 'tp'), P(None, 'tp', None), P(), P(None, None, 'tp'), P(None, 'tp'), P(None, 'tp', None), P())
    out_specs = (P('dp', None), cache_spec, cache_spec)

    def device_step(hidden, positions, k_cache, v_cache, ln_gain, ln_bias, w_qkv, b_qkv, w_dense, b_dense, w_up, b_up, w_down, b_down):
        freq = ROPE_THETA ** (-np.arange(HEAD // 2) * (2.0 / HEAD))
        freq = jnp.asarray(np.tile(freq, 2)[None].astype(np.float32))
        shape = k_cache.shape
        flat = (2, SEQS, ROWS, HEAD)
        kc = k_cache.reshape(flat)
        vc = v_cache.reshape(flat)
        done = ()
        heads, kb, vb = project(0, positions, freq, hidden, ln_gain, ln_bias, b_qkv, w_qkv, kc, vc)
        for layer in range(2):
            ko, vo, o, ml = attend(layer, positions, heads.reshape(-1, HEAD), kb, vb, flat, *done)
            done = (ko, vo)
            following = () if layer else (positions, freq, b_qkv, w_qkv, kc, vc)
            out = finish(layer, o.reshape(HEADS, SEQS, HEAD), ml, hidden, ln_gain, ln_bias, b_dense, b_up, b_down, w_dense, w_up, w_down, *following)
            hidden, heads, kb, vb = out if following else (out, None, None, None)
        return hidden, done[0].reshape(shape), done[1].reshape(shape)

    return jax.shard_map(device_step, mesh=mesh, in_specs=in_specs, out_specs=out_specs, check_vma=False)
```

```python
import functools

import jax
import jax.numpy as jnp
import numpy as np
from jax import lax
from jax.experimental import pallas as pl
from jax.experimental.pallas import tpu as pltpu
from jax.sharding import PartitionSpec as P

BLOCK_SIZE = 64
LOCAL_BLOCKS = 16
VERT_STRIDE = 8
ROPE_THETA = 1000000.0
GELU_LIMIT = 20.0
NORM_EPS = 0.00001
MASKED = -1e30

SEQS = 64
MODEL = 4096
HEAD = 128
KVL = 4
GROUP = 4
HEADS = KVL * GROUP
SLOTS = 128
ROWS = SLOTS * KVL
QKV_N = (GROUP + 2) * HEAD
UP_N = 512
UP_STEPS = 7
DOWN_K = 3584
HALF_K = DOWN_K // 2
DENSE_K = 1024
OUT_STEPS = 4
PIECE = 256
CHUNK = 8
MIB = 1024 * 1024
QKV_MIB = 20
ATTEND_MIB = 8
MLP_MIB = 45

A, B = range(2)
K0, K1, K2, K3 = range(4)
A_FAR, B_FAR, A_X, B_Y, A_Y, B_X, A_LAST, B_LAST = range(12, 20)

F32 = jnp.float32
BF16 = jnp.bfloat16
MESH = pl.DeviceIdType.MESH
VM = pl.BlockSpec(memory_space=pltpu.VMEM)
SM = pl.BlockSpec(memory_space=pltpu.SMEM)
HBM = pl.BlockSpec(memory_space=pltpu.HBM)


def kept(shape, dtype):
    return pltpu.VMEM(shape, dtype)


def pin(x):
    return pltpu.with_memory_space_constraint(x, pltpu.HBM)


def near(x):
    return pltpu.with_memory_space_constraint(x, pltpu.VMEM)


def exchange(number, mib):
    return pltpu.CompilerParams(collective_id=number, has_side_effects=True, vmem_limit_bytes=mib * MIB)


def rowsum(a):
    return jnp.sum(a, axis=1, keepdims=True)


def block(index, size):
    return pl.ds(pl.multiple_of(index * size, size), size)


def dot(a, b):
    return jnp.dot(a, b, preferred_element_type=F32)


def place():
    sp = lax.axis_index('sp')
    return lax.axis_index('tp'), sp, sp // 2, lax.rem(sp, 2)


def enter(peers):
    barrier = pltpu.get_barrier_semaphore()
    for peer in peers:
        pl.semaphore_signal(barrier, inc=1, device_id=peer, device_id_type=MESH)
    pl.semaphore_wait(barrier, len(peers))


def remote(src, dst, send, recv, peer):
    return pltpu.make_async_remote_copy(src_ref=src, dst_ref=dst, send_sem=send, recv_sem=recv, device_id=peer, device_id_type=MESH)


def norm_into(pieces, gain, shift, out_ref):
    width = pieces[0]().shape[1]
    total = sum(rowsum(p()) for p in pieces)
    mean = total * (1.0 / MODEL)
    square = sum(rowsum(jnp.square(p() - mean)) for p in pieces)
    scale = lax.rsqrt(square * (1.0 / MODEL) + NORM_EPS)
    for i, p in enumerate(pieces):
        cols = slice(i * width, (i + 1) * width)
        out_ref[:, cols] = ((p() - mean) * scale * gain(cols) + shift(cols)).astype(BF16)


def position_rows(pos_ref, rows_ref):
    row = lax.broadcasted_iota(jnp.int32, (8, HEAD), 0)
    for first in range(0, SEQS, 8):
        pos = jnp.zeros((8, HEAD), jnp.int32)
        for i in range(8):
            pos = jnp.where(row == i, pos_ref[first + i], pos)
        rows_ref[first:first + 8] = pos


def rope_tables(rows_ref, freq_ref, cos_ref, sin_ref):
    sign = jnp.where(lax.broadcasted_iota(jnp.int32, (SEQS, HEAD), 1) < HEAD // 2, -1.0, 1.0)
    angle = rows_ref[...].astype(F32) * freq_ref[...]
    cos_ref[...] = jnp.cos(angle)
    sin_ref[...] = jnp.sin(angle) * sign


def load_qkv(layer, c, w_ref, wbuf, sem, j):
    cols = block(c * 3 + j, UP_N)
    return pltpu.make_async_copy(w_ref.at[layer, :, cols], wbuf.at[j], sem.at[j])


def qkv_phase(layer, c, partner, product, bias_ref, cos_ref, sin_ref, heads, ssem, rsem):
    sent = []
    for j in range(3):
        cols = block(c * 3 + j, UP_N)
        proj = product(j) + bias_ref[layer:layer + 1, cols].astype(F32)
        for n in range(4):
            local, i = divmod(4 * j + n, GROUP + 2)
            kv = 2 * c + local
            part = proj[:, n * HEAD:(n + 1) * HEAD]
            if i <= GROUP:
                part = part * cos_ref[...] + pltpu.roll(part, HEAD // 2, 1) * sin_ref[...]
            slot = kv * GROUP + i if i < GROUP else HEADS + (i - GROUP) * KVL + kv
            heads[slot] = part.astype(BF16).astype(F32)
            piece = {GROUP - 1: pl.ds(kv * GROUP, GROUP), GROUP: pl.ds(HEADS + kv, 1), GROUP + 1: pl.ds(HEADS + KVL + kv, 1)}.get(i)
            if piece is not None:
                k = len(sent)
                sent.append(remote(heads.at[piece], heads.at[piece], ssem.at[k], rsem.at[k], partner))
                sent[-1].start()
    for copy in sent:
        copy.wait()


def copy_in(pairs, sems):
    copies = [pltpu.make_async_copy(src, dst, sems.at[i]) for i, (src, dst) in enumerate(pairs)]
    for copy in copies:
        copy.start()
    return copies


def cache_copies(layer, kc_ref, vc_ref, k_out, v_out, sems):
    return [pltpu.make_async_copy(src.at[layer], dst, sems.at[n]) for n, (src, dst) in enumerate(((kc_ref, k_out), (vc_ref, v_out)))]


def qkv_kernel(
    layer, pos_hbm, freq_hbm, h_hbm, gain_hbm, shift_hbm, bias_hbm, w_ref, kc_ref, vc_ref, out_ref, k_out, v_out, rows_out,
    wbuf, u, heads, cos, sin, pos, freq, h, gain, shift, bias, isem, wsem, ksem, ssem, rsem,
):
    tp, sp, x, c = place()
    small = copy_in([(h_hbm, h), (gain_hbm, gain), (shift_hbm, shift), (pos_hbm, pos), (freq_hbm, freq), (bias_hbm, bias)], isem)
    loads = [load_qkv(layer, c, w_ref, wbuf, wsem, j) for j in range(3)]
    partner = {'sp': sp + 1 - 2 * c}
    for copy in small:
        copy.wait()

    def begin(j, _):
        load_qkv(layer, c, w_ref, wbuf, wsem, j).start()
        return 0

    lax.fori_loop(0, 3, begin, 0)
    for copy in cache_copies(layer, kc_ref, vc_ref, k_out, v_out, ksem):
        copy.start()
    norm_into(
        [lambda i=i: h[:, i * 512:(i + 1) * 512].astype(F32) for i in range(8)],
        lambda cols: gain[layer, 0:1, cols].astype(F32),
        lambda cols: shift[layer, 0:1, cols].astype(F32),
        u,
    )
    position_rows(pos, rows_out)
    rope_tables(rows_out, freq, cos, sin)
    enter([partner])

    def product(j):
        loads[j].wait()
        return dot(u[...], wbuf[j])

    qkv_phase(layer, c, partner, product, bias, cos, sin, heads, ssem, rsem)
    out_ref[...] = heads[...]
    for copy in cache_copies(layer, kc_ref, vc_ref, k_out, v_out, ksem):
        copy.wait()


HEADS_SHAPE = (HEADS + 2 * KVL, SEQS, HEAD)


CACHE = kept((SEQS, ROWS, HEAD), BF16)


def project(layer, positions, freq, h, gain, shift, bias, w, kc, vc):
    dma = pltpu.SemaphoreType.DMA
    return pl.pallas_call(
        functools.partial(qkv_kernel, layer),
        out_shape=(kept(HEADS_SHAPE, F32), CACHE, CACHE, kept((SEQS, HEAD), jnp.int32)),
        in_specs=[HBM] * 9,
        out_specs=(VM, VM, VM, VM),
        scratch_shapes=[
            pltpu.VMEM((3, MODEL, UP_N), BF16),
            pltpu.VMEM((SEQS, MODEL), BF16),
            pltpu.VMEM(HEADS_SHAPE, F32),
            pltpu.VMEM((SEQS, HEAD), F32),
            pltpu.VMEM((SEQS, HEAD), F32),
            pltpu.SMEM((SEQS,), jnp.int32),
            pltpu.VMEM((1, HEAD), F32),
            pltpu.VMEM((SEQS, MODEL), BF16),
            pltpu.VMEM(gain.shape, BF16),
            pltpu.VMEM(shift.shape, BF16),
            pltpu.VMEM(bias.shape, BF16),
            dma((6,)), dma((3,)), dma((2,)), dma((6,)), dma((6,)),
        ],
        compiler_params=exchange(layer, QKV_MIB),
        name=f'qkv_{layer}',
    )(*map(pin, (positions, freq, h, gain, shift, bias, w, kc, vc)))


def attend_kernel(layer, sparse, pos_hbm, heads_ref, kb, vb, *rest):
    if layer:
        rest = rest[2:]
    ko_ref, vo_ref, o_ref, ml_ref, pos_ref, mref, lref, slot_of, keep_of, tiles, psem, ssem, tsem = rest
    tp, sp, x, c = place()
    steps = SEQS // CHUNK
    copy_in([(pos_hbm, pos_ref)], psem)

    def save(i, n):
        dst, buf = ((ko_ref, kb), (vo_ref, vb))[n]
        rows = pl.ds(i * CHUNK, CHUNK)
        return pltpu.make_async_copy(buf.at[rows], dst.at[layer, rows], ssem.at[n, i])

    def place_of(b):
        t = pos_ref[b] - sp * SLOTS
        inside = jnp.logical_and(t >= 0, t < SLOTS)
        t = jnp.clip(t, 0, SLOTS - 1)
        return t, inside, pl.multiple_of((t // 4) * (4 * KVL), 4 * KVL)

    def patch(b, n):
        base = place_of(b)[2]
        return pltpu.make_async_copy(tiles.at[n, b], (ko_ref, vo_ref)[n].at[layer, b, pl.ds(base, 4 * KVL)], tsem.at[n])

    for i in range(steps):
        for n in range(2):
            save(i, n).start()
    row = lax.broadcasted_iota(jnp.int32, (HEADS, ROWS), 0)
    col = lax.broadcasted_iota(jnp.int32, (HEADS, ROWS), 1)
    slot = sp * SLOTS + col // KVL
    slot_of[...] = jnp.where(lax.rem(col, KVL) == row // GROUP, slot, jnp.int32(1 << 30))
    if sparse:
        block = slot // BLOCK_SIZE
        vertical = lax.rem(block + tp * HEADS + row + 1, VERT_STRIDE) == 0
        keep_of[...] = jnp.where(vertical, jnp.int32(1 << 20), block)
    mref[...] = jnp.zeros_like(mref)
    lref[...] = jnp.ones_like(lref)
    lane = lax.broadcasted_iota(jnp.int32, (HEADS, HEAD), 1)
    row16 = lax.broadcasted_iota(jnp.int32, (4 * KVL, HEAD), 0)

    pltpu.make_async_copy(pos_hbm, pos_ref, psem.at[0]).wait()

    def repeat(part):
        return jnp.concatenate([jnp.broadcast_to(part[kv:kv + 1], (GROUP, HEAD)) for kv in range(KVL)], axis=0)

    def body(i, _):
        for first in range(0, CHUNK, 4):
            ids = [i * CHUNK + first + s for s in range(4)]
            keeps, hits, scores, news = [], [], [], []
            for b in ids:
                q = heads_ref[pl.ds(b, HEADS, stride=SEQS), :]
                new = heads_ref[pl.ds(HEADS * SEQS + b, 2 * KVL, stride=SEQS), :]
                raw = lax.dot_general(q.astype(BF16), kb[b], (((1,), (1,)), ((), ())), preferred_element_type=F32)
                pos = pos_ref[b]
                keep = slot_of[...] <= pos
                hit = slot_of[...] == pos
                if sparse:
                    keep = jnp.logical_and(keep, pos // BLOCK_SIZE - keep_of[...] < LOCAL_BLOCKS)
                raw = jnp.where(hit, rowsum(q * repeat(new[:KVL])), raw)
                keeps.append(keep)
                hits.append(hit)
                news.append(new)
                scores.append(jnp.where(keep, raw * (1.0 / HEAD), MASKED))
            weights, added = [], []
            for b, keep, hit, score in zip(ids, keeps, hits, scores):
                peak = jnp.max(score, axis=1, keepdims=True)
                weight = jnp.where(keep, jnp.exp(score - peak), 0.0)
                mref[...] = jnp.where(lane == b, peak, mref[...])
                lref[...] = jnp.where(lane == b, rowsum(weight), lref[...])
                weight = weight.astype(BF16).astype(F32)
                added.append(rowsum(jnp.where(hit, weight, 0.0)))
                weights.append(jnp.where(hit, 0.0, weight).astype(BF16))
            for b, weight, extra, new in zip(ids, weights, added, news):
                o_ref[pl.ds(b, HEADS, stride=SEQS), :] = dot(weight, vb[b]) + extra * repeat(new[KVL:])
            for b, new in zip(ids, news):
                t, inside, base = place_of(b)
                hit = jnp.logical_and(row16 // KVL == lax.rem(t, 4), inside)
                for n, buf in enumerate((kb, vb)):
                    fresh = jnp.concatenate([new[n * KVL:(n + 1) * KVL]] * 4, axis=0)
                    tiles[n, b] = jnp.where(hit, fresh, buf[b, pl.ds(base, 4 * KVL), :].astype(F32)).astype(BF16)
        for n in range(2):
            save(i, n).wait()
        for s in range(CHUNK):
            for n in range(2):
                patch(i * CHUNK + s, n).start()
        return 0

    lax.fori_loop(0, steps, body, 0)
    for kv in range(KVL):
        ml_ref[kv, 0:GROUP] = mref[kv * GROUP:(kv + 1) * GROUP]
        ml_ref[kv, GROUP:2 * GROUP] = lref[kv * GROUP:(kv + 1) * GROUP]

    for n in range(2):
        pltpu.make_async_copy(tiles.at[n], (ko_ref, vo_ref)[n].at[layer, :, pl.ds(0, 4 * KVL)], tsem.at[n]).wait()


def attend(layer, positions, heads, kb, vb, shape, *done):
    cache = jax.ShapeDtypeStruct(shape, BF16)
    dma = pltpu.SemaphoreType.DMA
    return pl.pallas_call(
        functools.partial(attend_kernel, layer, layer == 0),
        out_shape=(cache, cache, kept((HEADS * SEQS, HEAD), F32), kept((KVL, 2 * GROUP, HEAD), F32)),
        in_specs=[HBM, VM, VM, VM] + [HBM] * len(done),
        out_specs=(HBM, HBM, VM, VM),
        scratch_shapes=[
            pltpu.SMEM((SEQS,), jnp.int32),
            pltpu.VMEM((HEADS, HEAD), F32),
            pltpu.VMEM((HEADS, HEAD), F32),
            pltpu.VMEM((HEADS, ROWS), jnp.int32),
            pltpu.VMEM((HEADS, ROWS), jnp.int32),
            pltpu.VMEM((2, SEQS, 4 * KVL, HEAD), BF16),
            dma((1,)), dma((2, SEQS // CHUNK)), dma((2,)),
        ],
        input_output_aliases={4: 0, 5: 1} if done else {},
        compiler_params=pltpu.CompilerParams(vmem_limit_bytes=ATTEND_MIB * MIB),
        name=f'attend_{layer}',
    )(pin(positions), *map(near, (heads, kb, vb)), *map(pin, done))


def mlp_kernel(layer, last, ahead, o_ref, ml_ref, h_ref, gain_ref, shift_ref, bd_ref, bu_ref, bn_ref, wd_ref, wu_ref, wn_ref, *rest):
    if not last:
        rows_ref, freq_ref, bq_ref, wq_ref, kc_ref, vc_ref, out_ref, heads_out, k_out, v_out = rest[:10]
        heads, cos, sin, k_s, q_s, q_r = rest[-6:]
        rest = rest[10:-6]
    else:
        out_ref, rest = rest[0], rest[1:]
    (
        wu, wn, mls, mlx, fromcore, tosend, kept, fromx, mine, other, ob, part, ra, rb, xs, u, mf, mp, mb, ps, acc, st, mo,
        wsem, o_s, o_r, m_s, m_r, c_s, c_r, t_s, t_r,
    ) = rest
    tp, sp, x, c = place()
    y = tp
    core_peer = {'sp': sp + 1 - 2 * c}
    x_peer = {'sp': 2 * (1 - x) + 1 - c}
    y_peer = {'tp': 1 - tp, 'sp': 2 * x + 1 - c}
    c = lax.rem(c + x + y, 2)
    oc, ox, oy = 1 - c, 1 - x, 1 - y
    quarter = [2 * ox + oy, 2 * ox + y, 2 * x + oy, 2 * x + y]

    def turn(k):
        far, near = 1 - k // 2, k // 2
        return 2 * (far * ox + near * x) + (1 - k % 2) * oy + k % 2 * y

    def cols_of(k):
        return block(c * 4 + turn(k), UP_N)

    def load_dense(k):
        return pltpu.make_async_copy(wd_ref.at[layer, block(x, DENSE_K), cols_of(k)], wu.at[UP_STEPS - 1, pl.ds(k * DENSE_K, DENSE_K)], wsem.at[k])

    def load_up(j):
        cols = block((2 * x + c) * UP_STEPS + j, UP_N)
        return pltpu.make_async_copy(wu_ref.at[layer, :, cols], wu.at[j], wsem.at[4 + j])

    def load_down(k):
        rows = block(x, DOWN_K)
        to = wn.at[k] if k < ahead else wu.at[k - ahead, pl.ds(0, DOWN_K)]
        return pltpu.make_async_copy(wn_ref.at[layer, rows, cols_of(k)], to, wsem.at[4 + UP_STEPS + k])

    def down_half(k, half):
        rows = block(half, HALF_K)
        return dot(mb[:, rows], wn[k, rows] if k < ahead else wu[k - ahead, rows])

    def load_next(j):
        return load_qkv(layer + 1, c, wq_ref, wu.at[pl.ds(4, 3)], wsem, j)

    for k in range(OUT_STEPS):
        load_dense(k).start()
    for j in range(UP_STEPS - 1):
        load_up(j).start()
    for k in range(ahead):
        load_down(k).start()
    if not last:
        cache = cache_copies(layer + 1, kc_ref, vc_ref, k_out, v_out, k_s)
        for copy in cache:
            copy.start()
    everyone = [lax.rem(tp * 4 + sp + r, 8) for r in range(1, 8)]
    enter([{'tp': peer // 4, 'sp': lax.rem(peer, 4)} for peer in everyone])
    waits = []

    def swap(i, src, dst, peer):
        copy = remote(src, dst, o_s.at[i], o_r.at[i], peer)
        copy.start()
        waits.append(copy)
        return copy

    stats = swap(4, ml_ref, mls, core_peer)
    slabs = [None, None]
    for n, xd in enumerate((ox, x)):
        src = o_ref.at[pl.ds((2 * xd + oc) * GROUP, GROUP)]
        slabs[n] = swap(n, src, fromcore.at[n], core_peer)

    def columns(rows):
        return jnp.concatenate(rows + [jnp.zeros((HEAD - GROUP * len(rows), HEAD), F32)], axis=0).T[:SEQS]

    def merge(one, two):
        top = jnp.maximum(one[:GROUP], two[:GROUP])
        first, second = jnp.exp(one[:GROUP] - top), jnp.exp(two[:GROUP] - top)
        return first, second, top, first * one[GROUP:] + second * two[GROUP:]

    stats.wait_recv()
    rows = []
    for n, xd in enumerate((ox, x)):
        first, second, top, total = merge(ml_ref[2 * xd + c], mls[2 * xd + c])
        rows += [first, second]
        mlx[n] = jnp.concatenate([top, total], axis=0)
    cross_ml = swap(5, mlx.at[0], mlx.at[2], x_peer)
    scale = columns(rows)
    for n, (xd, out) in enumerate(((ox, tosend), (x, kept))):
        slabs[n].wait_recv()
        kv = 2 * xd + c
        for g in range(GROUP):
            i = 2 * n * GROUP + g
            out[g] = o_ref[kv * GROUP + g] * scale[:, i:i + 1] + fromcore[n, g] * scale[:, i + GROUP:i + GROUP + 1]
        if n == 0:
            cross = swap(2, tosend, fromx, x_peer)
    if not last:
        rope_tables(rows_ref, freq_ref, cos, sin)
    cross_ml.wait_recv()
    first, second, _, total = merge(mlx[1], mlx[2])
    scale = columns([first / total, second / total])
    cross.wait_recv()
    for g in range(GROUP):
        val = (kept[g] * scale[:, g:g + 1] + fromx[g] * scale[:, g + GROUP:g + GROUP + 1]).astype(BF16)
        mine[g] = val.astype(F32)
        ob[:, block(c * GROUP + g, HEAD)] = val
    share = swap(3, mine, other, core_peer)
    def dense_half(k, half):
        return dot(ob[:, block(half, UP_N)], wu[UP_STEPS - 1, block(2 * k + half, UP_N)])

    for k in range(OUT_STEPS):
        load_dense(k).wait()
        ps[k] = dense_half(k, c)
    share.wait_recv()
    for g in range(GROUP):
        ob[:, block(oc * GROUP + g, HEAD)] = other[g].astype(BF16)

    own = (c * 4 + quarter[K3]) * 2

    def all_reduce(ph, chunk, residual, bias_ref, after=lambda: None, stats=True):
        def post(i, src, dst, peer):
            copy = remote(src, dst, c_s.at[ph, int(i > 5)], c_r.at[ph, i], peer)
            copy.start()
            return copy

        def keep(k):
            val = chunk(k)
            part[ph, k, A] = val[:, :PIECE]
            part[ph, k, B] = val[:, PIECE:]

        keep(K0)
        a0 = post(0, part.at[ph, K0, A], ra.at[ph, K0], x_peer)
        b0 = post(1, part.at[ph, K0, B], rb.at[ph, K0], y_peer)
        keep(K1)
        a1 = post(2, part.at[ph, K1, A], ra.at[ph, K1], x_peer)
        keep(K2)
        b1 = post(3, part.at[ph, K2, B], rb.at[ph, K1], y_peer)
        keep(K3)
        after()
        b0.wait_recv()
        part[ph, K1, B] += rb[ph, K0]
        b2 = post(4, part.at[ph, K1, B], rb.at[ph, K2], x_peer)
        a0.wait_recv()
        part[ph, K2, A] += ra[ph, K0]
        a2 = post(5, part.at[ph, K2, A], ra.at[ph, K2], y_peer)
        for half, (first, second, landed) in enumerate(((a1, a2, ra), (b1, b2, rb))):
            first.wait_recv()
            second.wait_recv()
            cols = block(own + half, PIECE)
            full = part[ph, K3, half] + landed[ph, K1] + landed[ph, K2]
            xs[ph, own + half] = (residual(half, cols) + full + bias_ref[layer:layer + 1, cols].astype(F32)).astype(BF16).astype(F32)
        if stats:
            send_moments(ph)
        gather = {}
        for n in range(3):
            for half in range(2):
                peer = core_peer if n == 2 else (x_peer, y_peer)[(n + half) % 2]
                mine_ref = xs.at[ph, own + half]
                gather[half, n] = post(6 + 3 * half + n, mine_ref, mine_ref, peer)
        base = c * 8
        from_x = base + quarter[K1] * 2
        from_y = base + quarter[K2] * 2
        far = base + quarter[K0] * 2

        def forward(i, piece, peer):
            ref = xs.at[ph, piece]
            return post(i, ref, ref, peer)

        sent = {}

        def pump(step):
            if step == 0:
                gather[A, K0].wait_recv()
                sent[A_FAR] = forward(A_FAR, from_x, y_peer)
                sent[A_X] = forward(A_X, from_x, core_peer)
                gather[B, K0].wait_recv()
                sent[B_FAR] = forward(B_FAR, from_y + 1, x_peer)
                sent[B_Y] = forward(B_Y, from_y + 1, core_peer)
            elif step == 1:
                gather[A, K1].wait_recv()
                sent[A_Y] = forward(A_Y, from_y, core_peer)
                gather[B, K1].wait_recv()
                sent[B_X] = forward(B_X, from_x + 1, core_peer)
            else:
                sent[A_FAR].wait_recv()
                sent[A_LAST] = forward(A_LAST, far, core_peer)
                sent[B_FAR].wait_recv()
                sent[B_LAST] = forward(B_LAST, far + 1, core_peer)

        def arrive(group):
            for copy in {0: [gather[A, K2], gather[B, K2]], 1: [sent.get(i) for i in (A_X, B_Y, A_Y, B_X)], 2: [sent.get(i) for i in (A_LAST, B_LAST)]}[group]:
                copy.wait_recv()

        return pump, arrive

    me = tp * 4 + sp

    def send_moments(ph):
        a, b = xs[ph, own], xs[ph, own + 1]
        count = 2 * PIECE
        mean = (rowsum(a) + rowsum(b)) * (1.0 / count)
        spread = rowsum(jnp.square(a - mean)) + rowsum(jnp.square(b - mean))
        lane = lax.broadcasted_iota(jnp.int32, (SEQS, HEAD), 1)
        both = jnp.where(lane == 0, mean, jnp.where(lane == 1, spread, 0.0))
        st[ph, me] = jnp.concatenate([both, jnp.zeros((HEAD - SEQS, HEAD), F32)], axis=0).T[:8]
        for r in range(1, 8):
            peer = lax.rem(me + r, 8)
            remote(st.at[ph, me], st.at[ph, me], t_s.at[ph], t_r.at[ph], {'tp': peer // 4, 'sp': lax.rem(peer, 4)}).start()

    def moments(ph):
        remote(st.at[ph, pl.ds(0, 7)], st.at[ph, pl.ds(0, 7)], t_s.at[ph], t_r.at[ph], x_peer).wait()
        parts = [st[ph, i] for i in range(8)]
        mean = sum(p[0:1] for p in parts) * 0.125
        spread = sum(p[1:2] + (2.0 * PIECE) * jnp.square(p[0:1] - mean) for p in parts)
        scale = lax.rsqrt(spread * (1.0 / MODEL) + NORM_EPS)
        table = jnp.concatenate([mean, scale, jnp.zeros((HEAD - 2, HEAD), F32)], axis=0).T[:SEQS]
        mo[...] = table

    def slices(group):
        if group == 0:
            return c * 4 + quarter[K3], oc * 4 + quarter[K3]
        if group == 2:
            return c * 4 + quarter[K0], oc * 4 + quarter[K0]
        return [core * 4 + quarter[k] for core in (c, oc) for k in (1, 2)]

    def norm_group(ph, row, norm, group):
        mean, scale = mo[:, 0:1], mo[:, 1:2]
        for n, index in enumerate(slices(group)):
            for half in range(2):
                cols = block(2 * index + half, PIECE)
                gain, shift = gain_ref[row, norm:norm + 1, cols].astype(F32), shift_ref[row, norm:norm + 1, cols].astype(F32)
                at = (2 * n + half) * PIECE
                u[:, at:at + PIECE] = ((xs[ph, 2 * index + half] - mean) * scale * gain + shift).astype(BF16)

    def product(group, slot):
        total = 0.0
        for n, index in enumerate(slices(group)):
            rows = block(index, UP_N)
            total = total + dot(u[:, n * 512:(n + 1) * 512], wu[slot, rows])
        return total

    def normed_product(ph, row, norm, stages, first, count, wait, finish_step):
        pump, arrive = stages

        def add(group, low, high):
            def step(j, _):
                if group == 0:
                    wait(j)
                    acc[j] = product(group, first + j)
                else:
                    acc[j] += product(group, first + j)
                return 0

            lax.fori_loop(low, high, step, 0, unroll=True)

        half = count // 2 + 1
        moments(ph)
        arrive(0)
        norm_group(ph, row, norm, 0)
        pump(0)
        add(0, 0, half)
        pump(1)
        add(0, half, count)
        arrive(1)
        norm_group(ph, row, norm, 1)
        add(1, 0, half)
        pump(2)
        add(1, half, count)
        arrive(2)
        norm_group(ph, row, norm, 2)
        finish_step(lambda j: acc[j] + product(2, first + j))

    def dense_chunk(k):
        return ps[k] + dense_half(k, oc)

    stages = all_reduce(0, dense_chunk, lambda half, cols: h_ref[:, cols].astype(F32), bd_ref, load_up(UP_STEPS - 1).start)
    take = (lax.broadcasted_iota(jnp.int32, (2 * HEAD, HEAD), 0) == 2 * lax.broadcasted_iota(jnp.int32, (2 * HEAD, HEAD), 1)).astype(BF16)
    even = lax.rem(lax.broadcasted_iota(jnp.int32, (SEQS, UP_N), 1), 2) == 0

    def share_m(j):
        return remote(mf.at[j], mp.at[j], m_s.at[0], m_r.at[0], core_peer)

    def up_step(full, j):
        cols = block((2 * x + c) * UP_STEPS + j, UP_N)
        val = full(j) + bu_ref[layer:layer + 1, cols].astype(F32)
        gate = jnp.minimum(val, GELU_LIMIT)
        gate = gate * (1.0 / (1.0 + jnp.exp(-1.702 * gate)))
        linear = jnp.clip(val, -GELU_LIMIT, GELU_LIMIT) + 1.0
        mixed = jnp.where(even, gate * pltpu.roll(linear, UP_N - 1, 1), 0.0).astype(BF16)
        packed = jnp.concatenate([dot(mixed[:, i:i + 2 * HEAD], take) for i in range(0, UP_N, 2 * HEAD)], axis=1)
        mf[j] = packed
        share_m(j).start()
        mb[:, block(c * UP_STEPS + j, PIECE)] = packed.astype(BF16)

        if j < 4 - ahead:
            load_down(j + ahead).start()
        if not last and j >= 4:
            load_next(j - 4).start()

    def up_steps(full):
        for j in range(UP_STEPS):
            up_step(full, j)

    normed_product(0, layer, 1, stages, 0, UP_STEPS, lambda j: load_up(j).wait(), up_steps)
    for k in range(OUT_STEPS):
        load_down(k).wait()
        ps[k] = down_half(k, c)
    remote(mf, mp, m_s.at[0], m_r.at[0], core_peer).wait()
    for j in range(UP_STEPS):
        mb[:, block(oc * UP_STEPS + j, PIECE)] = mp[j].astype(BF16)

    def down_chunk(k):
        return ps[k] + down_half(k, oc)

    stages = all_reduce(1, down_chunk, lambda half, cols: xs[0, own + half], bn_ref, stats=not last)
    if last:
        pump, arrive = stages
        for step in range(3):
            pump(step)
        for group in range(3):
            arrive(group)
    else:
        def qkv_steps(full):
            qkv_phase(layer + 1, c, core_peer, full, bq_ref, cos, sin, heads, q_s, q_r)

        normed_product(1, layer + 1, 0, stages, 4, 3, lambda j: load_next(j).wait(), qkv_steps)
        heads_out[...] = heads[...]
        for copy in cache:
            copy.wait()
    for i in range(16):
        out_ref[:, i * PIECE:(i + 1) * PIECE] = xs[1, i].astype(BF16)
    for ph in range(2):
        for n, pieces in enumerate((6, 14)):
            remote(xs.at[ph, pl.ds(0, pieces)], xs.at[ph, pl.ds(0, pieces)], c_s.at[ph, n], c_r.at[ph, 0], x_peer).wait_send()
    for copy in waits:
        copy.wait_send()


def finish(layer, o, ml, h, gain, shift, bd, bu, bn, wd, wu, wn, *following):
    slab = pltpu.VMEM((GROUP, SEQS, HEAD), F32)
    dma = pltpu.SemaphoreType.DMA
    last = not following
    ahead = 4 if last else 1
    hidden = kept((SEQS, MODEL), BF16)
    table = pltpu.VMEM((SEQS, HEAD), F32)
    return pl.pallas_call(
        functools.partial(mlp_kernel, layer, last, ahead),
        out_shape=hidden if last else (hidden, kept(HEADS_SHAPE, F32), CACHE, CACHE),
        in_specs=[VM] * 8 + [HBM] * 3 + ([] if last else [VM, VM, VM, HBM, HBM, HBM]),
        out_specs=VM if last else (VM, VM, VM, VM),
        scratch_shapes=[
            pltpu.VMEM((UP_STEPS, MODEL, UP_N), BF16),
            pltpu.VMEM((ahead, DOWN_K, 512), BF16),
            pltpu.VMEM((KVL, 2 * GROUP, HEAD), F32),
            pltpu.VMEM((3, 2 * GROUP, HEAD), F32),
            pltpu.VMEM((2, GROUP, SEQS, HEAD), F32),
            slab, slab, slab, slab, slab,
            pltpu.VMEM((SEQS, 1024), BF16),
            pltpu.VMEM((2, 4, 2, SEQS, PIECE), F32),
            pltpu.VMEM((2, 3, SEQS, PIECE), F32),
            pltpu.VMEM((2, 3, SEQS, PIECE), F32),
            pltpu.VMEM((2, 16, SEQS, PIECE), F32),
            pltpu.VMEM((SEQS, 2048), BF16),
            pltpu.VMEM((UP_STEPS, SEQS, 256), F32),
            pltpu.VMEM((UP_STEPS, SEQS, 256), F32),
            pltpu.VMEM((SEQS, DOWN_K), BF16),
            pltpu.VMEM((4, SEQS, 512), F32),
            pltpu.VMEM((UP_STEPS, SEQS, UP_N), F32),
            pltpu.VMEM((2, 8, 8, HEAD), F32),
            pltpu.VMEM((SEQS, HEAD), F32),
            dma((8 + UP_STEPS,)), dma((6,)), dma((6,)), dma((1,)), dma((1,)), dma((2, 2)), dma((2, 20)), dma((2,)), dma((2,)),
        ] + ([] if last else [pltpu.VMEM(HEADS_SHAPE, F32), table, table, dma((2,)), dma((6,)), dma((6,))]),
        compiler_params=exchange(2 + layer, (60 if last else MLP_MIB)),
        name=f'mlp_{layer}',
    )(near(o), near(ml), near(h) if last else pin(h), *map(pin, (gain, shift, bd, bu, bn, wd, wu, wn)), *map(near, following[:1]), *map(pin, following[1:]))


def solution(mesh):
    cache_spec = P(None, 'dp', 'sp', 'tp', None)
    rows, bias, cols = P(None, 'tp', None), P(None, 'tp'), P(None, None, 'tp')
    in_specs = (P('dp'), P('dp'), cache_spec, cache_spec, P(), P(), cols, bias, rows, P(), cols, bias, rows, P())
    out_specs = (P('dp'), cache_spec, cache_spec)

    def device_step(hidden, positions, k_cache, v_cache, ln_gain, ln_bias, w_qkv, b_qkv, w_dense, b_dense, w_up, b_up, w_down, b_down):
        freq = ROPE_THETA ** (-np.arange(HEAD // 2) * (2.0 / HEAD))
        freq = jnp.asarray(np.tile(freq, 2)[None].astype(np.float32))
        shape = k_cache.shape
        flat = (2, SEQS, ROWS, HEAD)
        kc = k_cache.reshape(flat)
        vc = v_cache.reshape(flat)
        done = ()
        heads, kb, vb, rows = project(0, positions, freq, hidden, ln_gain, ln_bias, b_qkv, w_qkv, kc, vc)
        for layer in range(2):
            ko, vo, o, ml = attend(layer, positions, heads.reshape(-1, HEAD), kb, vb, flat, *done)
            done = (ko, vo)
            following = () if layer else (rows, freq, b_qkv, w_qkv, kc, vc)
            out = finish(layer, o.reshape(HEADS, SEQS, HEAD), ml, hidden, ln_gain, ln_bias, b_dense, b_up, b_down, w_dense, w_up, w_down, *following)
            hidden, heads, kb, vb = out if following else (out, None, None, None)
        return hidden, done[0].reshape(shape), done[1].reshape(shape)

    return jax.shard_map(device_step, mesh=mesh, in_specs=in_specs, out_specs=out_specs, check_vma=False)
```

```python
import functools

import jax
import jax.numpy as jnp
import numpy as np
from jax import lax
from jax.experimental import pallas as pl
from jax.experimental.pallas import tpu as pltpu
from jax.sharding import PartitionSpec as P

BLOCK_SIZE = 64
LOCAL_BLOCKS = 16
VERT_STRIDE = 8
ROPE_THETA = 1000000.0
GELU_LIMIT = 20.0
NORM_EPS = 0.00001
MASKED = -1e30

SEQS = 64
MODEL = 4096
HEAD = 128
KVL = 4
GROUP = 4
HEADS = KVL * GROUP
SLOTS = 128
ROWS = SLOTS * KVL
QKV_N = (GROUP + 2) * HEAD
UP_N = 512
UP_STEPS = 7
DOWN_K = 3584
HALF_K = DOWN_K // 2
DENSE_K = 1024
OUT_STEPS = 4
PIECE = 256
CHUNK = 8
MIB = 1024 * 1024
QKV_MIB = 20
ATTEND_MIB = 8
MLP_MIB = 45

A, B = range(2)
K0, K1, K2, K3 = range(4)
STRIP = 20
LATE_SEQS = 16
EARLY = pl.ds(0, SEQS - LATE_SEQS)
LATE = pl.ds(SEQS - LATE_SEQS, LATE_SEQS)
STRIPS = (pl.ds(0, HEAD), pl.ds(HEAD, HEAD))
A_FAR, B_FAR, A_X, B_Y, A_Y, B_X, A_LAST, B_LAST = range(12, STRIP)

F32 = jnp.float32
BF16 = jnp.bfloat16
MESH = pl.DeviceIdType.MESH
VM = pl.BlockSpec(memory_space=pltpu.VMEM)
SM = pl.BlockSpec(memory_space=pltpu.SMEM)
HBM = pl.BlockSpec(memory_space=pltpu.HBM)


def kept(shape, dtype):
    return pltpu.VMEM(shape, dtype)


def pin(x):
    return pltpu.with_memory_space_constraint(x, pltpu.HBM)


def near(x):
    return pltpu.with_memory_space_constraint(x, pltpu.VMEM)


def exchange(number, mib):
    return pltpu.CompilerParams(collective_id=number, has_side_effects=True, vmem_limit_bytes=mib * MIB)


def rowsum(a):
    return jnp.sum(a, axis=1, keepdims=True)


def block(index, size):
    return pl.ds(pl.multiple_of(index * size, size), size)


def dot(a, b):
    return jnp.dot(a, b, preferred_element_type=F32)


def place():
    sp = lax.axis_index('sp')
    return lax.axis_index('tp'), sp, sp // 2, lax.rem(sp, 2)


def enter(peers):
    barrier = pltpu.get_barrier_semaphore()
    for peer in peers:
        pl.semaphore_signal(barrier, inc=1, device_id=peer, device_id_type=MESH)
    pl.semaphore_wait(barrier, len(peers))


def remote(src, dst, send, recv, peer):
    return pltpu.make_async_remote_copy(src_ref=src, dst_ref=dst, send_sem=send, recv_sem=recv, device_id=peer, device_id_type=MESH)


def norm_into(pieces, gain, shift, out_ref):
    width = pieces[0]().shape[1]
    total = sum(rowsum(p()) for p in pieces)
    mean = total * (1.0 / MODEL)
    square = sum(rowsum(jnp.square(p() - mean)) for p in pieces)
    scale = lax.rsqrt(square * (1.0 / MODEL) + NORM_EPS)
    for i, p in enumerate(pieces):
        cols = slice(i * width, (i + 1) * width)
        out_ref[:, cols] = ((p() - mean) * scale * gain(cols) + shift(cols)).astype(BF16)


def position_rows(pos_ref, rows_ref):
    row = lax.broadcasted_iota(jnp.int32, (8, HEAD), 0)
    for first in range(0, SEQS, 8):
        pos = jnp.zeros((8, HEAD), jnp.int32)
        for i in range(8):
            pos = jnp.where(row == i, pos_ref[first + i], pos)
        rows_ref[first:first + 8] = pos


def rope_tables(rows_ref, freq_ref, cos_ref, sin_ref):
    sign = jnp.where(lax.broadcasted_iota(jnp.int32, (SEQS, HEAD), 1) < HEAD // 2, -1.0, 1.0)
    angle = rows_ref[...].astype(F32) * freq_ref[...]
    cos_ref[...] = jnp.cos(angle)
    sin_ref[...] = jnp.sin(angle) * sign


def load_qkv(layer, c, w_ref, wbuf, sem, j):
    cols = block(c * 3 + j, UP_N)
    return pltpu.make_async_copy(w_ref.at[layer, :, cols], wbuf.at[j], sem.at[j])


def qkv_phase(layer, c, partner, product, bias_ref, cos_ref, sin_ref, heads, ssem, rsem, meanwhile=lambda: None):
    sent = []
    for j in range(3):
        cols = block(c * 3 + j, UP_N)
        proj = product(j) + bias_ref[layer:layer + 1, cols].astype(F32)
        for n in range(4):
            local, i = divmod(4 * j + n, GROUP + 2)
            kv = 2 * c + local
            part = proj[:, n * HEAD:(n + 1) * HEAD]
            if i <= GROUP:
                part = part * cos_ref[...] + pltpu.roll(part, HEAD // 2, 1) * sin_ref[...]
            slot = kv * GROUP + i if i < GROUP else HEADS + (i - GROUP) * KVL + kv
            heads[slot] = part.astype(BF16).astype(F32)
            piece = {GROUP - 1: pl.ds(kv * GROUP, GROUP), GROUP: pl.ds(HEADS + kv, 1), GROUP + 1: pl.ds(HEADS + KVL + kv, 1)}.get(i)
            if piece is not None:
                k = len(sent)
                sent.append(remote(heads.at[piece], heads.at[piece], ssem.at[k], rsem.at[k], partner))
                sent[-1].start()
    meanwhile()
    for copy in sent:
        copy.wait()


def copy_in(pairs, sems):
    copies = [pltpu.make_async_copy(src, dst, sems.at[i]) for i, (src, dst) in enumerate(pairs)]
    for copy in copies:
        copy.start()
    return copies


def cache_copies(layer, kc_ref, vc_ref, k_out, v_out, sems, rows=pl.ds(0, SEQS)):
    return [pltpu.make_async_copy(src.at[layer, rows], dst.at[pl.ds(0, rows.size)], sems.at[n]) for n, (src, dst) in enumerate(((kc_ref, k_out), (vc_ref, v_out)))]


def qkv_kernel(
    layer, pos_hbm, freq_hbm, h_hbm, gain_hbm, shift_hbm, bias_hbm, w_ref, kc_ref, vc_ref, out_ref, k_out, v_out, rows_out,
    wbuf, u, heads, cos, sin, pos, freq, h, gain, shift, bias, isem, wsem, ksem, ssem, rsem,
):
    tp, sp, x, c = place()
    small = copy_in([(h_hbm, h), (gain_hbm, gain), (shift_hbm, shift), (pos_hbm, pos), (freq_hbm, freq), (bias_hbm, bias)], isem)
    loads = [load_qkv(layer, c, w_ref, wbuf, wsem, j) for j in range(3)]
    partner = {'sp': sp + 1 - 2 * c}
    for copy in small:
        copy.wait()

    def begin(j, _):
        load_qkv(layer, c, w_ref, wbuf, wsem, j).start()
        return 0

    lax.fori_loop(0, 3, begin, 0)
    for copy in cache_copies(layer, kc_ref, vc_ref, k_out, v_out, ksem, EARLY):
        copy.start()
    norm_into(
        [lambda i=i: h[:, i * 512:(i + 1) * 512].astype(F32) for i in range(8)],
        lambda cols: gain[layer, 0:1, cols].astype(F32),
        lambda cols: shift[layer, 0:1, cols].astype(F32),
        u,
    )
    position_rows(pos, rows_out)
    rope_tables(rows_out, freq, cos, sin)
    enter([partner])

    def product(j):
        loads[j].wait()
        return dot(u[...], wbuf[j])

    qkv_phase(layer, c, partner, product, bias, cos, sin, heads, ssem, rsem)
    out_ref[...] = heads[...]
    for copy in cache_copies(layer, kc_ref, vc_ref, k_out, v_out, ksem, EARLY):
        copy.wait()


HEADS_SHAPE = (HEADS + 2 * KVL, SEQS, HEAD)


CACHE = kept((SEQS, ROWS, HEAD), BF16)


def project(layer, positions, freq, h, gain, shift, bias, w, kc, vc):
    dma = pltpu.SemaphoreType.DMA
    return pl.pallas_call(
        functools.partial(qkv_kernel, layer),
        out_shape=(kept(HEADS_SHAPE, F32), CACHE, CACHE, kept((SEQS, HEAD), jnp.int32)),
        in_specs=[HBM] * 9,
        out_specs=(VM, VM, VM, VM),
        scratch_shapes=[
            pltpu.VMEM((3, MODEL, UP_N), BF16),
            pltpu.VMEM((SEQS, MODEL), BF16),
            pltpu.VMEM(HEADS_SHAPE, F32),
            pltpu.VMEM((SEQS, HEAD), F32),
            pltpu.VMEM((SEQS, HEAD), F32),
            pltpu.SMEM((SEQS,), jnp.int32),
            pltpu.VMEM((1, HEAD), F32),
            pltpu.VMEM((SEQS, MODEL), BF16),
            pltpu.VMEM(gain.shape, BF16),
            pltpu.VMEM(shift.shape, BF16),
            pltpu.VMEM(bias.shape, BF16),
            dma((6,)), dma((3,)), dma((2,)), dma((6,)), dma((6,)),
        ],
        compiler_params=exchange(layer, QKV_MIB),
        name=f'qkv_{layer}',
    )(*map(pin, (positions, freq, h, gain, shift, bias, w, kc, vc)))


def attend_kernel(layer, sparse, pos_hbm, heads_ref, kb, vb, *rest):
    aside, rest = rest[:2], rest[2:]
    ko_ref, vo_ref, o_ref, ml_ref, pos_ref, mref, lref, slot_of, keep_of, tiles, psem, ssem, tsem, *late = rest
    early = SEQS - LATE_SEQS if late else SEQS
    tp, sp, x, c = place()
    steps = SEQS // CHUNK
    copy_in([(pos_hbm, pos_ref)], psem)

    def save(bufs, skip, i, n):
        return pltpu.make_async_copy(bufs[n].at[pl.ds(i * CHUNK - skip, CHUNK)], (ko_ref, vo_ref)[n].at[layer, pl.ds(i * CHUNK, CHUNK)], ssem.at[n, i])

    def place_of(b):
        t = pos_ref[b] - sp * SLOTS
        inside = jnp.logical_and(t >= 0, t < SLOTS)
        t = jnp.clip(t, 0, SLOTS - 1)
        return t, inside, pl.multiple_of((t // 4) * (4 * KVL), 4 * KVL)

    def patch(b, n):
        base = place_of(b)[2]
        return pltpu.make_async_copy(tiles.at[n, b], (ko_ref, vo_ref)[n].at[layer, b, pl.ds(base, 4 * KVL)], tsem.at[n])

    if late:
        lk, lv, late_sem = late
        late_loads = cache_copies(layer, *aside, lk, lv, late_sem, LATE)
        for copy in late_loads:
            copy.start()
    for i in range(early // CHUNK):
        for n in range(2):
            save((kb, vb), 0, i, n).start()
    row = lax.broadcasted_iota(jnp.int32, (HEADS, ROWS), 0)
    col = lax.broadcasted_iota(jnp.int32, (HEADS, ROWS), 1)
    slot = sp * SLOTS + col // KVL
    slot_of[...] = jnp.where(lax.rem(col, KVL) == row // GROUP, slot, jnp.int32(1 << 30))
    if sparse:
        block = slot // BLOCK_SIZE
        vertical = lax.rem(block + tp * HEADS + row + 1, VERT_STRIDE) == 0
        keep_of[...] = jnp.where(vertical, jnp.int32(1 << 20), block)
    mref[...] = jnp.zeros_like(mref)
    lref[...] = jnp.ones_like(lref)
    lane = lax.broadcasted_iota(jnp.int32, (HEADS, HEAD), 1)
    row16 = lax.broadcasted_iota(jnp.int32, (4 * KVL, HEAD), 0)

    pltpu.make_async_copy(pos_hbm, pos_ref, psem.at[0]).wait()

    def repeat(part):
        return jnp.concatenate([jnp.broadcast_to(part[kv:kv + 1], (GROUP, HEAD)) for kv in range(KVL)], axis=0)

    def body(bufs, skip, i, _):
        kb, vb = bufs
        for first in range(0, CHUNK, 4):
            ids = [i * CHUNK + first + s for s in range(4)]
            keeps, hits, scores, news = [], [], [], []
            for b in ids:
                q = heads_ref[pl.ds(b, HEADS, stride=SEQS), :]
                new = heads_ref[pl.ds(HEADS * SEQS + b, 2 * KVL, stride=SEQS), :]
                raw = lax.dot_general(q.astype(BF16), kb[b - skip], (((1,), (1,)), ((), ())), preferred_element_type=F32)
                pos = pos_ref[b]
                keep = slot_of[...] <= pos
                hit = slot_of[...] == pos
                if sparse:
                    keep = jnp.logical_and(keep, pos // BLOCK_SIZE - keep_of[...] < LOCAL_BLOCKS)
                raw = jnp.where(hit, rowsum(q * repeat(new[:KVL])), raw)
                keeps.append(keep)
                hits.append(hit)
                news.append(new)
                scores.append(jnp.where(keep, raw * (1.0 / HEAD), MASKED))
            weights, added = [], []
            for b, keep, hit, score in zip(ids, keeps, hits, scores):
                peak = jnp.max(score, axis=1, keepdims=True)
                weight = jnp.where(keep, jnp.exp(score - peak), 0.0)
                mref[...] = jnp.where(lane == b, peak, mref[...])
                lref[...] = jnp.where(lane == b, rowsum(weight), lref[...])
                weight = weight.astype(BF16).astype(F32)
                added.append(rowsum(jnp.where(hit, weight, 0.0)))
                weights.append(jnp.where(hit, 0.0, weight).astype(BF16))
            for b, weight, extra, new in zip(ids, weights, added, news):
                o_ref[pl.ds(b, HEADS, stride=SEQS), :] = dot(weight, vb[b - skip]) + extra * repeat(new[KVL:])
            for b, new in zip(ids, news):
                t, inside, base = place_of(b)
                hit = jnp.logical_and(row16 // KVL == lax.rem(t, 4), inside)
                for n, buf in enumerate((kb, vb)):
                    fresh = jnp.concatenate([new[n * KVL:(n + 1) * KVL]] * 4, axis=0)
                    tiles[n, b] = jnp.where(hit, fresh, buf[b - skip, pl.ds(base, 4 * KVL), :].astype(F32)).astype(BF16)
        for n in range(2):
            save(bufs, skip, i, n).wait()
        for s in range(CHUNK):
            for n in range(2):
                patch(i * CHUNK + s, n).start()
        return 0

    lax.fori_loop(0, early // CHUNK, functools.partial(body, (kb, vb), 0), 0)
    if late:
        for copy in late_loads:
            copy.wait()
        for i in range(early // CHUNK, steps):
            for n in range(2):
                save((lk, lv), early, i, n).start()
        lax.fori_loop(early // CHUNK, steps, functools.partial(body, (lk, lv), early), 0)
    for kv in range(KVL):
        ml_ref[kv, 0:GROUP] = mref[kv * GROUP:(kv + 1) * GROUP]
        ml_ref[kv, GROUP:2 * GROUP] = lref[kv * GROUP:(kv + 1) * GROUP]

    for n in range(2):
        pltpu.make_async_copy(tiles.at[n], (ko_ref, vo_ref)[n].at[layer, :, pl.ds(0, 4 * KVL)], tsem.at[n]).wait()


def attend(layer, positions, heads, kb, vb, shape, *aside):
    cache = jax.ShapeDtypeStruct(shape, BF16)
    dma = pltpu.SemaphoreType.DMA
    return pl.pallas_call(
        functools.partial(attend_kernel, layer, layer == 0),
        out_shape=(cache, cache, kept((HEADS * SEQS, HEAD), F32), kept((KVL, 2 * GROUP, HEAD), F32)),
        in_specs=[HBM, VM, VM, VM, HBM, HBM],
        out_specs=(HBM, HBM, VM, VM),
        scratch_shapes=[
            pltpu.SMEM((SEQS,), jnp.int32),
            pltpu.VMEM((HEADS, HEAD), F32),
            pltpu.VMEM((HEADS, HEAD), F32),
            pltpu.VMEM((HEADS, ROWS), jnp.int32),
            pltpu.VMEM((HEADS, ROWS), jnp.int32),
            pltpu.VMEM((2, SEQS, 4 * KVL, HEAD), BF16),
            dma((1,)), dma((2, SEQS // CHUNK)), dma((2,)),
        ] + ([] if layer else [pltpu.VMEM((LATE_SEQS, ROWS, HEAD), BF16)] * 2 + [dma((2,))]),
        input_output_aliases={4: 0, 5: 1} if layer else {},
        compiler_params=pltpu.CompilerParams(vmem_limit_bytes=ATTEND_MIB * MIB),
        name=f'attend_{layer}',
    )(pin(positions), *map(near, (heads, kb, vb)), *map(pin, aside))


def mlp_kernel(layer, last, ahead, o_ref, ml_ref, h_ref, gain_ref, shift_ref, bd_ref, bu_ref, bn_ref, wd_ref, wu_ref, wn_ref, *rest):
    if not last:
        rows_ref, freq_ref, bq_ref, wq_ref, kc_ref, vc_ref, out_ref, heads_out, k_out, v_out = rest[:10]
        heads, cos, sin, k_s, q_s, q_r = rest[-6:]
        rest = rest[10:-6]
    else:
        out_ref, rest = rest[0], rest[1:]
    (
        wu, wn, mls, mlx, fromcore, tosend, kept, fromx, mine, other, ob, part, ra, rb, xs, u, mf, mp, mb, ps, acc, st, mo,
        wsem, o_s, o_r, m_s, m_r, c_s, c_r, t_s, t_r,
    ) = rest
    tp, sp, x, c = place()
    y = tp
    core_peer = {'sp': sp + 1 - 2 * c}
    x_peer = {'sp': 2 * (1 - x) + 1 - c}
    y_peer = {'tp': 1 - tp, 'sp': 2 * x + 1 - c}
    c = lax.rem(c + x + y, 2)
    oc, ox, oy = 1 - c, 1 - x, 1 - y
    quarter = [2 * ox + oy, 2 * ox + y, 2 * x + oy, 2 * x + y]

    def turn(k):
        far, near = 1 - k // 2, k // 2
        return 2 * (far * ox + near * x) + (1 - k % 2) * oy + k % 2 * y

    def cols_of(k):
        return block(c * 4 + turn(k), UP_N)

    def load_dense(k):
        return pltpu.make_async_copy(wd_ref.at[layer, block(x, DENSE_K), cols_of(k)], wu.at[UP_STEPS - 1, pl.ds(k * DENSE_K, DENSE_K)], wsem.at[k])

    def load_up(j):
        cols = block((2 * x + c) * UP_STEPS + j, UP_N)
        return pltpu.make_async_copy(wu_ref.at[layer, :, cols], wu.at[j], wsem.at[4 + j])

    def load_down(k):
        rows = block(x, DOWN_K)
        to = wn.at[k] if k < ahead else wu.at[k - ahead, pl.ds(0, DOWN_K)]
        return pltpu.make_async_copy(wn_ref.at[layer, rows, cols_of(k)], to, wsem.at[4 + UP_STEPS + k])

    def down_half(k, half):
        rows = block(half, HALF_K)
        return dot(mb[:, rows], wn[k, rows] if k < ahead else wu[k - ahead, rows])

    def load_next(j):
        return load_qkv(layer + 1, c, wq_ref, wu.at[pl.ds(4, 3)], wsem, j)

    for k in range(OUT_STEPS):
        load_dense(k).start()
    for j in range(UP_STEPS - 1):
        load_up(j).start()
    for k in range(ahead):
        load_down(k).start()
    if not last:
        cache = cache_copies(layer + 1, kc_ref, vc_ref, k_out, v_out, k_s)
        for copy in cache:
            copy.start()
    everyone = [lax.rem(tp * 4 + sp + r, 8) for r in range(1, 8)]
    enter([{'tp': peer // 4, 'sp': lax.rem(peer, 4)} for peer in everyone])
    waits = []

    def swap(i, src, dst, peer):
        copy = remote(src, dst, o_s.at[i], o_r.at[i], peer)
        copy.start()
        waits.append(copy)
        return copy

    stats = swap(4, ml_ref, mls, core_peer)
    slabs = [None, None]
    for n, xd in enumerate((ox, x)):
        src = o_ref.at[pl.ds((2 * xd + oc) * GROUP, GROUP)]
        slabs[n] = swap(n, src, fromcore.at[n], core_peer)

    def columns(rows):
        return jnp.concatenate(rows + [jnp.zeros((HEAD - GROUP * len(rows), HEAD), F32)], axis=0).T[:SEQS]

    def merge(one, two):
        top = jnp.maximum(one[:GROUP], two[:GROUP])
        first, second = jnp.exp(one[:GROUP] - top), jnp.exp(two[:GROUP] - top)
        return first, second, top, first * one[GROUP:] + second * two[GROUP:]

    stats.wait_recv()
    rows = []
    for n, xd in enumerate((ox, x)):
        first, second, top, total = merge(ml_ref[2 * xd + c], mls[2 * xd + c])
        rows += [first, second]
        mlx[n] = jnp.concatenate([top, total], axis=0)
    cross_ml = swap(5, mlx.at[0], mlx.at[2], x_peer)
    scale = columns(rows)
    for n, (xd, out) in enumerate(((ox, tosend), (x, kept))):
        slabs[n].wait_recv()
        kv = 2 * xd + c
        for g in range(GROUP):
            i = 2 * n * GROUP + g
            out[g] = o_ref[kv * GROUP + g] * scale[:, i:i + 1] + fromcore[n, g] * scale[:, i + GROUP:i + GROUP + 1]
        if n == 0:
            cross = swap(2, tosend, fromx, x_peer)
    if not last:
        rope_tables(rows_ref, freq_ref, cos, sin)
    cross_ml.wait_recv()
    first, second, _, total = merge(mlx[1], mlx[2])
    scale = columns([first / total, second / total])
    cross.wait_recv()
    for g in range(GROUP):
        val = (kept[g] * scale[:, g:g + 1] + fromx[g] * scale[:, g + GROUP:g + GROUP + 1]).astype(BF16)
        mine[g] = val.astype(F32)
        ob[:, block(c * GROUP + g, HEAD)] = val
    share = swap(3, mine, other, core_peer)
    def dense_half(k, half):
        return dot(ob[:, block(half, UP_N)], wu[UP_STEPS - 1, block(2 * k + half, UP_N)])

    for k in range(OUT_STEPS):
        load_dense(k).wait()
        ps[k] = dense_half(k, c)
    share.wait_recv()
    for g in range(GROUP):
        ob[:, block(oc * GROUP + g, HEAD)] = other[g].astype(BF16)

    own = (c * 4 + quarter[K3]) * 2

    def all_reduce(ph, chunk, residual, bias_ref, after=lambda: None, stats=True):
        def post(i, src, dst, peer):
            copy = remote(src, dst, c_s.at[ph, int(5 < i < STRIP)], c_r.at[ph, i], peer)
            copy.start()
            return copy

        def keep(k):
            val = chunk(k)
            part[ph, k, A] = val[:, :PIECE]
            part[ph, k, B] = val[:, PIECE:]

        def strips(i, src, dst, peer):
            return [post((i, i + STRIP)[n], src.at[:, cols], dst.at[:, cols], peer) for n, cols in enumerate(STRIPS)]

        keep(K0)
        a0 = strips(0, part.at[ph, K0, A], ra.at[ph, K0], x_peer)
        b0 = strips(1, part.at[ph, K0, B], rb.at[ph, K0], y_peer)
        keep(K1)
        a1 = post(2, part.at[ph, K1, A], ra.at[ph, K1], x_peer)
        keep(K2)
        b1 = post(3, part.at[ph, K2, B], rb.at[ph, K1], y_peer)
        keep(K3)
        after()
        a2, b2 = [], []
        for n, cols in enumerate(STRIPS):
            b0[n].wait_recv()
            part[ph, K1, B, :, cols] += rb[ph, K0, :, cols]
            ref = part.at[ph, K1, B, :, cols]
            b2.append(post((4, 4 + STRIP)[n], ref, rb.at[ph, K2, :, cols], x_peer))
            a0[n].wait_recv()
            part[ph, K2, A, :, cols] += ra[ph, K0, :, cols]
            ref = part.at[ph, K2, A, :, cols]
            a2.append(post((5, 5 + STRIP)[n], ref, ra.at[ph, K2, :, cols], y_peer))
        for half, (first, second, landed) in enumerate(((a1, a2, ra), (b1, b2, rb))):
            for copy in (first, *second):
                copy.wait_recv()
            cols = block(own + half, PIECE)
            full = part[ph, K3, half] + landed[ph, K1] + landed[ph, K2]
            xs[ph, own + half] = (residual(half, cols) + full + bias_ref[layer:layer + 1, cols].astype(F32)).astype(BF16).astype(F32)
        if stats:
            send_moments(ph)
        gather = {}
        for n in range(3):
            for half in range(2):
                peer = core_peer if n == 2 else (x_peer, y_peer)[(n + half) % 2]
                mine_ref = xs.at[ph, own + half]
                gather[half, n] = post(6 + 3 * half + n, mine_ref, mine_ref, peer)
        base = c * 8
        from_x = base + quarter[K1] * 2
        from_y = base + quarter[K2] * 2
        far = base + quarter[K0] * 2

        def forward(i, piece, peer):
            ref = xs.at[ph, piece]
            return post(i, ref, ref, peer)

        sent = {}

        def pump(step):
            if step == 0:
                gather[A, K0].wait_recv()
                sent[A_FAR] = forward(A_FAR, from_x, y_peer)
                sent[A_X] = forward(A_X, from_x, core_peer)
                gather[B, K0].wait_recv()
                sent[B_FAR] = forward(B_FAR, from_y + 1, x_peer)
                sent[B_Y] = forward(B_Y, from_y + 1, core_peer)
            elif step == 1:
                gather[A, K1].wait_recv()
                sent[A_Y] = forward(A_Y, from_y, core_peer)
                gather[B, K1].wait_recv()
                sent[B_X] = forward(B_X, from_x + 1, core_peer)
            else:
                sent[A_FAR].wait_recv()
                sent[A_LAST] = forward(A_LAST, far, core_peer)
                sent[B_FAR].wait_recv()
                sent[B_LAST] = forward(B_LAST, far + 1, core_peer)

        def arrive(group):
            for copy in {0: [gather[A, K2], gather[B, K2]], 1: [sent.get(i) for i in (A_X, B_Y, A_Y, B_X)], 2: [sent.get(i) for i in (A_LAST, B_LAST)]}[group]:
                copy.wait_recv()

        return pump, arrive

    me = tp * 4 + sp

    def send_moments(ph):
        a, b = xs[ph, own], xs[ph, own + 1]
        count = 2 * PIECE
        mean = (rowsum(a) + rowsum(b)) * (1.0 / count)
        spread = rowsum(jnp.square(a - mean)) + rowsum(jnp.square(b - mean))
        lane = lax.broadcasted_iota(jnp.int32, (SEQS, HEAD), 1)
        both = jnp.where(lane == 0, mean, jnp.where(lane == 1, spread, 0.0))
        st[ph, me] = jnp.concatenate([both, jnp.zeros((HEAD - SEQS, HEAD), F32)], axis=0).T[:8]
        for r in range(1, 8):
            peer = lax.rem(me + r, 8)
            remote(st.at[ph, me], st.at[ph, me], t_s.at[ph], t_r.at[ph], {'tp': peer // 4, 'sp': lax.rem(peer, 4)}).start()

    def moments(ph):
        remote(st.at[ph, pl.ds(0, 7)], st.at[ph, pl.ds(0, 7)], t_s.at[ph], t_r.at[ph], x_peer).wait()
        parts = [st[ph, i] for i in range(8)]
        mean = sum(p[0:1] for p in parts) * 0.125
        spread = sum(p[1:2] + (2.0 * PIECE) * jnp.square(p[0:1] - mean) for p in parts)
        scale = lax.rsqrt(spread * (1.0 / MODEL) + NORM_EPS)
        table = jnp.concatenate([mean, scale, jnp.zeros((HEAD - 2, HEAD), F32)], axis=0).T[:SEQS]
        mo[...] = table

    def slices(group):
        if group == 0:
            return c * 4 + quarter[K3], oc * 4 + quarter[K3]
        if group == 2:
            return c * 4 + quarter[K0], oc * 4 + quarter[K0]
        return [core * 4 + quarter[k] for core in (c, oc) for k in (1, 2)]

    def norm_group(ph, row, norm, group):
        mean, scale = mo[:, 0:1], mo[:, 1:2]
        for n, index in enumerate(slices(group)):
            for half in range(2):
                cols = block(2 * index + half, PIECE)
                gain, shift = gain_ref[row, norm:norm + 1, cols].astype(F32), shift_ref[row, norm:norm + 1, cols].astype(F32)
                at = (2 * n + half) * PIECE
                u[:, at:at + PIECE] = ((xs[ph, 2 * index + half] - mean) * scale * gain + shift).astype(BF16)

    def product(group, slot):
        total = 0.0
        for n, index in enumerate(slices(group)):
            rows = block(index, UP_N)
            total = total + dot(u[:, n * 512:(n + 1) * 512], wu[slot, rows])
        return total

    def normed_product(ph, row, norm, stages, first, count, wait, finish_step):
        pump, arrive = stages

        def add(group, low, high):
            def step(j, _):
                if group == 0:
                    wait(j)
                    acc[j] = product(group, first + j)
                else:
                    acc[j] += product(group, first + j)
                return 0

            lax.fori_loop(low, high, step, 0, unroll=True)

        half = count // 2 + 1
        moments(ph)
        arrive(0)
        norm_group(ph, row, norm, 0)
        pump(0)
        add(0, 0, half)
        pump(1)
        add(0, half, count)
        arrive(1)
        norm_group(ph, row, norm, 1)
        add(1, 0, half)
        pump(2)
        add(1, half, count)
        arrive(2)
        norm_group(ph, row, norm, 2)
        finish_step(lambda j: acc[j] + product(2, first + j))

    def dense_chunk(k):
        return ps[k] + dense_half(k, oc)

    stages = all_reduce(0, dense_chunk, lambda half, cols: h_ref[:, cols].astype(F32), bd_ref, load_up(UP_STEPS - 1).start)
    take = (lax.broadcasted_iota(jnp.int32, (2 * HEAD, HEAD), 0) == 2 * lax.broadcasted_iota(jnp.int32, (2 * HEAD, HEAD), 1)).astype(BF16)
    even = lax.rem(lax.broadcasted_iota(jnp.int32, (SEQS, UP_N), 1), 2) == 0

    def share_m(j):
        return remote(mf.at[j], mp.at[j], m_s.at[0], m_r.at[0], core_peer)

    def up_step(full, j):
        cols = block((2 * x + c) * UP_STEPS + j, UP_N)
        val = full(j) + bu_ref[layer:layer + 1, cols].astype(F32)
        gate = jnp.minimum(val, GELU_LIMIT)
        gate = gate * (1.0 / (1.0 + jnp.exp(-1.702 * gate)))
        linear = jnp.clip(val, -GELU_LIMIT, GELU_LIMIT) + 1.0
        mixed = jnp.where(even, gate * pltpu.roll(linear, UP_N - 1, 1), 0.0).astype(BF16)
        packed = jnp.concatenate([dot(mixed[:, i:i + 2 * HEAD], take) for i in range(0, UP_N, 2 * HEAD)], axis=1)
        mf[j] = packed
        share_m(j).start()
        mb[:, block(c * UP_STEPS + j, PIECE)] = packed.astype(BF16)

        if j < 4 - ahead:
            load_down(j + ahead).start()
        if not last and j >= 4:
            load_next(j - 4).start()

    def up_steps(full):
        for j in range(UP_STEPS):
            up_step(full, j)

    normed_product(0, layer, 1, stages, 0, UP_STEPS, lambda j: load_up(j).wait(), up_steps)
    for k in range(OUT_STEPS):
        load_down(k).wait()
        ps[k] = down_half(k, c)
    remote(mf, mp, m_s.at[0], m_r.at[0], core_peer).wait()
    for j in range(UP_STEPS):
        mb[:, block(oc * UP_STEPS + j, PIECE)] = mp[j].astype(BF16)

    def down_chunk(k):
        return ps[k] + down_half(k, oc)

    stages = all_reduce(1, down_chunk, lambda half, cols: xs[0, own + half], bn_ref, stats=not last)
    def write(group):
        for index in slices(group):
            for half in range(2):
                out_ref[:, block(2 * index + half, PIECE)] = xs[1, 2 * index + half].astype(BF16)

    if last:
        pump, arrive = stages
        for group in range(3):
            pump(group)
            if group:
                arrive(group - 1)
                write(group - 1)
        arrive(2)
        write(2)
    else:
        def qkv_steps(full):
            qkv_phase(layer + 1, c, core_peer, full, bq_ref, cos, sin, heads, q_s, q_r, lambda: [write(group) for group in range(3)])

        normed_product(1, layer + 1, 0, stages, 4, 3, lambda j: load_next(j).wait(), qkv_steps)
        heads_out[...] = heads[...]
        for copy in cache:
            copy.wait()
    for ph in range(2):
        for n, pieces in enumerate((6, 14)):
            remote(xs.at[ph, pl.ds(0, pieces)], xs.at[ph, pl.ds(0, pieces)], c_s.at[ph, n], c_r.at[ph, 0], x_peer).wait_send()
    for copy in waits:
        copy.wait_send()


def finish(layer, o, ml, h, gain, shift, bd, bu, bn, wd, wu, wn, *following):
    slab = pltpu.VMEM((GROUP, SEQS, HEAD), F32)
    dma = pltpu.SemaphoreType.DMA
    last = not following
    ahead = 4 if last else 1
    hidden = kept((SEQS, MODEL), BF16)
    table = pltpu.VMEM((SEQS, HEAD), F32)
    return pl.pallas_call(
        functools.partial(mlp_kernel, layer, last, ahead),
        out_shape=hidden if last else (hidden, kept(HEADS_SHAPE, F32), CACHE, CACHE),
        in_specs=[VM] * 8 + [HBM] * 3 + ([] if last else [VM, VM, VM, HBM, HBM, HBM]),
        out_specs=VM if last else (VM, VM, VM, VM),
        scratch_shapes=[
            pltpu.VMEM((UP_STEPS, MODEL, UP_N), BF16),
            pltpu.VMEM((ahead, DOWN_K, 512), BF16),
            pltpu.VMEM((KVL, 2 * GROUP, HEAD), F32),
            pltpu.VMEM((3, 2 * GROUP, HEAD), F32),
            pltpu.VMEM((2, GROUP, SEQS, HEAD), F32),
            slab, slab, slab, slab, slab,
            pltpu.VMEM((SEQS, 1024), BF16),
            pltpu.VMEM((2, 4, 2, SEQS, PIECE), F32),
            pltpu.VMEM((2, 3, SEQS, PIECE), F32),
            pltpu.VMEM((2, 3, SEQS, PIECE), F32),
            pltpu.VMEM((2, 16, SEQS, PIECE), F32),
            pltpu.VMEM((SEQS, 2048), BF16),
            pltpu.VMEM((UP_STEPS, SEQS, 256), F32),
            pltpu.VMEM((UP_STEPS, SEQS, 256), F32),
            pltpu.VMEM((SEQS, DOWN_K), BF16),
            pltpu.VMEM((4, SEQS, 512), F32),
            pltpu.VMEM((UP_STEPS, SEQS, UP_N), F32),
            pltpu.VMEM((2, 8, 8, HEAD), F32),
            pltpu.VMEM((SEQS, HEAD), F32),
            dma((8 + UP_STEPS,)), dma((6,)), dma((6,)), dma((1,)), dma((1,)), dma((2, 2)), dma((2, STRIP + 6)), dma((2,)), dma((2,)),
        ] + ([] if last else [pltpu.VMEM(HEADS_SHAPE, F32), table, table, dma((2,)), dma((6,)), dma((6,))]),
        compiler_params=exchange(2 + layer, (60 if last else MLP_MIB)),
        name=f'mlp_{layer}',
    )(near(o), near(ml), near(h) if last else pin(h), *map(pin, (gain, shift, bd, bu, bn, wd, wu, wn)), *map(near, following[:1]), *map(pin, following[1:]))


def solution(mesh):
    cache_spec = P(None, 'dp', 'sp', 'tp', None)
    rows, bias, cols = P(None, 'tp', None), P(None, 'tp'), P(None, None, 'tp')
    in_specs = (P('dp'), P('dp'), cache_spec, cache_spec, P(), P(), cols, bias, rows, P(), cols, bias, rows, P())
    out_specs = (P('dp'), cache_spec, cache_spec)

    def device_step(hidden, positions, k_cache, v_cache, ln_gain, ln_bias, w_qkv, b_qkv, w_dense, b_dense, w_up, b_up, w_down, b_down):
        freq = ROPE_THETA ** (-np.arange(HEAD // 2) * (2.0 / HEAD))
        freq = jnp.asarray(np.tile(freq, 2)[None].astype(np.float32))
        shape = k_cache.shape
        flat = (2, SEQS, ROWS, HEAD)
        kc = k_cache.reshape(flat)
        vc = v_cache.reshape(flat)
        done = ()
        heads, kb, vb, rows = project(0, positions, freq, hidden, ln_gain, ln_bias, b_qkv, w_qkv, kc, vc)
        for layer in range(2):
            ko, vo, o, ml = attend(layer, positions, heads.reshape(-1, HEAD), kb, vb, flat, *(done or (kc, vc)))
            done = (ko, vo)
            following = () if layer else (rows, freq, b_qkv, w_qkv, kc, vc)
            out = finish(layer, o.reshape(HEADS, SEQS, HEAD), ml, hidden, ln_gain, ln_bias, b_dense, b_up, b_down, w_dense, w_up, w_down, *following)
            hidden, heads, kb, vb = out if following else (out, None, None, None)
        return hidden, done[0].reshape(shape), done[1].reshape(shape)

    return jax.shard_map(device_step, mesh=mesh, in_specs=in_specs, out_specs=out_specs, check_vma=False)
```

```python
import functools

import jax
import jax.numpy as jnp
import numpy as np
from jax import lax
from jax.experimental import pallas as pl
from jax.experimental.pallas import tpu as pltpu
from jax.sharding import PartitionSpec as P

BLOCK_SIZE = 64
LOCAL_BLOCKS = 16
VERT_STRIDE = 8
ROPE_THETA = 1000000.0
GELU_LIMIT = 20.0
NORM_EPS = 0.00001
MASKED = -1e30

SEQS = 64
MODEL = 4096
HEAD = 128
KVL = 4
GROUP = 4
HEADS = KVL * GROUP
SLOTS = 128
ROWS = SLOTS * KVL
QKV_N = (GROUP + 2) * HEAD
UP_N = 512
UP_STEPS = 7
DOWN_K = 3584
HALF_K = DOWN_K // 2
DENSE_K = 1024
OUT_STEPS = 4
PIECE = 256
CHUNK = 8
MIB = 1024 * 1024
QKV_MIB = 20
ATTEND_MIB = 8
MLP_MIB = 43

A, B = range(2)
K0, K1, K2, K3 = range(4)
STRIP = 20
LATE_SEQS = 16
EARLY = pl.ds(0, SEQS - LATE_SEQS)
LATE = pl.ds(SEQS - LATE_SEQS, LATE_SEQS)
STRIPS = (pl.ds(0, HEAD), pl.ds(HEAD, HEAD))
A_FAR, B_FAR, A_X, B_Y, A_Y, B_X, A_LAST, B_LAST = range(12, STRIP)

F32 = jnp.float32
BF16 = jnp.bfloat16
MESH = pl.DeviceIdType.MESH
VM = pl.BlockSpec(memory_space=pltpu.VMEM)
SM = pl.BlockSpec(memory_space=pltpu.SMEM)
HBM = pl.BlockSpec(memory_space=pltpu.HBM)


def kept(shape, dtype):
    return pltpu.VMEM(shape, dtype)


def pin(x):
    return pltpu.with_memory_space_constraint(x, pltpu.HBM)


def near(x):
    return pltpu.with_memory_space_constraint(x, pltpu.VMEM)


def exchange(number, mib):
    return pltpu.CompilerParams(collective_id=number, has_side_effects=True, vmem_limit_bytes=mib * MIB)


def rowsum(a):
    return jnp.sum(a, axis=1, keepdims=True)


def block(index, size):
    return pl.ds(pl.multiple_of(index * size, size), size)


def dot(a, b):
    return jnp.dot(a, b, preferred_element_type=F32)


def place():
    sp = lax.axis_index('sp')
    return lax.axis_index('tp'), sp, sp // 2, lax.rem(sp, 2)


def enter(peers):
    barrier = pltpu.get_barrier_semaphore()
    for peer in peers:
        pl.semaphore_signal(barrier, inc=1, device_id=peer, device_id_type=MESH)
    pl.semaphore_wait(barrier, len(peers))


def remote(src, dst, send, recv, peer):
    return pltpu.make_async_remote_copy(src_ref=src, dst_ref=dst, send_sem=send, recv_sem=recv, device_id=peer, device_id_type=MESH)


def norm_into(pieces, gain, shift, out_ref):
    width = pieces[0]().shape[1]
    total = sum(rowsum(p()) for p in pieces)
    mean = total * (1.0 / MODEL)
    square = sum(rowsum(jnp.square(p() - mean)) for p in pieces)
    scale = lax.rsqrt(square * (1.0 / MODEL) + NORM_EPS)
    for i, p in enumerate(pieces):
        cols = slice(i * width, (i + 1) * width)
        out_ref[:, cols] = ((p() - mean) * scale * gain(cols) + shift(cols)).astype(BF16)


def position_rows(pos_ref, rows_ref):
    row = lax.broadcasted_iota(jnp.int32, (8, HEAD), 0)
    for first in range(0, SEQS, 8):
        pos = jnp.zeros((8, HEAD), jnp.int32)
        for i in range(8):
            pos = jnp.where(row == i, pos_ref[first + i], pos)
        rows_ref[first:first + 8] = pos


def rope_tables(rows_ref, freq_ref, cos_ref, sin_ref):
    sign = jnp.where(lax.broadcasted_iota(jnp.int32, (SEQS, HEAD), 1) < HEAD // 2, -1.0, 1.0)
    angle = rows_ref[...].astype(F32) * freq_ref[...]
    cos_ref[...] = jnp.cos(angle)
    sin_ref[...] = jnp.sin(angle) * sign


def load_qkv(layer, c, w_ref, wbuf, sem, j):
    cols = block(c * 3 + j, UP_N)
    return pltpu.make_async_copy(w_ref.at[layer, :, cols], wbuf.at[j], sem.at[j])


def qkv_phase(layer, c, partner, product, bias_ref, cos_ref, sin_ref, heads, ssem, rsem, meanwhile=lambda: None):
    sent = []
    for j in range(3):
        cols = block(c * 3 + j, UP_N)
        proj = product(j) + bias_ref[layer:layer + 1, cols].astype(F32)
        for n in range(4):
            local, i = divmod(4 * j + n, GROUP + 2)
            kv = 2 * c + local
            part = proj[:, n * HEAD:(n + 1) * HEAD]
            if i <= GROUP:
                part = part * cos_ref[...] + pltpu.roll(part, HEAD // 2, 1) * sin_ref[...]
            slot = kv * GROUP + i if i < GROUP else HEADS + (i - GROUP) * KVL + kv
            heads[slot] = part.astype(BF16).astype(F32)
            piece = {GROUP - 1: pl.ds(kv * GROUP, GROUP), GROUP: pl.ds(HEADS + kv, 1), GROUP + 1: pl.ds(HEADS + KVL + kv, 1)}.get(i)
            if piece is not None:
                k = len(sent)
                sent.append(remote(heads.at[piece], heads.at[piece], ssem.at[k], rsem.at[k], partner))
                sent[-1].start()
    meanwhile()
    for copy in sent:
        copy.wait()


def copy_in(pairs, sems):
    copies = [pltpu.make_async_copy(src, dst, sems.at[i]) for i, (src, dst) in enumerate(pairs)]
    for copy in copies:
        copy.start()
    return copies


def cache_copies(layer, kc_ref, vc_ref, k_out, v_out, sems, rows=pl.ds(0, SEQS)):
    return [pltpu.make_async_copy(src.at[layer, rows], dst.at[pl.ds(0, rows.size)], sems.at[n]) for n, (src, dst) in enumerate(((kc_ref, k_out), (vc_ref, v_out)))]


def qkv_kernel(
    layer, pos_hbm, freq_hbm, h_hbm, gain_hbm, shift_hbm, bias_hbm, w_ref, kc_ref, vc_ref, out_ref, k_out, v_out, rows_out,
    wbuf, u, heads, cos, sin, pos, freq, h, gain, shift, bias, isem, wsem, ksem, ssem, rsem,
):
    tp, sp, x, c = place()
    small = copy_in([(h_hbm, h), (gain_hbm, gain), (shift_hbm, shift), (pos_hbm, pos), (freq_hbm, freq), (bias_hbm, bias)], isem)
    loads = [load_qkv(layer, c, w_ref, wbuf, wsem, j) for j in range(3)]
    partner = {'sp': sp + 1 - 2 * c}
    for copy in small:
        copy.wait()

    def begin(j, _):
        load_qkv(layer, c, w_ref, wbuf, wsem, j).start()
        return 0

    lax.fori_loop(0, 3, begin, 0)
    for copy in cache_copies(layer, kc_ref, vc_ref, k_out, v_out, ksem, EARLY):
        copy.start()
    norm_into(
        [lambda i=i: h[:, i * 512:(i + 1) * 512].astype(F32) for i in range(8)],
        lambda cols: gain[layer, 0:1, cols].astype(F32),
        lambda cols: shift[layer, 0:1, cols].astype(F32),
        u,
    )
    position_rows(pos, rows_out)
    rope_tables(rows_out, freq, cos, sin)
    enter([partner])

    def product(j):
        loads[j].wait()
        return dot(u[...], wbuf[j])

    qkv_phase(layer, c, partner, product, bias, cos, sin, heads, ssem, rsem)
    out_ref[...] = heads[...]
    for copy in cache_copies(layer, kc_ref, vc_ref, k_out, v_out, ksem, EARLY):
        copy.wait()


HEADS_SHAPE = (HEADS + 2 * KVL, SEQS, HEAD)


CACHE = kept((SEQS, ROWS, HEAD), BF16)


def project(layer, positions, freq, h, gain, shift, bias, w, kc, vc):
    dma = pltpu.SemaphoreType.DMA
    return pl.pallas_call(
        functools.partial(qkv_kernel, layer),
        out_shape=(kept(HEADS_SHAPE, F32), CACHE, CACHE, kept((SEQS, HEAD), jnp.int32)),
        in_specs=[HBM] * 9,
        out_specs=(VM, VM, VM, VM),
        scratch_shapes=[
            pltpu.VMEM((3, MODEL, UP_N), BF16),
            pltpu.VMEM((SEQS, MODEL), BF16),
            pltpu.VMEM(HEADS_SHAPE, F32),
            pltpu.VMEM((SEQS, HEAD), F32),
            pltpu.VMEM((SEQS, HEAD), F32),
            pltpu.SMEM((SEQS,), jnp.int32),
            pltpu.VMEM((1, HEAD), F32),
            pltpu.VMEM((SEQS, MODEL), BF16),
            pltpu.VMEM(gain.shape, BF16),
            pltpu.VMEM(shift.shape, BF16),
            pltpu.VMEM(bias.shape, BF16),
            dma((6,)), dma((3,)), dma((2,)), dma((6,)), dma((6,)),
        ],
        compiler_params=exchange(layer, QKV_MIB),
        name=f'qkv_{layer}',
    )(*map(pin, (positions, freq, h, gain, shift, bias, w, kc, vc)))


def attend_kernel(layer, sparse, pos_hbm, heads_ref, kb, vb, *rest):
    aside, rest = rest[:2], rest[2:]
    ko_ref, vo_ref, o_ref, ml_ref, pos_ref, mref, lref, slot_of, keep_of, tiles, psem, ssem, tsem, *late = rest
    early = SEQS - LATE_SEQS if late else SEQS
    tp, sp, x, c = place()
    steps = SEQS // CHUNK
    copy_in([(pos_hbm, pos_ref)], psem)

    def save(bufs, skip, i, n):
        return pltpu.make_async_copy(bufs[n].at[pl.ds(i * CHUNK - skip, CHUNK)], (ko_ref, vo_ref)[n].at[layer, pl.ds(i * CHUNK, CHUNK)], ssem.at[n, i])

    def place_of(b):
        t = pos_ref[b] - sp * SLOTS
        inside = jnp.logical_and(t >= 0, t < SLOTS)
        t = jnp.clip(t, 0, SLOTS - 1)
        return t, inside, pl.multiple_of((t // 4) * (4 * KVL), 4 * KVL)

    def patch(b, n):
        base = place_of(b)[2]
        return pltpu.make_async_copy(tiles.at[n, b], (ko_ref, vo_ref)[n].at[layer, b, pl.ds(base, 4 * KVL)], tsem.at[n])

    if late:
        lk, lv, late_sem = late
        late_loads = cache_copies(layer, *aside, lk, lv, late_sem, LATE)
        for copy in late_loads:
            copy.start()
    for i in range(early // CHUNK):
        for n in range(2):
            save((kb, vb), 0, i, n).start()
    row = lax.broadcasted_iota(jnp.int32, (HEADS, ROWS), 0)
    col = lax.broadcasted_iota(jnp.int32, (HEADS, ROWS), 1)
    slot = sp * SLOTS + col // KVL
    slot_of[...] = jnp.where(lax.rem(col, KVL) == row // GROUP, slot, jnp.int32(1 << 30))
    if sparse:
        block = slot // BLOCK_SIZE
        vertical = lax.rem(block + tp * HEADS + row + 1, VERT_STRIDE) == 0
        keep_of[...] = jnp.where(vertical, jnp.int32(1 << 20), block)
    mref[...] = jnp.zeros_like(mref)
    lref[...] = jnp.ones_like(lref)
    lane = lax.broadcasted_iota(jnp.int32, (HEADS, HEAD), 1)
    row16 = lax.broadcasted_iota(jnp.int32, (4 * KVL, HEAD), 0)

    pltpu.make_async_copy(pos_hbm, pos_ref, psem.at[0]).wait()

    def repeat(part):
        return jnp.concatenate([jnp.broadcast_to(part[kv:kv + 1], (GROUP, HEAD)) for kv in range(KVL)], axis=0)

    def body(bufs, skip, i, _):
        kb, vb = bufs
        for first in range(0, CHUNK, 4):
            ids = [i * CHUNK + first + s for s in range(4)]
            keeps, hits, scores, news = [], [], [], []
            for b in ids:
                q = heads_ref[pl.ds(b, HEADS, stride=SEQS), :]
                new = heads_ref[pl.ds(HEADS * SEQS + b, 2 * KVL, stride=SEQS), :]
                raw = lax.dot_general(q.astype(BF16), kb[b - skip], (((1,), (1,)), ((), ())), preferred_element_type=F32)
                pos = pos_ref[b]
                keep = slot_of[...] <= pos
                hit = slot_of[...] == pos
                if sparse:
                    keep = jnp.logical_and(keep, pos // BLOCK_SIZE - keep_of[...] < LOCAL_BLOCKS)
                raw = jnp.where(hit, rowsum(q * repeat(new[:KVL])), raw)
                keeps.append(keep)
                hits.append(hit)
                news.append(new)
                scores.append(jnp.where(keep, raw * (1.0 / HEAD), MASKED))
            weights, added = [], []
            for b, keep, hit, score in zip(ids, keeps, hits, scores):
                peak = jnp.max(score, axis=1, keepdims=True)
                weight = jnp.where(keep, jnp.exp(score - peak), 0.0)
                mref[...] = jnp.where(lane == b, peak, mref[...])
                lref[...] = jnp.where(lane == b, rowsum(weight), lref[...])
                weight = weight.astype(BF16).astype(F32)
                added.append(rowsum(jnp.where(hit, weight, 0.0)))
                weights.append(jnp.where(hit, 0.0, weight).astype(BF16))
            for b, weight, extra, new in zip(ids, weights, added, news):
                o_ref[pl.ds(b, HEADS, stride=SEQS), :] = dot(weight, vb[b - skip]) + extra * repeat(new[KVL:])
            for b, new in zip(ids, news):
                t, inside, base = place_of(b)
                hit = jnp.logical_and(row16 // KVL == lax.rem(t, 4), inside)
                for n, buf in enumerate((kb, vb)):
                    fresh = jnp.concatenate([new[n * KVL:(n + 1) * KVL]] * 4, axis=0)
                    tiles[n, b] = jnp.where(hit, fresh, buf[b - skip, pl.ds(base, 4 * KVL), :].astype(F32)).astype(BF16)
        for n in range(2):
            save(bufs, skip, i, n).wait()
        for s in range(CHUNK):
            for n in range(2):
                patch(i * CHUNK + s, n).start()
        return 0

    lax.fori_loop(0, early // CHUNK, functools.partial(body, (kb, vb), 0), 0)
    if late:
        for copy in late_loads:
            copy.wait()
        for i in range(early // CHUNK, steps):
            for n in range(2):
                save((lk, lv), early, i, n).start()
        lax.fori_loop(early // CHUNK, steps, functools.partial(body, (lk, lv), early), 0)
    for kv in range(KVL):
        ml_ref[kv, 0:GROUP] = mref[kv * GROUP:(kv + 1) * GROUP]
        ml_ref[kv, GROUP:2 * GROUP] = lref[kv * GROUP:(kv + 1) * GROUP]

    for n in range(2):
        pltpu.make_async_copy(tiles.at[n], (ko_ref, vo_ref)[n].at[layer, :, pl.ds(0, 4 * KVL)], tsem.at[n]).wait()


def attend(layer, positions, heads, kb, vb, shape, *aside):
    cache = jax.ShapeDtypeStruct(shape, BF16)
    dma = pltpu.SemaphoreType.DMA
    return pl.pallas_call(
        functools.partial(attend_kernel, layer, layer == 0),
        out_shape=(cache, cache, kept((HEADS * SEQS, HEAD), F32), kept((KVL, 2 * GROUP, HEAD), F32)),
        in_specs=[HBM, VM, VM, VM, HBM, HBM],
        out_specs=(HBM, HBM, VM, VM),
        scratch_shapes=[
            pltpu.SMEM((SEQS,), jnp.int32),
            pltpu.VMEM((HEADS, HEAD), F32),
            pltpu.VMEM((HEADS, HEAD), F32),
            pltpu.VMEM((HEADS, ROWS), jnp.int32),
            pltpu.VMEM((HEADS, ROWS), jnp.int32),
            pltpu.VMEM((2, SEQS, 4 * KVL, HEAD), BF16),
            dma((1,)), dma((2, SEQS // CHUNK)), dma((2,)),
        ] + ([] if layer else [pltpu.VMEM((LATE_SEQS, ROWS, HEAD), BF16)] * 2 + [dma((2,))]),
        input_output_aliases={4: 0, 5: 1} if layer else {},
        compiler_params=pltpu.CompilerParams(vmem_limit_bytes=ATTEND_MIB * MIB),
        name=f'attend_{layer}',
    )(pin(positions), *map(near, (heads, kb, vb)), *map(pin, aside))


def mlp_kernel(layer, last, ahead, o_ref, ml_ref, h_ref, gain_ref, shift_ref, bd_ref, bu_ref, bn_ref, wd_ref, wu_ref, wn_ref, *rest):
    if not last:
        rows_ref, freq_ref, bq_ref, wq_ref, kc_ref, vc_ref, out_ref, heads_out, k_out, v_out = rest[:10]
        heads, cos, sin, k_s, q_s, q_r = rest[-6:]
        rest = rest[10:-6]
    else:
        out_ref, rest = rest[0], rest[1:]
    (
        wu, wn, mls, mlx, fromcore, tosend, kept, fromx, mine, other, ob, part, ra, rb, xs, u, mf, mp, mb, ps, acc, st, mo,
        wsem, o_s, o_r, m_s, m_r, c_s, c_r, t_s, t_r,
    ) = rest
    tp, sp, x, c = place()
    y = tp
    core_peer = {'sp': sp + 1 - 2 * c}
    x_peer = {'sp': 2 * (1 - x) + 1 - c}
    y_peer = {'tp': 1 - tp, 'sp': 2 * x + 1 - c}
    c = lax.rem(c + x + y, 2)
    oc, ox, oy = 1 - c, 1 - x, 1 - y
    quarter = [2 * ox + oy, 2 * ox + y, 2 * x + oy, 2 * x + y]

    def turn(k):
        far, near = 1 - k // 2, k // 2
        return 2 * (far * ox + near * x) + (1 - k % 2) * oy + k % 2 * y

    def cols_of(k):
        return block(c * 4 + turn(k), UP_N)

    def load_dense(k):
        return pltpu.make_async_copy(wd_ref.at[layer, block(x, DENSE_K), cols_of(k)], wu.at[UP_STEPS - 1, pl.ds(k * DENSE_K, DENSE_K)], wsem.at[k])

    def load_up(j):
        cols = block((2 * x + c) * UP_STEPS + j, UP_N)
        return pltpu.make_async_copy(wu_ref.at[layer, :, cols], wu.at[j], wsem.at[4 + j])

    def load_down(k):
        rows = block(x, DOWN_K)
        to = wn.at[k] if k < ahead else wu.at[k - ahead, pl.ds(0, DOWN_K)]
        return pltpu.make_async_copy(wn_ref.at[layer, rows, cols_of(k)], to, wsem.at[4 + UP_STEPS + k])

    def down_half(k, half):
        rows = block(half, HALF_K)
        return dot(mb[:, rows], wn[k, rows] if k < ahead else wu[k - ahead, rows])

    def load_next(j):
        return load_qkv(layer + 1, c, wq_ref, wu.at[pl.ds(4, 3)], wsem, j)

    for k in range(OUT_STEPS):
        load_dense(k).start()
    for j in range(UP_STEPS - 1):
        load_up(j).start()
    for k in range(ahead):
        load_down(k).start()
    if not last:
        cache = cache_copies(layer + 1, kc_ref, vc_ref, k_out, v_out, k_s)
        for copy in cache:
            copy.start()
    everyone = [lax.rem(tp * 4 + sp + r, 8) for r in range(1, 8)]
    enter([{'tp': peer // 4, 'sp': lax.rem(peer, 4)} for peer in everyone])
    waits = []

    def swap(i, src, dst, peer):
        copy = remote(src, dst, o_s.at[i], o_r.at[i], peer)
        copy.start()
        waits.append(copy)
        return copy

    stats = swap(4, ml_ref, mls, core_peer)
    slabs = [None, None]
    for n, xd in enumerate((ox, x)):
        src = o_ref.at[pl.ds((2 * xd + oc) * GROUP, GROUP)]
        slabs[n] = swap(n, src, fromcore.at[n], core_peer)

    def columns(rows):
        return jnp.concatenate(rows + [jnp.zeros((HEAD - GROUP * len(rows), HEAD), F32)], axis=0).T[:SEQS]

    def merge(one, two):
        top = jnp.maximum(one[:GROUP], two[:GROUP])
        first, second = jnp.exp(one[:GROUP] - top), jnp.exp(two[:GROUP] - top)
        return first, second, top, first * one[GROUP:] + second * two[GROUP:]

    stats.wait_recv()
    rows = []
    for n, xd in enumerate((ox, x)):
        first, second, top, total = merge(ml_ref[2 * xd + c], mls[2 * xd + c])
        rows += [first, second]
        mlx[n] = jnp.concatenate([top, total], axis=0)
    cross_ml = swap(5, mlx.at[0], mlx.at[2], x_peer)
    scale = columns(rows)
    for n, (xd, out) in enumerate(((ox, tosend), (x, kept))):
        slabs[n].wait_recv()
        kv = 2 * xd + c
        for g in range(GROUP):
            i = 2 * n * GROUP + g
            out[g] = o_ref[kv * GROUP + g] * scale[:, i:i + 1] + fromcore[n, g] * scale[:, i + GROUP:i + GROUP + 1]
        if n == 0:
            cross = swap(2, tosend, fromx, x_peer)
    if not last:
        rope_tables(rows_ref, freq_ref, cos, sin)
    cross_ml.wait_recv()
    first, second, _, total = merge(mlx[1], mlx[2])
    scale = columns([first / total, second / total])
    cross.wait_recv()
    for g in range(GROUP):
        val = (kept[g] * scale[:, g:g + 1] + fromx[g] * scale[:, g + GROUP:g + GROUP + 1]).astype(BF16)
        mine[g] = val.astype(F32)
        ob[:, block(c * GROUP + g, HEAD)] = val
    share = swap(3, mine, other, core_peer)
    def dense_half(k, half):
        return dot(ob[:, block(half, UP_N)], wu[UP_STEPS - 1, block(2 * k + half, UP_N)])

    for k in range(OUT_STEPS):
        load_dense(k).wait()
        ps[k] = dense_half(k, c)
    share.wait_recv()
    for g in range(GROUP):
        ob[:, block(oc * GROUP + g, HEAD)] = other[g].astype(BF16)

    own = (c * 4 + quarter[K3]) * 2

    def all_reduce(ph, chunk, residual, bias_ref, after=lambda: None, stats=True):
        def post(i, src, dst, peer):
            copy = remote(src, dst, c_s.at[ph, int(5 < i < STRIP)], c_r.at[ph, i], peer)
            copy.start()
            return copy

        def keep(k):
            val = chunk(k)
            part[ph, k, A] = val[:, :PIECE]
            part[ph, k, B] = val[:, PIECE:]

        def strips(i, src, dst, peer):
            return [post((i, i + STRIP)[n], src.at[:, cols], dst.at[:, cols], peer) for n, cols in enumerate(STRIPS)]

        keep(K0)
        a0 = strips(0, part.at[ph, K0, A], ra.at[ph, K0], x_peer)
        b0 = strips(1, part.at[ph, K0, B], rb.at[ph, K0], y_peer)
        keep(K1)
        a1 = post(2, part.at[ph, K1, A], ra.at[ph, K1], x_peer)
        keep(K2)
        b1 = post(3, part.at[ph, K2, B], rb.at[ph, K1], y_peer)
        keep(K3)
        after()
        a2, b2 = [], []
        for n, cols in enumerate(STRIPS):
            b0[n].wait_recv()
            part[ph, K1, B, :, cols] += rb[ph, K0, :, cols]
            ref = part.at[ph, K1, B, :, cols]
            b2.append(post((4, 4 + STRIP)[n], ref, rb.at[ph, K2, :, cols], x_peer))
            a0[n].wait_recv()
            part[ph, K2, A, :, cols] += ra[ph, K0, :, cols]
            ref = part.at[ph, K2, A, :, cols]
            a2.append(post((5, 5 + STRIP)[n], ref, ra.at[ph, K2, :, cols], y_peer))
        for half, (first, second, landed) in enumerate(((a1, a2, ra), (b1, b2, rb))):
            for copy in (first, *second):
                copy.wait_recv()
            cols = block(own + half, PIECE)
            full = part[ph, K3, half] + landed[ph, K1] + landed[ph, K2]
            xs[ph, own + half] = (residual(half, cols) + full + bias_ref[layer:layer + 1, cols].astype(F32)).astype(BF16).astype(F32)
        if stats:
            send_moments(ph)
        gather = {}
        for n in range(3):
            for half in range(2):
                peer = core_peer if n == 2 else (x_peer, y_peer)[(n + half) % 2]
                mine_ref = xs.at[ph, own + half]
                gather[half, n] = post(6 + 3 * half + n, mine_ref, mine_ref, peer)
        base = c * 8
        from_x = base + quarter[K1] * 2
        from_y = base + quarter[K2] * 2
        far = base + quarter[K0] * 2

        def forward(i, piece, peer):
            ref = xs.at[ph, piece]
            return post(i, ref, ref, peer)

        sent = {}

        def pump(step):
            if step == 0:
                gather[A, K0].wait_recv()
                sent[A_FAR] = forward(A_FAR, from_x, y_peer)
                sent[A_X] = forward(A_X, from_x, core_peer)
                gather[B, K0].wait_recv()
                sent[B_FAR] = forward(B_FAR, from_y + 1, x_peer)
                sent[B_Y] = forward(B_Y, from_y + 1, core_peer)
            elif step == 1:
                gather[A, K1].wait_recv()
                sent[A_Y] = forward(A_Y, from_y, core_peer)
                gather[B, K1].wait_recv()
                sent[B_X] = forward(B_X, from_x + 1, core_peer)
            else:
                sent[A_FAR].wait_recv()
                sent[A_LAST] = forward(A_LAST, far, core_peer)
                sent[B_FAR].wait_recv()
                sent[B_LAST] = forward(B_LAST, far + 1, core_peer)

        def arrive(group):
            for copy in {0: [gather[A, K2], gather[B, K2]], 2: [sent.get(i) for i in (A_X, B_Y, A_Y, B_X)], 3: [sent.get(i) for i in (A_LAST, B_LAST)]}.get(group, ()):
                copy.wait_recv()

        return pump, arrive

    me = tp * 4 + sp

    def send_moments(ph):
        a, b = xs[ph, own], xs[ph, own + 1]
        count = 2 * PIECE
        mean = (rowsum(a) + rowsum(b)) * (1.0 / count)
        spread = rowsum(jnp.square(a - mean)) + rowsum(jnp.square(b - mean))
        lane = lax.broadcasted_iota(jnp.int32, (SEQS, HEAD), 1)
        both = jnp.where(lane == 0, mean, jnp.where(lane == 1, spread, 0.0))
        st[ph, me] = jnp.concatenate([both, jnp.zeros((HEAD - SEQS, HEAD), F32)], axis=0).T[:8]
        for r in range(1, 8):
            peer = lax.rem(me + r, 8)
            remote(st.at[ph, me], st.at[ph, me], t_s.at[ph], t_r.at[ph], {'tp': peer // 4, 'sp': lax.rem(peer, 4)}).start()

    def moments(ph):
        remote(st.at[ph, pl.ds(0, 7)], st.at[ph, pl.ds(0, 7)], t_s.at[ph], t_r.at[ph], x_peer).wait()
        parts = [st[ph, i] for i in range(8)]
        mean = sum(p[0:1] for p in parts) * 0.125
        spread = sum(p[1:2] + (2.0 * PIECE) * jnp.square(p[0:1] - mean) for p in parts)
        scale = lax.rsqrt(spread * (1.0 / MODEL) + NORM_EPS)
        table = jnp.concatenate([mean, scale, jnp.zeros((HEAD - 2, HEAD), F32)], axis=0).T[:SEQS]
        mo[...] = table

    def slices(group):
        if group in (0, 3):
            return [core * 4 + quarter[K0 if group else K3] for core in (c, oc)]
        return [(oc if group == 2 else c) * 4 + quarter[k] for k in (K1, K2)]

    def norm_group(ph, row, norm, group):
        mean, scale = mo[:, 0:1], mo[:, 1:2]
        for n, index in enumerate(slices(group)):
            for half in range(2):
                cols = block(2 * index + half, PIECE)
                gain, shift = gain_ref[row, norm:norm + 1, cols].astype(F32), shift_ref[row, norm:norm + 1, cols].astype(F32)
                at = (2 * n + half) * PIECE
                u[:, at:at + PIECE] = ((xs[ph, 2 * index + half] - mean) * scale * gain + shift).astype(BF16)

    def product(group, slot):
        total = 0.0
        for n, index in enumerate(slices(group)):
            rows = block(index, UP_N)
            total = total + dot(u[:, n * 512:(n + 1) * 512], wu[slot, rows])
        return total

    def normed_product(ph, row, norm, stages, first, count, wait, finish_step):
        pump, arrive = stages

        def add(group, low, high):
            def step(j, _):
                if group == 0:
                    wait(j)
                    acc[j] = product(group, first + j)
                else:
                    acc[j] += product(group, first + j)
                return 0

            lax.fori_loop(low, high, step, 0, unroll=True)

        half = count // 2 + 1
        moments(ph)
        arrive(0)
        norm_group(ph, row, norm, 0)
        pump(0)
        add(0, 0, half)
        pump(1)
        add(0, half, count)
        for group in (1, 2):
            arrive(group)
            norm_group(ph, row, norm, group)
            add(group, 0, count)
            if group == 1:
                pump(2)
        arrive(3)
        norm_group(ph, row, norm, 3)
        finish_step(lambda j: acc[j] + product(3, first + j))

    def dense_chunk(k):
        return ps[k] + dense_half(k, oc)

    stages = all_reduce(0, dense_chunk, lambda half, cols: h_ref[:, cols].astype(F32), bd_ref, load_up(UP_STEPS - 1).start)
    take = (lax.broadcasted_iota(jnp.int32, (2 * HEAD, HEAD), 0) == 2 * lax.broadcasted_iota(jnp.int32, (2 * HEAD, HEAD), 1)).astype(BF16)
    even = lax.rem(lax.broadcasted_iota(jnp.int32, (SEQS, UP_N), 1), 2) == 0

    def share_m(j):
        return remote(mf.at[j], mp.at[j], m_s.at[0], m_r.at[0], core_peer)

    def up_step(full, j):
        cols = block((2 * x + c) * UP_STEPS + j, UP_N)
        val = full(j) + bu_ref[layer:layer + 1, cols].astype(F32)
        gate = jnp.minimum(val, GELU_LIMIT)
        gate = gate * (1.0 / (1.0 + jnp.exp(-1.702 * gate)))
        linear = jnp.clip(val, -GELU_LIMIT, GELU_LIMIT) + 1.0
        mixed = jnp.where(even, gate * pltpu.roll(linear, UP_N - 1, 1), 0.0).astype(BF16)
        packed = jnp.concatenate([dot(mixed[:, i:i + 2 * HEAD], take) for i in range(0, UP_N, 2 * HEAD)], axis=1)
        mf[j] = packed
        share_m(j).start()
        mb[:, block(c * UP_STEPS + j, PIECE)] = packed.astype(BF16)

        if j < 4 - ahead:
            load_down(j + ahead).start()
        if not last and j >= 4:
            load_next(j - 4).start()

    def up_steps(full):
        for j in range(UP_STEPS):
            up_step(full, j)

    normed_product(0, layer, 1, stages, 0, UP_STEPS, lambda j: load_up(j).wait(), up_steps)
    for k in range(OUT_STEPS):
        load_down(k).wait()
        ps[k] = down_half(k, c)
    remote(mf, mp, m_s.at[0], m_r.at[0], core_peer).wait()
    for j in range(UP_STEPS):
        mb[:, block(oc * UP_STEPS + j, PIECE)] = mp[j].astype(BF16)

    def down_chunk(k):
        return ps[k] + down_half(k, oc)

    stages = all_reduce(1, down_chunk, lambda half, cols: xs[0, own + half], bn_ref, stats=not last)
    def write(group):
        for index in slices(group):
            for half in range(2):
                out_ref[:, block(2 * index + half, PIECE)] = xs[1, 2 * index + half].astype(BF16)

    if last:
        pump, arrive = stages
        for step in range(3):
            pump(step)
            arrive(step)
            write(step)
        arrive(3)
        write(3)
    else:
        def qkv_steps(full):
            qkv_phase(layer + 1, c, core_peer, full, bq_ref, cos, sin, heads, q_s, q_r, lambda: [write(group) for group in range(4)])

        normed_product(1, layer + 1, 0, stages, 4, 3, lambda j: load_next(j).wait(), qkv_steps)
        heads_out[...] = heads[...]
        for copy in cache:
            copy.wait()
    for ph in range(2):
        for n, pieces in enumerate((6, 14)):
            remote(xs.at[ph, pl.ds(0, pieces)], xs.at[ph, pl.ds(0, pieces)], c_s.at[ph, n], c_r.at[ph, 0], x_peer).wait_send()
    for copy in waits:
        copy.wait_send()


def finish(layer, o, ml, h, gain, shift, bd, bu, bn, wd, wu, wn, *following):
    slab = pltpu.VMEM((GROUP, SEQS, HEAD), F32)
    dma = pltpu.SemaphoreType.DMA
    last = not following
    ahead = 4 if last else 1
    hidden = kept((SEQS, MODEL), BF16)
    table = pltpu.VMEM((SEQS, HEAD), F32)
    return pl.pallas_call(
        functools.partial(mlp_kernel, layer, last, ahead),
        out_shape=hidden if last else (hidden, kept(HEADS_SHAPE, F32), CACHE, CACHE),
        in_specs=[VM] * 8 + [HBM] * 3 + ([] if last else [VM, VM, VM, HBM, HBM, HBM]),
        out_specs=VM if last else (VM, VM, VM, VM),
        scratch_shapes=[
            pltpu.VMEM((UP_STEPS, MODEL, UP_N), BF16),
            pltpu.VMEM((ahead, DOWN_K, 512), BF16),
            pltpu.VMEM((KVL, 2 * GROUP, HEAD), F32),
            pltpu.VMEM((3, 2 * GROUP, HEAD), F32),
            pltpu.VMEM((2, GROUP, SEQS, HEAD), F32),
            slab, slab, slab, slab, slab,
            pltpu.VMEM((SEQS, 1024), BF16),
            pltpu.VMEM((2, 4, 2, SEQS, PIECE), F32),
            pltpu.VMEM((2, 3, SEQS, PIECE), F32),
            pltpu.VMEM((2, 3, SEQS, PIECE), F32),
            pltpu.VMEM((2, 16, SEQS, PIECE), F32),
            pltpu.VMEM((SEQS, 1024), BF16),
            pltpu.VMEM((UP_STEPS, SEQS, 256), F32),
            pltpu.VMEM((UP_STEPS, SEQS, 256), F32),
            pltpu.VMEM((SEQS, DOWN_K), BF16),
            pltpu.VMEM((4, SEQS, 512), F32),
            pltpu.VMEM((UP_STEPS, SEQS, UP_N), F32),
            pltpu.VMEM((2, 8, 8, HEAD), F32),
            pltpu.VMEM((SEQS, HEAD), F32),
            dma((8 + UP_STEPS,)), dma((6,)), dma((6,)), dma((1,)), dma((1,)), dma((2, 2)), dma((2, STRIP + 6)), dma((2,)), dma((2,)),
        ] + ([] if last else [pltpu.VMEM(HEADS_SHAPE, F32), table, table, dma((2,)), dma((6,)), dma((6,))]),
        compiler_params=exchange(2 + layer, 54 if last else MLP_MIB),
        name=f'mlp_{layer}',
    )(near(o), near(ml), near(h) if last else pin(h), *map(near, (gain, shift, bd, bu, bn)), *map(pin, (wd, wu, wn)), *map(near, following[:1]), *map(pin, following[1:]))


def solution(mesh):
    cache_spec = P(None, 'dp', 'sp', 'tp', None)
    rows, bias, cols = P(None, 'tp', None), P(None, 'tp'), P(None, None, 'tp')
    in_specs = (P('dp'), P('dp'), cache_spec, cache_spec, P(), P(), cols, bias, rows, P(), cols, bias, rows, P())
    out_specs = (P('dp'), cache_spec, cache_spec)

    def device_step(hidden, positions, k_cache, v_cache, ln_gain, ln_bias, w_qkv, b_qkv, w_dense, b_dense, w_up, b_up, w_down, b_down):
        freq = ROPE_THETA ** (-np.arange(HEAD // 2) * (2.0 / HEAD))
        freq = jnp.asarray(np.tile(freq, 2)[None].astype(np.float32))
        shape = k_cache.shape
        flat = (2, SEQS, ROWS, HEAD)
        kc = k_cache.reshape(flat)
        vc = v_cache.reshape(flat)
        done = ()
        heads, kb, vb, rows = project(0, positions, freq, hidden, ln_gain, ln_bias, b_qkv, w_qkv, kc, vc)
        for layer in range(2):
            ko, vo, o, ml = attend(layer, positions, heads.reshape(-1, HEAD), kb, vb, flat, *(done or (kc, vc)))
            done = (ko, vo)
            following = () if layer else (rows, freq, b_qkv, w_qkv, kc, vc)
            out = finish(layer, o.reshape(HEADS, SEQS, HEAD), ml, hidden, ln_gain, ln_bias, b_dense, b_up, b_down, w_dense, w_up, w_down, *following)
            hidden, heads, kb, vb = out if following else (out, None, None, None)
        return hidden, done[0].reshape(shape), done[1].reshape(shape)

    return jax.shard_map(device_step, mesh=mesh, in_specs=in_specs, out_specs=out_specs, check_vma=False)
```
